128 devices in a mesh: tile: 32 (over x, y, core), head: 4 (over z).
Axes of the slice: x: 4, y: 4, z: 4, core: 2. Of those that a mesh axis runs over, the one named last changes fastest.
Arguments:
- latent: bfloat16 [64, 512, 512], P('tile', 'head'), may hold values from -6 to 6
- norm1_gain: float32 [512], replicated, may hold values from 0.25 to 1.75
- norm1_shift: float32 [512], replicated, may hold values from -1.75 to 1.75
- conv1_weight: bfloat16 [3, 3, 512, 512], replicated, may hold values from -0.09375 to 0.09375
- conv1_bias: float32 [512], replicated, may hold values from -1.75 to 1.75
- norm2_gain: float32 [512], replicated, may hold values from 0.25 to 1.75
- norm2_shift: float32 [512], replicated, may hold values from -1.75 to 1.75
- conv2_weight: bfloat16 [3, 3, 512, 512], replicated, may hold values from -0.09375 to 0.09375
- conv2_bias: float32 [512], replicated, may hold values from -1.75 to 1.75
- norm3_gain: float32 [512], replicated, may hold values from 0.25 to 1.75
- norm3_shift: float32 [512], replicated, may hold values from -1.75 to 1.75
- query_weight: bfloat16 [512, 512], replicated, may hold values from -2 to 2
- query_bias: float32 [512], replicated, may hold values from -3 to 3
- key_weight: bfloat16 [512, 512], replicated, may hold values from -2 to 2
- value_weight: bfloat16 [512, 512], replicated, may hold values from -0.25 to 0.25
- value_bias: float32 [512], replicated, may hold values from -3 to 3
- out_weight: bfloat16 [512, 512], replicated, may hold values from -0.5 to 0.5
- out_bias: float32 [512], replicated, may hold values from -1.75 to 1.75
Outputs:
- block_out: bfloat16 [64, 512, 512], P('tile', 'head')
The draws below stay inside these ranges and needn't reach their ends.
All inputs are finite; a program needn't handle non-finite values.
Results may differ from the reference program's by a relative error of at most 0.01615.
Values may be sent and summed in bfloat16 or wider, within the bound.
A program may use at most 128 MiB of HBM per device.

```python
import jax
import jax.numpy as jnp
from jax import lax

C = 512
GROUPS = 32
W = 512
H = 64


def base_projection(key, salt):
    entries = jax.random.normal(jax.random.fold_in(key, salt), (C, C), jnp.float32)
    return jnp.clip(entries, -4.0, 4.0) * (1.0 / jnp.sqrt(jnp.float32(C // 4)))


def draw_query_weight(key, part):
    weight = base_projection(key, 311)
    return weight.astype(jnp.bfloat16)


def draw_key_weight(key, part):
    weight = base_projection(key, 523)
    return weight.astype(jnp.bfloat16)


def smooth_field(key):
    freq_rows = jax.random.randint(jax.random.fold_in(key, 7101), (4,), 1, 4).astype(jnp.float32)
    freq_cols = jax.random.randint(jax.random.fold_in(key, 7102), (4,), 0, 4).astype(jnp.float32)
    phases = jax.random.uniform(jax.random.fold_in(key, 7103), (4,), jnp.float32, -jnp.pi, jnp.pi)
    amplitudes = jax.random.uniform(jax.random.fold_in(key, 7104), (4,), jnp.float32, 0.5, 0.9)
    row_pos = jnp.arange(H, dtype=jnp.float32) / jnp.float32(H)
    col_pos = jnp.arange(W, dtype=jnp.float32) / jnp.float32(W)
    phase_grid = 2.0 * jnp.pi * (freq_rows[:, None, None] * row_pos[None, :, None] + freq_cols[:, None, None] * col_pos[None, None, :]) + phases[:, None, None]
    return jnp.sum(amplitudes[:, None, None] * jnp.cos(phase_grid), axis=0) + 0.4


def draw_latent(key, part):
    field = smooth_field(key)
    loading = jax.random.normal(jax.random.fold_in(key, 7105), (C,), jnp.float32)
    noise = 0.7 * jax.random.normal(jax.random.fold_in(key, 7106), (H, W, C), jnp.float32)
    values = noise + field[:, :, None] * loading[None, None, :]
    return jnp.clip(values, -6.0, 6.0).astype(jnp.bfloat16)


def gaussian(key, dims, scale, most, kind=jnp.bfloat16):
    return jnp.clip(scale * jax.random.normal(key, dims, jnp.float32), -most, most).astype(kind)


def setup_inputs(seed: int = 0) -> dict:
    arg_keys = jax.random.split(jax.random.key(seed), 19)
    latent = draw_latent(jax.random.fold_in(arg_keys[18], 71), 0)
    norm1_gain = jnp.clip(1.0 + 0.15 * jax.random.normal(arg_keys[1], (C,), jnp.float32), 0.25, 1.75)
    norm1_shift = gaussian(arg_keys[2], (C,), 0.3, 1.75, jnp.float32)
    conv1_weight = gaussian(arg_keys[3], (3, 3, C, C), (9 * C) ** -0.5, 0.09375)
    conv1_bias = gaussian(arg_keys[4], (C,), 0.3, 1.75, jnp.float32)
    norm2_gain = jnp.clip(1.0 + 0.15 * jax.random.normal(arg_keys[5], (C,), jnp.float32), 0.25, 1.75)
    norm2_shift = gaussian(arg_keys[6], (C,), 0.3, 1.75, jnp.float32)
    conv2_weight = gaussian(arg_keys[7], (3, 3, C, C), (9 * C) ** -0.5, 0.09375)
    conv2_bias = gaussian(arg_keys[8], (C,), 0.3, 1.75, jnp.float32)
    norm3_gain = jnp.clip(1.0 + 0.15 * jax.random.normal(arg_keys[9], (C,), jnp.float32), 0.25, 1.75)
    norm3_shift = gaussian(arg_keys[10], (C,), 0.3, 1.75, jnp.float32)
    query_weight = draw_query_weight(jax.random.fold_in(arg_keys[18], 71), 0)
    query_bias = gaussian(arg_keys[12], (C,), 0.5, 3.0, jnp.float32)
    key_weight = draw_key_weight(jax.random.fold_in(arg_keys[18], 71), 0)
    value_weight = gaussian(arg_keys[14], (C, C), C ** -0.5, 0.25)
    value_bias = gaussian(arg_keys[15], (C,), 0.5, 3.0, jnp.float32)
    out_weight = gaussian(arg_keys[16], (C, C), (C // 4) ** -0.5, 0.5)
    out_bias = gaussian(arg_keys[17], (C,), 0.3, 1.75, jnp.float32)
    return dict(latent=latent, norm1_gain=norm1_gain, norm1_shift=norm1_shift, conv1_weight=conv1_weight, conv1_bias=conv1_bias, norm2_gain=norm2_gain, norm2_shift=norm2_shift, conv2_weight=conv2_weight, conv2_bias=conv2_bias, norm3_gain=norm3_gain, norm3_shift=norm3_shift, query_weight=query_weight, query_bias=query_bias, key_weight=key_weight, value_weight=value_weight, value_bias=value_bias, out_weight=out_weight, out_bias=out_bias)


def group_norm(values, gain, shift):
    grouped = values.reshape(-1, GROUPS, C // GROUPS)
    mean = lax.optimization_barrier(jnp.mean(grouped, axis=(0, 2)))
    deviation = grouped - mean[None, :, None]
    variance = lax.optimization_barrier(jnp.mean(deviation * deviation, axis=(0, 2)))
    normalized = deviation * lax.rsqrt(variance + 1e-06)[None, :, None]
    return normalized.reshape(values.shape) * gain + shift

def conv_three(act, weight, bias):
    result = lax.conv_general_dilated(act[None], weight, (1, 1), ((1, 1), (1, 1)), dimension_numbers=('NHWC', 'HWIO', 'NHWC'), preferred_element_type=jnp.float32)[0]
    return result + bias

def reference(latent, norm1_gain, norm1_shift, conv1_weight, conv1_bias, norm2_gain, norm2_shift, conv2_weight, conv2_bias, norm3_gain, norm3_shift, query_weight, query_bias, key_weight, value_weight, value_bias, out_weight, out_bias):
    latent32 = latent.astype(jnp.float32)
    act1 = jax.nn.silu(group_norm(latent32, norm1_gain, norm1_shift)).astype(jnp.bfloat16)
    hidden = conv_three(act1, conv1_weight, conv1_bias)
    act2 = jax.nn.silu(group_norm(hidden, norm2_gain, norm2_shift)).astype(jnp.bfloat16)
    resid = (latent32 + conv_three(act2, conv2_weight, conv2_bias)).astype(jnp.bfloat16)
    flat_res = resid.reshape(-1, C)
    normed = group_norm(flat_res.astype(jnp.float32), norm3_gain, norm3_shift).astype(jnp.bfloat16)
    queries = (jnp.dot(normed, query_weight, preferred_element_type=jnp.float32) + query_bias).astype(jnp.bfloat16)
    keys = jnp.dot(normed, key_weight, preferred_element_type=jnp.float32).astype(jnp.bfloat16)
    values = (jnp.dot(normed, value_weight, preferred_element_type=jnp.float32) + value_bias).astype(jnp.bfloat16)
    total_rows = queries.shape[0]
    block_rows = 1024 if total_rows % 1024 == 0 else total_rows
    softmax_scale = 1.0 / C ** 0.5

    def attend(query_block):
        scores = jnp.dot(query_block, keys.T, preferred_element_type=jnp.float32) * softmax_scale
        top = lax.optimization_barrier(jnp.max(scores, axis=1, keepdims=True))
        expo = jnp.exp(scores - top)
        row_sum = lax.optimization_barrier(jnp.sum(expo, axis=1, keepdims=True))
        weighted = jnp.dot(expo.astype(jnp.bfloat16), values, preferred_element_type=jnp.float32)
        return (weighted / row_sum).astype(jnp.bfloat16)
    attended = lax.map(attend, queries.reshape(total_rows // block_rows, block_rows, C)).reshape(total_rows, C)
    mixed = flat_res.astype(jnp.float32) + jnp.dot(attended, out_weight, preferred_element_type=jnp.float32) + out_bias
    return mixed.astype(jnp.bfloat16).reshape(latent.shape)
```

```python
import functools

import jax
import jax.numpy as jnp
from jax import lax
from jax.experimental import pallas as pl
from jax.experimental.pallas import tpu as pltpu
from jax.sharding import Mesh
from jax.sharding import PartitionSpec as P

C = 512
GROUPS = 32
AXES = ("tile_0", "tile_1", "tile_2", "head")
TILE = ("tile_0", "tile_1", "tile_2")
MESH = pl.DeviceIdType.MESH
BF = jnp.bfloat16
F32 = jnp.float32
EPS = 1e-06

ROWS, COLS = 2, 128
POS = ROWS * COLS
RING = 4
TILES = 32
SLOTS = 16
CHUNKS = 8
QT = 512
KC = 1024
LPAD = 16
HPAD = 8
NT = (((1,), (1,)), ((), ()))
NN = (((1,), (0,)), ((), ()))


def slot_of(dx, dy):
    if dy == 0:
        return dx
    if dx == 0:
        return 3 + dy
    return 7 + (dx - 1) * 3 + (dy - 1)


def dot(a, b, dims=NN):
    return lax.dot_general(a, b, dims, preferred_element_type=F32)


def copy_to(src, dst, send, recv, dev):
    return pltpu.make_async_remote_copy(
        src_ref=src, dst_ref=dst, send_sem=send, recv_sem=recv, device_id=dev, device_id_type=MESH
    )


def block_kernel(*refs):
    hbm = refs[:18]
    out_hbm = refs[18]
    (
        vecs, w1, w2, wp, ext, tmp, act, acc_c, hext, ar_tx, ar_rx,
        kv, qres, qq, s0, s1, p0, p1, acc0, acc1, m0, m1, l0, l1, a0, a1,
        ctx_tx, lse_tx, ctx_rx, lse_rx, out_v,
        ld, out_sem, h_send, h_recv, ar_send, ar_recv,
        kv_send, kv_recv, d_send, d_recv, q_send, q_recv, c_send, c_recv, e_send, e_recv,
    ) = refs[19:]
    x = lax.axis_index("tile_0")
    y = lax.axis_index("tile_1")
    c = lax.axis_index("tile_2")
    z = lax.axis_index("head")
    t = (x * RING + y) * 2 + c

    def ring(v, i):
        return lax.rem(v + i, RING)

    def tile_dev(dt, dz):
        n = lax.rem(t + dt + TILES, TILES)
        return (n // 8, lax.rem(n // 2, RING), lax.rem(n, 2), lax.rem(z + dz + RING, RING))

    sibling = (x, y, 1 - c, z)

    (lat, g1, b1, cw1, cb1, g2, b2, cw2, cb2, g3, b3, wq, bq, wk, wv, bv, wo, bo) = hbm
    loads = [pltpu.make_async_copy(lat, ext.at[1:3, LPAD : LPAD + COLS], ld.at[0])]
    for i, v in enumerate((g1, b1, cb1, g2, b2, cb2, g3, b3, bq, bv, bo)):
        loads.append(pltpu.make_async_copy(v, vecs.at[i], ld.at[1 + i]))
    loads.append(pltpu.make_async_copy(cw1, w1, ld.at[12]))
    loads.append(pltpu.make_async_copy(cw2, w2, ld.at[13]))
    for i, w in enumerate((wq, wk, wv, wo)):
        loads.append(pltpu.make_async_copy(w, wp.at[i], ld.at[14 + i]))
    for copy in loads:
        copy.start()

    barrier = pltpu.get_barrier_semaphore()
    peers = [sibling]
    for i in range(1, RING):
        peers += [(ring(x, i), y, c, z), (x, ring(y, i), c, z), (x, y, c, ring(z, i))]
    for dt in (-1, 1):
        for dz in (-1, 0, 1):
            peers.append(tile_dev(dt, dz))
    for dev in peers:
        pl.semaphore_signal(barrier, inc=1, device_id=dev, device_id_type=MESH)
    pl.semaphore_wait(barrier, len(peers))

    loads[0].wait()

    def halo(buf, pad, k):
        lo, hi = pad, pad + COLS
        own = slice(lo, hi)
        first, last = slice(lo, lo + pad), slice(hi - pad, hi)
        left, right = slice(0, lo), slice(hi, hi + pad)
        plan = [
            ((1, 2, own), (3, 4, own), (-1, 0)),
            ((2, 3, own), (0, 1, own), (1, 0)),
            ((1, 3, first), (1, 3, right), (0, -1)),
            ((1, 3, last), (1, 3, left), (0, 1)),
            ((1, 2, first), (3, 4, right), (-1, -1)),
            ((1, 2, last), (3, 4, left), (-1, 1)),
            ((2, 3, first), (0, 1, right), (1, -1)),
            ((2, 3, last), (0, 1, left), (1, 1)),
        ]
        copies = []
        for n, (s, d, (dt, dz)) in enumerate(plan):
            copies.append(
                copy_to(
                    buf.at[s[0] : s[1], s[2]], buf.at[d[0] : d[1], d[2]],
                    h_send.at[k, n], h_recv.at[k, n], tile_dev(dt, dz),
                )
            )
        return copies

    def moments(v):
        return jnp.concatenate(
            [jnp.sum(v, axis=0, keepdims=True), jnp.sum(v * v, axis=0, keepdims=True)], axis=0
        )

    STAGES = (("z", 0), ("x", 3), ("y", 6), ("c", 9))

    def stat_copies(k, stage):
        name, base = STAGES[stage]
        copies = []
        for i in range(1, 2 if name == "c" else RING):
            dev = {
                "z": (x, y, c, ring(z, i)),
                "x": (ring(x, i), y, c, z),
                "y": (x, ring(y, i), c, z),
                "c": sibling,
            }[name]
            n = base + i - 1
            copies.append(
                copy_to(ar_tx.at[k, stage], ar_rx.at[k, n], ar_send.at[k, n], ar_recv.at[k, n], dev)
            )
        return copies

    def all_stats(k, local, after=(None, None, None, None)):
        total = local
        pending = []
        for stage in range(4):
            ar_tx[k, stage] = total
            copies = stat_copies(k, stage)
            for copy in copies:
                copy.start()
            if after[stage] is not None:
                after[stage]()
            base = STAGES[stage][1]
            for n, copy in enumerate(copies):
                copy.wait_recv()
                total = total + ar_rx[k, base + n]
            pending += copies
        for copy in pending:
            copy.wait_send()
        return total

    lane = lax.broadcasted_iota(jnp.int32, (8, C), 1)

    def affine(total, gain, shift):
        both = jnp.concatenate([total, jnp.zeros((6, C), F32)], axis=0)
        for d in (1, 2, 4, 8):
            up = pltpu.roll(both, C - d, 1)
            down = pltpu.roll(both, d, 1)
            both = both + jnp.where((lane & d) == 0, up, down)
        members = float(POS * TILES * RING * (C // GROUPS))
        mean = both[0:1] / members
        var = jnp.maximum(both[1:2] / members - mean * mean, 0.0)
        scale = lax.rsqrt(var + EPS) * gain
        return scale, shift - mean * scale

    def activate(buf, pad, width, scale, shift):
        col = lax.broadcasted_iota(jnp.int32, (width, 1), 0)
        edge = ((col >= pad) | (z > 0)) & ((col < pad + COLS) | (z < RING - 1))

        def one_row(r, _):
            inside = ((r > 0) | (t > 0)) & ((r < 3) | (t < TILES - 1))
            u = buf[r].astype(F32) * scale + shift
            u = u / (1.0 + jnp.exp(-u))
            tmp[0:width] = jnp.where(edge & inside, u, 0.0)
            for dj in range(3):
                act[dj, r] = tmp[pad - 1 + dj : pad - 1 + dj + COLS].astype(BF)
            return 0

        lax.fori_loop(0, 4, one_row, 0)

    def conv(weight):
        acc_c[...] = jnp.zeros_like(acc_c)

        def three_taps(di, _):
            part = None
            for dj in range(3):
                a = act[dj, pl.ds(di, 2)].reshape(POS, C)
                d = dot(a, weight[di * 3 + dj])
                part = d if part is None else part + d
            acc_c[...] += part
            return 0

        lax.fori_loop(0, 3, three_taps, 0)

    def vec(i):
        return vecs[i]

    halo0 = halo(ext, LPAD, 0)
    latent = ext[1:3, LPAD : LPAD + COLS].astype(F32).reshape(POS, C)

    def start_halo0():
        for copy in halo0:
            copy.start()

    total = all_stats(0, moments(latent), (start_halo0, None, None, None))
    for copy in loads[1:12]:
        copy.wait()
    for copy in halo0:
        copy.wait_recv()
    scale, shift = affine(total, vec(0), vec(1))
    activate(ext, LPAD, COLS + 2 * LPAD, scale, shift)
    loads[12].wait()
    conv(w1)

    hid = acc_c[...] + vec(2)
    hext[1:3, HPAD : HPAD + COLS] = hid.reshape(ROWS, COLS, C)
    halo1 = halo(hext, HPAD, 1)

    def start_halo1():
        for copy in halo1:
            copy.start()

    total = all_stats(1, moments(hid), (start_halo1, None, None, None))
    for copy in halo1:
        copy.wait_recv()
    scale, shift = affine(total, vec(3), vec(4))
    activate(hext, HPAD, COLS + 2 * HPAD, scale, shift)
    loads[13].wait()
    conv(w2)
    latent = ext[1:3, LPAD : LPAD + COLS].astype(F32).reshape(POS, C)
    res = (latent + (acc_c[...] + vec(5))).astype(BF)
    kv[0, 0] = res

    def half(n, h):
        return kv.at[n, 0, pl.ds(h * COLS, COLS)]

    def own_copy(axis, i, h, n):
        dev = (ring(x, i), y, c, z) if axis == "x" else (x, ring(y, i), c, z)
        back = RING - i
        there = slot_of(back, 0) if axis == "x" else slot_of(0, back)
        return copy_to(half(0, h), half(there, h), kv_send.at[n], kv_recv.at[there, h], dev)

    first_x = [own_copy("x", i, 0, k) for k, i in enumerate((1, 3, 2))]
    first_y = [own_copy("y", i, 1, 3 + k) for k, i in enumerate((1, 3, 2))]
    later_x = [own_copy("x", i, 1, 6 + k) for k, i in enumerate((1, 3, 2))]
    later_y = [own_copy("y", i, 0, 9 + k) for k, i in enumerate((1, 3, 2))]
    onward = []
    for k in range(1, RING):
        for i in (1, 3, 2):
            there = slot_of(k, RING - i)
            here = slot_of(k, 0)
            onward.append(
                copy_to(half(here, 0), half(there, 0), kv_send.at[12 + len(onward)],
                        kv_recv.at[there, 0], (x, ring(y, i), c, z))
            )
            there = slot_of(RING - i, k)
            here = slot_of(0, k)
            onward.append(
                copy_to(half(here, 1), half(there, 1), kv_send.at[12 + len(onward)],
                        kv_recv.at[there, 1], (ring(x, i), y, c, z))
            )
    to_z = [
        copy_to(kv.at[0, 0], qres.at[RING - 1 - i], q_send.at[i - 1], q_recv.at[RING - 1 - i],
                (x, y, c, ring(z, i)))
        for i in (1, 3, 2)
    ]
    pass_own = copy_to(kv.at[0, 0], kv.at[0, 1], d_send.at[0], d_recv.at[0], sibling)

    def begin(copies):
        for copy in copies:
            copy.start()

    res32 = res.astype(F32)
    total = all_stats(
        2,
        moments(res32),
        (
            lambda: begin(to_z + first_x[:2] + first_y),
            lambda: begin(first_x[2:] + later_x),
            lambda: begin(later_y),
            lambda: begin([pass_own]),
        ),
    )
    for k in range(1, RING):
        copy_to(half(0, 0), half(slot_of(k, 0), 0), kv_send.at[0], kv_recv.at[slot_of(k, 0), 0],
                sibling).wait_recv()
        copy_to(half(0, 1), half(slot_of(0, k), 1), kv_send.at[0], kv_recv.at[slot_of(0, k), 1],
                sibling).wait_recv()
    begin(onward)

    scale3, shift3 = affine(total, vec(6), vec(7))
    for copy in loads[14:]:
        copy.wait()
    qres[RING - 1] = res
    for r in range(RING - 1):
        copy_to(kv.at[0, 0], qres.at[r], q_send.at[0], q_recv.at[r], sibling).wait_recv()
    to_exp2 = scale3 * (1.4426950408889634 / C**0.5)
    for r in range(RING):
        normed = (qres[r].astype(F32) * scale3 + shift3).astype(BF)
        q = (dot(normed, wp[0]) + vec(8)).astype(BF)
        qq[r * POS : (r + 1) * POS] = (dot(q, wp[1], NT) * to_exp2).astype(BF)

    for ref in (acc0, acc1, l0, l1):
        ref[...] = jnp.zeros_like(ref)
    for ref in (m0, m1):
        ref[...] = jnp.full_like(ref, -1e30)
    a1[...] = jnp.ones_like(a1)
    p1[...] = jnp.zeros_like(p1)

    def pass_on(n):
        return copy_to(kv.at[n, 0], kv.at[n, 1], d_send.at[n], d_recv.at[n], sibling)

    def wait_half(n, h):
        ref = kv.at[n, 0, pl.ds(h * COLS, COLS)]
        copy_to(ref, ref, kv_send.at[0], kv_recv.at[n, h], sibling).wait_recv()

    def keys(ck):
        return kv[pl.ds(2 * ck, 2)].reshape(KC, C)

    def score(qt, ck, s):
        s[...] = dot(qq[qt * QT : (qt + 1) * QT], keys(ck), NT)

    def soften(s, p, m, l, a):
        step = 32
        for r in range(0, QT, step):
            rows = slice(r, r + step)
            sc = s[rows]
            old = m[rows]
            new = jnp.maximum(old, jnp.max(sc, axis=1, keepdims=True))
            e = jnp.exp2(sc - jnp.concatenate([new] * (KC // 128), axis=1)).astype(BF)
            p[rows] = e
            factor = jnp.exp2(old - new)
            e32 = e.astype(F32)
            part = l[rows] * factor
            for j in range(KC // 128):
                part = part + e32[:, j * 128 : (j + 1) * 128]
            l[rows] = part
            m[rows] = new
            a[rows] = factor

    def weigh(p, acc, a, ck):
        factor = a[...]
        acc[...] = acc[...] * jnp.concatenate([factor] * 4, axis=1) + dot(p[...], keys(ck))

    for k in range(1, 4):
        wait_half(k, 1)
        pass_on(k).start()
    copy_to(kv.at[0, 0], kv.at[0, 1], d_send.at[0], d_recv.at[0], sibling).wait_recv()
    pass_on(1).wait_recv()
    score(0, 0, s0)

    def chunk(ck, _):
        score(1, ck, s1)
        soften(s0, p0, m0, l0, a0)
        weigh(p1, acc1, a1, jnp.maximum(ck - 1, 0))
        nxt = jnp.minimum(ck + 1, CHUNKS - 1)

        @pl.when(ck < CHUNKS - 1)
        def _():
            for j in range(2):
                pass_on(2 * nxt + j).wait_recv()

        ahead = ck + 2

        @pl.when(ahead < CHUNKS)
        def _():
            for j in range(2):
                n = 2 * ahead + j

                @pl.when(n > 6)
                def _():
                    wait_half(n, 0)

                @pl.when(n > 6)
                def _():
                    wait_half(n, 1)

                @pl.when(n <= 6)
                def _():
                    wait_half(n, 0)

                pass_on(n).start()

        score(0, nxt, s0)
        soften(s1, p1, m1, l1, a1)
        weigh(p0, acc0, a0, ck)
        return 0

    lax.fori_loop(0, CHUNKS, chunk, 0)
    weigh(p1, acc1, a1, CHUNKS - 1)

    def finish(r):
        acc, m, l = ((acc0, m0, l0), (acc1, m1, l1))[r // 2]
        rows = slice((r % 2) * POS, (r % 2 + 1) * POS)
        total_l = jnp.sum(l[rows], axis=1, keepdims=True)
        ctx = acc[rows] * (1.0 / total_l) * scale3 + shift3
        return ctx, m[rows] + jnp.log2(total_l)

    sent = []
    for r in range(RING - 1):
        ctx, lse = finish(r)
        ctx_tx[r] = ctx.astype(BF)
        lse_tx[r] = lse.T[0:8]
        there = RING - 2 - r
        dev = (x, y, c, ring(z, r + 1))
        sent.append(copy_to(ctx_tx.at[r], ctx_rx.at[there], c_send.at[r], c_recv.at[there], dev))
        sent.append(copy_to(lse_tx.at[r], lse_rx.at[there], e_send.at[r], e_recv.at[there], dev))
        begin(sent[-2:])
    ctx, lse = finish(RING - 1)
    for copy in sent:
        copy.wait_recv()
    others = [jnp.broadcast_to(lse_rx[r, 0:1], (128, POS)).T for r in range(RING - 1)]
    top = lse
    for o in others:
        top = jnp.maximum(top, o)
    weight = jnp.exp2(lse - top)
    norm = weight
    ctx = ctx * jnp.concatenate([weight] * 4, axis=1)
    for r, o in enumerate(others):
        w = jnp.exp2(o - top)
        norm = norm + w
        ctx = ctx + ctx_rx[r].astype(F32) * jnp.concatenate([w] * 4, axis=1)
    inv = 1.0 / norm
    ctx = (ctx * jnp.concatenate([inv] * 4, axis=1)).astype(BF)
    attended = (dot(ctx, wp[2]) + vec(9)).astype(BF)
    mixed = qres[RING - 1].astype(F32) + dot(attended, wp[3]) + vec(10)
    out_v[...] = mixed.astype(BF).reshape(ROWS, COLS, C)
    done = pltpu.make_async_copy(out_v, out_hbm, out_sem)
    done.start()
    for copy in halo0 + halo1 + first_x + first_y + later_x + later_y + onward + to_z + sent:
        copy.wait_send()
    for n in range(SLOTS):
        pass_on(n).wait_send()
    done.wait()


def per_device(latent, *params):
    row = lambda v: v.reshape(1, C)
    args = [latent]
    for p in params:
        args.append(row(p) if p.ndim == 1 else (p.reshape(9, C, C) if p.ndim == 4 else p))
    dma = pltpu.SemaphoreType.DMA
    v = pltpu.VMEM
    scratch = [
        v((11, 1, C), F32), v((9, C, C), BF), v((9, C, C), BF), v((4, C, C), BF),
        v((4, COLS + 2 * LPAD, C), BF), v((COLS + 2 * LPAD, C), F32), v((3, 4, COLS, C), BF),
        v((POS, C), F32), v((4, COLS + 2 * HPAD, C), F32),
        v((3, 4, 2, C), F32), v((3, 10, 2, C), F32),
        v((SLOTS, 2, POS, C), BF), v((RING, POS, C), BF), v((RING * POS, C), BF),
        v((QT, KC), F32), v((QT, KC), F32), v((QT, KC), BF), v((QT, KC), BF),
        v((QT, C), F32), v((QT, C), F32),
        v((QT, 128), F32), v((QT, 128), F32), v((QT, 128), F32), v((QT, 128), F32),
        v((QT, 128), F32), v((QT, 128), F32),
        v((3, POS, C), BF), v((3, 8, POS), F32), v((3, POS, C), BF), v((3, 8, POS), F32),
        v((ROWS, COLS, C), BF),
        dma((18,)), dma, dma((2, 8)), dma((2, 8)), dma((3, 10)), dma((3, 10)),
        dma((30,)), dma((SLOTS, 2)), dma((SLOTS,)), dma((SLOTS,)), dma((3,)), dma((3,)),
        dma((3,)), dma((3,)), dma((3,)), dma((3,)),
    ]
    return pl.pallas_call(
        block_kernel,
        out_shape=jax.ShapeDtypeStruct((ROWS, COLS, C), BF),
        in_specs=[pl.BlockSpec(memory_space=pl.ANY)] * 18,
        out_specs=pl.BlockSpec(memory_space=pl.ANY),
        scratch_shapes=scratch,
        compiler_params=pltpu.CompilerParams(
            collective_id=0, has_side_effects=True, vmem_limit_bytes=60 * 1024 * 1024
        ),
    )(*args)


def solution(mesh):
    finer = Mesh(mesh.devices.reshape(4, 4, 2, mesh.shape["head"]), AXES)
    return jax.shard_map(
        per_device,
        mesh=finer,
        in_specs=(P(TILE, "head", None),) + (P(),) * 17,
        out_specs=P(TILE, "head", None),
        check_vma=False,
    )
```

```python
import functools

import jax
import jax.numpy as jnp
from jax import lax
from jax.experimental import pallas as pl
from jax.experimental.pallas import tpu as pltpu
from jax.sharding import Mesh
from jax.sharding import PartitionSpec as P

C = 512
GROUPS = 32
AXES = ("tile_0", "tile_1", "tile_2", "head")
TILE = ("tile_0", "tile_1", "tile_2")
MESH = pl.DeviceIdType.MESH
BF = jnp.bfloat16
F32 = jnp.float32
EPS = 1e-06

ROWS, COLS = 2, 128
POS = ROWS * COLS
RING = 4
TILES = 32
SLOTS = 16
CHUNKS = 8
QT = 512
KC = 1024
LPAD = 16
HPAD = 8
NT = (((1,), (1,)), ((), ()))
NN = (((1,), (0,)), ((), ()))


FAR = ((1, 1), (3, 3), (1, 3), (3, 1), (2, 1), (1, 2), (3, 2), (2, 3), (2, 2))


def slot_of(dx, dy):
    if dy == 0:
        return dx
    if dx == 0:
        return 3 + dy
    return 7 + FAR.index((dx, dy))


def dot(a, b, dims=NN):
    return lax.dot_general(a, b, dims, preferred_element_type=F32)


def copy_to(src, dst, send, recv, dev):
    return pltpu.make_async_remote_copy(
        src_ref=src, dst_ref=dst, send_sem=send, recv_sem=recv, device_id=dev, device_id_type=MESH
    )


def block_kernel(*refs):
    hbm = refs[:18]
    out_hbm = refs[18]
    (
        vecs, w1, w2, wp, ext, tmp, act, acc_c, hext, ar_tx, ar_rx,
        kv, qres, qq, s0, s1, p0, p1, acc0, acc1, m0, m1, l0, l1, a0, a1,
        ctx_tx, lse_tx, ctx_rx, lse_rx, out_v,
        ld, out_sem, h_send, h_recv, ar_send, ar_recv,
        kv_send, kv_recv, d_send, d_recv, q_send, q_recv, c_send, c_recv, e_send, e_recv,
    ) = refs[19:]
    x = lax.axis_index("tile_0")
    y = lax.axis_index("tile_1")
    c = lax.axis_index("tile_2")
    z = lax.axis_index("head")
    t = (x * RING + y) * 2 + c

    def ring(v, i):
        return lax.rem(v + i, RING)

    def tile_dev(dt, dz):
        n = lax.rem(t + dt + TILES, TILES)
        return (n // 8, lax.rem(n // 2, RING), lax.rem(n, 2), lax.rem(z + dz + RING, RING))

    sibling = (x, y, 1 - c, z)

    (lat, g1, b1, cw1, cb1, g2, b2, cw2, cb2, g3, b3, wq, bq, wk, wv, bv, wo, bo) = hbm
    loads = [pltpu.make_async_copy(lat, ext.at[1:3, LPAD : LPAD + COLS], ld.at[0])]
    for i, v in enumerate((g1, b1, cb1, g2, b2, cb2, g3, b3, bq, bv, bo)):
        loads.append(pltpu.make_async_copy(v, vecs.at[i], ld.at[1 + i]))
    loads.append(pltpu.make_async_copy(cw1, w1, ld.at[12]))
    loads.append(pltpu.make_async_copy(cw2, w2, ld.at[13]))
    for i, w in enumerate((wq, wk, wv, wo)):
        loads.append(pltpu.make_async_copy(w, wp.at[i], ld.at[14 + i]))
    for copy in loads:
        copy.start()

    for ref in (acc0, acc1, l0, l1):
        ref[...] = jnp.zeros_like(ref)
    for ref in (m0, m1):
        ref[...] = jnp.full_like(ref, -1e30)
    a1[...] = jnp.ones_like(a1)
    p1[...] = jnp.zeros_like(p1)

    barrier = pltpu.get_barrier_semaphore()
    column = [sibling]
    for i in (1, 3, 2):
        column += [(x, y, c, ring(z, i)), (x, y, 1 - c, ring(z, i))]
    plane = []
    for i in range(RING):
        plane += [(ring(x, i), ring(y, j), c, z) for j in range(RING) if i + j > 0]
    peers = column + plane
    for dt in (-1, 1):
        for dz in (-1, 0, 1):
            peers.append(tile_dev(dt, dz))
    for dev in peers:
        pl.semaphore_signal(barrier, inc=1, device_id=dev, device_id_type=MESH)
    pl.semaphore_wait(barrier, len(peers))

    loads[0].wait()

    def halo(buf, pad, k):
        lo, hi = pad, pad + COLS
        own = slice(lo, hi)
        first, last = slice(lo, lo + pad), slice(hi - pad, hi)
        left, right = slice(0, lo), slice(hi, hi + pad)
        plan = [
            ((1, 2, own), (3, 4, own), (-1, 0)),
            ((2, 3, own), (0, 1, own), (1, 0)),
            ((1, 3, first), (1, 3, right), (0, -1)),
            ((1, 3, last), (1, 3, left), (0, 1)),
            ((1, 2, first), (3, 4, right), (-1, -1)),
            ((1, 2, last), (3, 4, left), (-1, 1)),
            ((2, 3, first), (0, 1, right), (1, -1)),
            ((2, 3, last), (0, 1, left), (1, 1)),
        ]
        copies = []
        for n, (s, d, (dt, dz)) in enumerate(plan):
            copies.append(
                copy_to(
                    buf.at[s[0] : s[1], s[2]], buf.at[d[0] : d[1], d[2]],
                    h_send.at[k, n], h_recv.at[k, n], tile_dev(dt, dz),
                )
            )
        return copies

    def moments(v):
        return jnp.concatenate(
            [jnp.sum(v, axis=0, keepdims=True), jnp.sum(v * v, axis=0, keepdims=True)], axis=0
        )

    def all_stats(k, local, after_first, after_second):
        total = local
        pending = []
        for stage, devices, after in ((0, column, after_first), (1, plane, after_second)):
            base = stage * len(column)
            ar_tx[k, stage] = total
            copies = [
                copy_to(ar_tx.at[k, stage], ar_rx.at[k, base + n], ar_send.at[k, base + n],
                        ar_recv.at[k, base + n], dev)
                for n, dev in enumerate(devices)
            ]
            for copy in copies:
                copy.start()
            after()
            for n, copy in enumerate(copies):
                copy.wait_recv()
                total = total + ar_rx[k, base + n]
            pending += copies
        for copy in pending:
            copy.wait_send()
        return total

    lane = lax.broadcasted_iota(jnp.int32, (8, C), 1)

    def affine(total, gain, shift):
        both = jnp.concatenate([total, jnp.zeros((6, C), F32)], axis=0)
        for d in (1, 2, 4, 8):
            up = pltpu.roll(both, C - d, 1)
            down = pltpu.roll(both, d, 1)
            both = both + jnp.where((lane & d) == 0, up, down)
        members = float(POS * TILES * RING * (C // GROUPS))
        mean = both[0:1] / members
        var = jnp.maximum(both[1:2] / members - mean * mean, 0.0)
        scale = lax.rsqrt(var + EPS) * gain
        return scale, shift - mean * scale

    def activate(buf, pad, width, scale, shift):
        col = lax.broadcasted_iota(jnp.int32, (width, 1), 0)
        edge = ((col >= pad) | (z > 0)) & ((col < pad + COLS) | (z < RING - 1))

        def one_row(r, _):
            inside = ((r > 0) | (t > 0)) & ((r < 3) | (t < TILES - 1))
            u = buf[r].astype(F32) * scale + shift
            u = u / (1.0 + jnp.exp(-u))
            tmp[0:width] = jnp.where(edge & inside, u, 0.0)
            for dj in range(3):
                act[dj, r] = tmp[pad - 1 + dj : pad - 1 + dj + COLS].astype(BF)
            return 0

        lax.fori_loop(0, 4, one_row, 0)

    def conv(weight):
        acc_c[...] = jnp.zeros_like(acc_c)

        def three_taps(di, _):
            part = None
            for dj in range(3):
                a = act[dj, pl.ds(di, 2)].reshape(POS, C)
                d = dot(a, weight[di * 3 + dj])
                part = d if part is None else part + d
            acc_c[...] += part
            return 0

        lax.fori_loop(0, 3, three_taps, 0)

    def vec(i):
        return vecs[i]

    halo0 = halo(ext, LPAD, 0)
    latent = ext[1:3, LPAD : LPAD + COLS].astype(F32).reshape(POS, C)

    def start_halo0():
        for copy in halo0:
            copy.start()

    total = all_stats(0, moments(latent), start_halo0, lambda: None)
    for copy in loads[1:12]:
        copy.wait()
    for copy in halo0:
        copy.wait_recv()
    scale, shift = affine(total, vec(0), vec(1))
    activate(ext, LPAD, COLS + 2 * LPAD, scale, shift)
    loads[12].wait()
    conv(w1)

    hid = acc_c[...] + vec(2)
    hext[1:3, HPAD : HPAD + COLS] = hid.reshape(ROWS, COLS, C)
    halo1 = halo(hext, HPAD, 1)

    def start_halo1():
        for copy in halo1:
            copy.start()

    total = all_stats(1, moments(hid), start_halo1, lambda: None)
    for copy in halo1:
        copy.wait_recv()
    scale, shift = affine(total, vec(3), vec(4))
    activate(hext, HPAD, COLS + 2 * HPAD, scale, shift)
    loads[13].wait()
    conv(w2)
    latent = ext[1:3, LPAD : LPAD + COLS].astype(F32).reshape(POS, C)
    res = (latent + (acc_c[...] + vec(5))).astype(BF)
    kv[0, 0] = res

    def half(n, h):
        return kv.at[n, 0, pl.ds(h * COLS, COLS)]

    def own_copy(axis, i, h, n):
        dev = (ring(x, i), y, c, z) if axis == "x" else (x, ring(y, i), c, z)
        back = RING - i
        there = slot_of(back, 0) if axis == "x" else slot_of(0, back)
        return copy_to(half(0, h), half(there, h), kv_send.at[n], kv_recv.at[there, h], dev)

    first_x = [own_copy("x", i, 0, k) for k, i in enumerate((1, 3, 2))]
    first_y = [own_copy("y", i, 1, 3 + k) for k, i in enumerate((1, 3, 2))]
    later_x = [own_copy("x", i, 1, 6 + k) for k, i in enumerate((1, 3, 2))]
    later_y = [own_copy("y", i, 0, 9 + k) for k, i in enumerate((1, 3, 2))]
    onward = []
    for dx, dy in FAR:
        there = slot_of(dx, dy)
        onward.append(
            copy_to(half(slot_of(dx, 0), 0), half(there, 0), kv_send.at[12 + len(onward)],
                    kv_recv.at[there, 0], (x, ring(y, RING - dy), c, z))
        )
        onward.append(
            copy_to(half(slot_of(0, dy), 1), half(there, 1), kv_send.at[12 + len(onward)],
                    kv_recv.at[there, 1], (ring(x, RING - dx), y, c, z))
        )
    to_z = [
        copy_to(kv.at[0, 0], qres.at[RING - 1 - i], q_send.at[i - 1], q_recv.at[RING - 1 - i],
                (x, y, c, ring(z, i)))
        for i in (1, 3, 2)
    ]
    pass_own = copy_to(kv.at[0, 0], kv.at[0, 1], d_send.at[0], d_recv.at[0], sibling)

    def begin(copies):
        for copy in copies:
            copy.start()

    res32 = res.astype(F32)
    total = all_stats(
        2,
        moments(res32),
        lambda: begin(to_z + first_x[:2] + first_y[:2] + [pass_own]),
        lambda: begin(first_x[2:] + first_y[2:] + later_x + later_y),
    )
    for k in range(1, RING):
        copy_to(half(0, 0), half(slot_of(k, 0), 0), kv_send.at[0], kv_recv.at[slot_of(k, 0), 0],
                sibling).wait_recv()
        copy_to(half(0, 1), half(slot_of(0, k), 1), kv_send.at[0], kv_recv.at[slot_of(0, k), 1],
                sibling).wait_recv()
    begin(onward)

    scale3, shift3 = affine(total, vec(6), vec(7))
    for copy in loads[14:]:
        copy.wait()
    qres[RING - 1] = res
    to_exp2 = scale3 * (1.4426950408889634 / C**0.5)
    for tile in (1, 0):
        for r in range(2 * tile, min(2 * tile + 2, RING - 1)):
            copy_to(kv.at[0, 0], qres.at[r], q_send.at[0], q_recv.at[r], sibling).wait_recv()
        both = qres[2 * tile : 2 * tile + 2].reshape(QT, C)
        normed = (both.astype(F32) * scale3 + shift3).astype(BF)
        q = (dot(normed, wp[0]) + vec(8)).astype(BF)
        qq[tile * QT : (tile + 1) * QT] = (dot(q, wp[1], NT) * to_exp2).astype(BF)

    def pass_on(n):
        return copy_to(kv.at[n, 0], kv.at[n, 1], d_send.at[n], d_recv.at[n], sibling)

    def wait_half(n, h):
        ref = kv.at[n, 0, pl.ds(h * COLS, COLS)]
        copy_to(ref, ref, kv_send.at[0], kv_recv.at[n, h], sibling).wait_recv()

    def keys(ck):
        return kv[pl.ds(2 * ck, 2)].reshape(KC, C)

    def score(qt, ck, s):
        s[...] = dot(qq[qt * QT : (qt + 1) * QT], keys(ck), NT)

    def soften(s, p, m, l, a):
        step = 32
        for r in range(0, QT, step):
            rows = slice(r, r + step)
            sc = s[rows]
            old = m[rows]
            new = jnp.maximum(old, jnp.max(sc, axis=1, keepdims=True))
            e = jnp.exp2(sc - jnp.concatenate([new] * (KC // 128), axis=1)).astype(BF)
            p[rows] = e
            factor = jnp.exp2(old - new)
            e32 = e.astype(F32)
            part = l[rows] * factor
            for j in range(KC // 128):
                part = part + e32[:, j * 128 : (j + 1) * 128]
            l[rows] = part
            m[rows] = new
            a[rows] = factor

    def weigh(p, acc, a, ck):
        factor = a[...]
        acc[...] = acc[...] * jnp.concatenate([factor] * 4, axis=1) + dot(p[...], keys(ck))

    acc, m, l = (acc0, acc1), (m0, m1), (l0, l1)
    s, p, a = (s0, s1), (p0, p1), (a0, a1)

    def arrived(n):
        if isinstance(n, int):
            if n < 4 or n > 6:
                wait_half(n, 1)
            if n > 3:
                wait_half(n, 0)
        pass_on(n).start()

    def ready(ck):
        for j in range(2):
            pass_on(2 * ck + j).wait_recv()

    def step(b, score_of, soft_of, weigh_of):
        if weigh_of is not None:
            tile, ck = weigh_of
            weigh(p[1 - b], acc[tile], a[1 - b], ck)
        if score_of is not None:
            score(*score_of, s[1 - b])
        if soft_of is not None:
            soften(s[b], p[b], m[soft_of], l[soft_of], a[b])

    for n in range(1, 4):
        arrived(n)
    pass_on(0).wait_recv()
    pass_on(1).wait_recv()
    score(0, 0, s0)

    def chunk(ck, _):
        first = 2 * ck + 4
        for n in (first, first + 1):
            wait_half(n, 0)

            @pl.when(n > 6)
            def _():
                wait_half(n, 1)

            pass_on(n).start()
        ready(ck + 1)
        step(0, (1, ck), 0, (1, jnp.maximum(ck - 1, 0)))
        step(1, (0, ck + 1), 1, (0, ck))
        return 0

    lax.fori_loop(0, 4, chunk, 0)
    arrived(12)
    arrived(13)
    ready(5)
    step(0, (0, 5), 0, (1, 3))
    arrived(14)
    arrived(15)
    ready(6)
    step(1, (0, 6), 0, (0, 4))
    ready(7)
    step(0, (0, 7), 0, (0, 5))
    step(1, (1, 4), 0, (0, 6))
    step(0, (1, 5), 1, (0, 7))
    def finish(r):
        rows = slice((r % 2) * POS, (r % 2 + 1) * POS)
        total_l = jnp.sum(l[r // 2][rows], axis=1, keepdims=True)
        ctx = acc[r // 2][rows] * (1.0 / total_l) * scale3 + shift3
        return ctx, m[r // 2][rows] + jnp.log2(total_l)

    sent = []

    def send(r):
        ctx, lse = finish(r)
        ctx_tx[r] = ctx.astype(BF)
        lse_tx[r] = lse.T[0:8]
        there = RING - 2 - r
        dev = (x, y, c, ring(z, r + 1))
        sent.append(copy_to(ctx_tx.at[r], ctx_rx.at[there], c_send.at[r], c_recv.at[there], dev))
        sent.append(copy_to(lse_tx.at[r], lse_rx.at[there], e_send.at[r], e_recv.at[there], dev))
        begin(sent[-2:])

    send(1)
    send(0)
    step(1, (1, 6), 1, (1, 4))
    step(0, (1, 7), 1, (1, 5))
    step(1, None, 1, (1, 6))
    step(0, None, None, (1, 7))
    send(2)
    ctx, lse = finish(RING - 1)
    for copy in sent:
        copy.wait_recv()
    others = [jnp.broadcast_to(lse_rx[r, 0:1], (128, POS)).T for r in range(RING - 1)]
    top = lse
    for o in others:
        top = jnp.maximum(top, o)
    weight = jnp.exp2(lse - top)
    norm = weight
    ctx = ctx * jnp.concatenate([weight] * 4, axis=1)
    for r, o in enumerate(others):
        w = jnp.exp2(o - top)
        norm = norm + w
        ctx = ctx + ctx_rx[r].astype(F32) * jnp.concatenate([w] * 4, axis=1)
    inv = 1.0 / norm
    ctx = (ctx * jnp.concatenate([inv] * 4, axis=1)).astype(BF)
    attended = (dot(ctx, wp[2]) + vec(9)).astype(BF)
    mixed = qres[RING - 1].astype(F32) + dot(attended, wp[3]) + vec(10)
    out_v[...] = mixed.astype(BF).reshape(ROWS, COLS, C)
    done = pltpu.make_async_copy(out_v, out_hbm, out_sem)
    done.start()
    for copy in halo0 + halo1 + first_x + first_y + later_x + later_y + onward + to_z + sent:
        copy.wait_send()
    for n in range(SLOTS):
        pass_on(n).wait_send()
    done.wait()


def per_device(latent, *params):
    row = lambda v: v.reshape(1, C)
    args = [latent]
    for p in params:
        args.append(row(p) if p.ndim == 1 else (p.reshape(9, C, C) if p.ndim == 4 else p))
    dma = pltpu.SemaphoreType.DMA
    v = pltpu.VMEM
    scratch = [
        v((11, 1, C), F32), v((9, C, C), BF), v((9, C, C), BF), v((4, C, C), BF),
        v((4, COLS + 2 * LPAD, C), BF), v((COLS + 2 * LPAD, C), F32), v((3, 4, COLS, C), BF),
        v((POS, C), F32), v((4, COLS + 2 * HPAD, C), F32),
        v((3, 2, 2, C), F32), v((3, 22, 2, C), F32),
        v((SLOTS, 2, POS, C), BF), v((RING, POS, C), BF), v((RING * POS, C), BF),
        v((QT, KC), F32), v((QT, KC), F32), v((QT, KC), BF), v((QT, KC), BF),
        v((QT, C), F32), v((QT, C), F32),
        v((QT, 128), F32), v((QT, 128), F32), v((QT, 128), F32), v((QT, 128), F32),
        v((QT, 128), F32), v((QT, 128), F32),
        v((3, POS, C), BF), v((3, 8, POS), F32), v((3, POS, C), BF), v((3, 8, POS), F32),
        v((ROWS, COLS, C), BF),
        dma((18,)), dma, dma((2, 8)), dma((2, 8)), dma((3, 22)), dma((3, 22)),
        dma((30,)), dma((SLOTS, 2)), dma((SLOTS,)), dma((SLOTS,)), dma((3,)), dma((3,)),
        dma((3,)), dma((3,)), dma((3,)), dma((3,)),
    ]
    return pl.pallas_call(
        block_kernel,
        out_shape=jax.ShapeDtypeStruct((ROWS, COLS, C), BF),
        in_specs=[pl.BlockSpec(memory_space=pl.ANY)] * 18,
        out_specs=pl.BlockSpec(memory_space=pl.ANY),
        scratch_shapes=scratch,
        compiler_params=pltpu.CompilerParams(
            collective_id=0, has_side_effects=True, vmem_limit_bytes=60 * 1024 * 1024
        ),
    )(*args)


def solution(mesh):
    finer = Mesh(mesh.devices.reshape(4, 4, 2, mesh.shape["head"]), AXES)
    return jax.shard_map(
        per_device,
        mesh=finer,
        in_specs=(P(TILE, "head", None),) + (P(),) * 17,
        out_specs=P(TILE, "head", None),
        check_vma=False,
    )
```

```python
import functools

import jax
import jax.numpy as jnp
from jax import lax
from jax.experimental import pallas as pl
from jax.experimental.pallas import tpu as pltpu
from jax.sharding import Mesh
from jax.sharding import PartitionSpec as P

C = 512
GROUPS = 32
AXES = ("tile_0", "tile_1", "tile_2", "head")
TILE = ("tile_0", "tile_1", "tile_2")
MESH = pl.DeviceIdType.MESH
BF = jnp.bfloat16
F32 = jnp.float32
EPS = 1e-06

ROWS, COLS = 2, 128
POS = ROWS * COLS
RING = 4
TILES = 32
SLOTS = 16
CHUNKS = 8
QT = 512
KC = 1024
LPAD = 16
HPAD = 8
NT = (((1,), (1,)), ((), ()))
NN = (((1,), (0,)), ((), ()))


ORDER = (
    (0, 0), (1, 0), (3, 0), (0, 1), (0, 3), (1, 1), (3, 3), (2, 0),
    (0, 2), (1, 3), (3, 1), (2, 1), (1, 2), (3, 2), (2, 3), (2, 2),
)


def slot_of(dx, dy):
    return ORDER.index((dx, dy))


def dot(a, b, dims=NN):
    return lax.dot_general(a, b, dims, preferred_element_type=F32)


def copy_to(src, dst, send, recv, dev):
    return pltpu.make_async_remote_copy(
        src_ref=src, dst_ref=dst, send_sem=send, recv_sem=recv, device_id=dev, device_id_type=MESH
    )


def block_kernel(*refs):
    hbm = refs[:18]
    out = refs[18]
    (
        vecs, w1, w2, wp, ext, tmp, act, acc_c, hext, ar_tx, ar_rx,
        kv, qres, qq, s0, s1, p0, p1, acc0, acc1, m0, m1, l0, l1, a0, a1,
        ctx_tx, lse_tx, ctx_rx, lse_rx,
        ld, h_send, h_recv, ar_send, ar_recv,
        kv_send, kv_recv, d_send, d_recv, q_send, q_recv, c_send, c_recv, e_send, e_recv,
    ) = refs[19:]
    x = lax.axis_index("tile_0")
    y = lax.axis_index("tile_1")
    c = lax.axis_index("tile_2")
    z = lax.axis_index("head")
    t = (x * RING + y) * 2 + c

    def ring(v, i):
        return lax.rem(v + i, RING)

    def tile_dev(dt, dz):
        n = lax.rem(t + dt + TILES, TILES)
        return (n // 8, lax.rem(n // 2, RING), lax.rem(n, 2), lax.rem(z + dz + RING, RING))

    sibling = (x, y, 1 - c, z)

    (lat, g1, b1, cw1, cb1, g2, b2, cw2, cb2, g3, b3, wq, bq, wk, wv, bv, wo, bo) = hbm
    loads = [pltpu.make_async_copy(lat, ext.at[1:3, LPAD : LPAD + COLS], ld.at[0])]
    for i, v in enumerate((g1, b1, cb1, g2, b2, cb2, g3, b3, bq, bv, bo)):
        loads.append(pltpu.make_async_copy(v, vecs.at[i], ld.at[1 + i]))
    loads.append(pltpu.make_async_copy(cw1, w1, ld.at[12]))
    loads.append(pltpu.make_async_copy(cw2, w2, ld.at[13]))
    for i, w in enumerate((wq, wk, wv, wo)):
        loads.append(pltpu.make_async_copy(w, wp.at[i], ld.at[14 + i]))
    for copy in loads:
        copy.start()

    for ref in (acc0, acc1, l0, l1):
        ref[...] = jnp.zeros_like(ref)
    for ref in (m0, m1):
        ref[...] = jnp.full_like(ref, -1e30)
    a1[...] = jnp.ones_like(a1)
    p1[...] = jnp.zeros_like(p1)

    barrier = pltpu.get_barrier_semaphore()
    column = [sibling]
    for i in (1, 3, 2):
        column += [(x, y, c, ring(z, i)), (x, y, 1 - c, ring(z, i))]
    plane = []
    for i in range(RING):
        plane += [(ring(x, i), ring(y, j), c, z) for j in range(RING) if i + j > 0]
    peers = column + plane
    for dt in (-1, 1):
        for dz in (-1, 0, 1):
            peers.append(tile_dev(dt, dz))
    for dev in peers:
        pl.semaphore_signal(barrier, inc=1, device_id=dev, device_id_type=MESH)
    pl.semaphore_wait(barrier, len(peers))

    loads[0].wait()

    def halo(buf, pad, k):
        lo, hi = pad, pad + COLS
        own = slice(lo, hi)
        first, last = slice(lo, lo + pad), slice(hi - pad, hi)
        left, right = slice(0, lo), slice(hi, hi + pad)
        plan = [
            ((1, 2, own), (3, 4, own), (-1, 0)),
            ((2, 3, own), (0, 1, own), (1, 0)),
            ((1, 3, first), (1, 3, right), (0, -1)),
            ((1, 3, last), (1, 3, left), (0, 1)),
            ((1, 2, first), (3, 4, right), (-1, -1)),
            ((1, 2, last), (3, 4, left), (-1, 1)),
            ((2, 3, first), (0, 1, right), (1, -1)),
            ((2, 3, last), (0, 1, left), (1, 1)),
        ]
        copies = []
        for n, (s, d, (dt, dz)) in enumerate(plan):
            copies.append(
                copy_to(
                    buf.at[s[0] : s[1], s[2]], buf.at[d[0] : d[1], d[2]],
                    h_send.at[k, n], h_recv.at[k, n], tile_dev(dt, dz),
                )
            )
        return copies

    def moments(v):
        return jnp.concatenate(
            [jnp.sum(v, axis=0, keepdims=True), jnp.sum(v * v, axis=0, keepdims=True)], axis=0
        )

    def all_stats(k, local, after_first, after_second):
        total = local
        pending = []
        for stage, devices, after in ((0, column, after_first), (1, plane, after_second)):
            base = stage * len(column)
            ar_tx[k, stage] = total
            copies = [
                copy_to(ar_tx.at[k, stage], ar_rx.at[k, base + n], ar_send.at[k, base + n],
                        ar_recv.at[k, base + n], dev)
                for n, dev in enumerate(devices)
            ]
            for copy in copies:
                copy.start()
            after()
            for n, copy in enumerate(copies):
                copy.wait_recv()
                total = total + ar_rx[k, base + n]
            pending += copies
        for copy in pending:
            copy.wait_send()
        return total

    lane = lax.broadcasted_iota(jnp.int32, (8, C), 1)

    def affine(total, gain, shift):
        both = jnp.concatenate([total, jnp.zeros((6, C), F32)], axis=0)
        for d in (1, 2, 4, 8):
            up = pltpu.roll(both, C - d, 1)
            down = pltpu.roll(both, d, 1)
            both = both + jnp.where((lane & d) == 0, up, down)
        members = float(POS * TILES * RING * (C // GROUPS))
        mean = both[0:1] / members
        var = jnp.maximum(both[1:2] / members - mean * mean, 0.0)
        scale = lax.rsqrt(var + EPS) * gain
        return scale, shift - mean * scale

    def activate(buf, pad, width, scale, shift):
        col = lax.broadcasted_iota(jnp.int32, (width, 1), 0)
        edge = ((col >= pad) | (z > 0)) & ((col < pad + COLS) | (z < RING - 1))

        def one_row(r, _):
            inside = ((r > 0) | (t > 0)) & ((r < 3) | (t < TILES - 1))
            u = buf[r].astype(F32) * scale + shift
            u = u / (1.0 + jnp.exp(-u))
            tmp[0:width] = jnp.where(edge & inside, u, 0.0)
            for dj in range(3):
                act[dj, r] = tmp[pad - 1 + dj : pad - 1 + dj + COLS].astype(BF)
            return 0

        lax.fori_loop(0, 4, one_row, 0)

    def conv(weight):
        acc_c[...] = jnp.zeros_like(acc_c)

        def three_taps(di, _):
            part = None
            for dj in range(3):
                a = act[dj, pl.ds(di, 2)].reshape(POS, C)
                d = dot(a, weight[di * 3 + dj])
                part = d if part is None else part + d
            acc_c[...] += part
            return 0

        lax.fori_loop(0, 3, three_taps, 0)

    def vec(i):
        return vecs[i]

    halo0 = halo(ext, LPAD, 0)
    latent = ext[1:3, LPAD : LPAD + COLS].astype(F32).reshape(POS, C)

    def start_halo0():
        for copy in halo0:
            copy.start()

    total = all_stats(0, moments(latent), start_halo0, lambda: None)
    for copy in loads[1:12]:
        copy.wait()
    for copy in halo0:
        copy.wait_recv()
    scale, shift = affine(total, vec(0), vec(1))
    activate(ext, LPAD, COLS + 2 * LPAD, scale, shift)
    loads[12].wait()
    conv(w1)

    hid = acc_c[...] + vec(2)
    hext[1:3, HPAD : HPAD + COLS] = hid.reshape(ROWS, COLS, C)
    halo1 = halo(hext, HPAD, 1)

    def start_halo1():
        for copy in halo1:
            copy.start()

    total = all_stats(1, moments(hid), start_halo1, lambda: None)
    for copy in halo1:
        copy.wait_recv()
    scale, shift = affine(total, vec(3), vec(4))
    activate(hext, HPAD, COLS + 2 * HPAD, scale, shift)
    loads[13].wait()
    conv(w2)
    latent = ext[1:3, LPAD : LPAD + COLS].astype(F32).reshape(POS, C)
    res = (latent + (acc_c[...] + vec(5))).astype(BF)
    kv[0, 0] = res

    def half(n, h):
        return kv.at[n, 0, pl.ds(h * COLS, COLS)]

    def own_copy(axis, i, h, n):
        dev = (ring(x, i), y, c, z) if axis == "x" else (x, ring(y, i), c, z)
        back = RING - i
        there = slot_of(back, 0) if axis == "x" else slot_of(0, back)
        return copy_to(half(0, h), half(there, h), kv_send.at[n], kv_recv.at[there, h], dev)

    first_x = [own_copy("x", i, 0, k) for k, i in enumerate((1, 3, 2))]
    first_y = [own_copy("y", i, 1, 3 + k) for k, i in enumerate((1, 3, 2))]
    later_x = [own_copy("x", i, 1, 6 + k) for k, i in enumerate((1, 3))]
    later_y = [own_copy("y", i, 0, 8 + k) for k, i in enumerate((1, 3))]
    moved = []

    def hand_on(axis, h, source, there):
        step = (source[0] - there[0], source[1] - there[1])
        dev = (ring(x, step[0] % RING), y, c, z) if axis == "x" else (x, ring(y, step[1] % RING), c, z)
        n = slot_of(*there)
        copy = copy_to(half(slot_of(*source), h), half(n, h), kv_send.at[10 + len(moved)],
                       kv_recv.at[n, h], dev)
        moved.append(copy)
        return copy

    onward = []
    for dx, dy in ORDER:
        if dx and dy:
            if dy != 2 or dx == 2:
                onward.append(hand_on("y", 0, (dx, 0), (dx, dy)))
            if dx != 2 or dy == 2:
                onward.append(hand_on("x", 1, (0, dy), (dx, dy)))
    relays = {
        (1, 0): [hand_on("x", 1, (1, 0), (2, 0))],
        (0, 1): [hand_on("y", 0, (0, 1), (0, 2))],
        (1, 1): [hand_on("y", 0, (1, 1), (1, 2)), hand_on("x", 1, (1, 1), (2, 1))],
        (3, 3): [hand_on("y", 0, (3, 3), (3, 2)), hand_on("x", 1, (3, 3), (2, 3))],
    }
    to_z = [
        copy_to(kv.at[0, 0], qres.at[RING - 1 - i], q_send.at[i - 1], q_recv.at[RING - 1 - i],
                (x, y, c, ring(z, i)))
        for i in (1, 3, 2)
    ]
    pass_own = copy_to(kv.at[0, 0], kv.at[0, 1], d_send.at[0], d_recv.at[0], sibling)

    def begin(copies):
        for copy in copies:
            copy.start()

    res32 = res.astype(F32)
    total = all_stats(
        2,
        moments(res32),
        lambda: begin(to_z + first_x[:2] + first_y[:2] + [pass_own]),
        lambda: begin(first_x[2:] + first_y[2:] + later_x + later_y),
    )
    for k in range(1, RING):
        copy_to(half(0, 0), half(slot_of(k, 0), 0), kv_send.at[0], kv_recv.at[slot_of(k, 0), 0],
                sibling).wait_recv()
        copy_to(half(0, 1), half(slot_of(0, k), 1), kv_send.at[0], kv_recv.at[slot_of(0, k), 1],
                sibling).wait_recv()
    begin(onward)

    def pass_on(n):
        return copy_to(kv.at[n, 0], kv.at[n, 1], d_send.at[n], d_recv.at[n], sibling)

    def wait_half(n, h):
        ref = kv.at[n, 0, pl.ds(h * COLS, COLS)]
        copy_to(ref, ref, kv_send.at[0], kv_recv.at[n, h], sibling).wait_recv()

    def arrived(n):
        dx, dy = ORDER[n]
        if dx:
            wait_half(n, 1)
        if dy:
            wait_half(n, 0)
        begin(relays.get((dx, dy), []))
        pass_on(n).start()

    def ready(ck):
        for j in range(2):
            pass_on(2 * ck + j).wait_recv()

    scale3, shift3 = affine(total, vec(6), vec(7))
    for copy in loads[14:]:
        copy.wait()
    qres[RING - 1] = res
    to_exp2 = scale3 * (1.4426950408889634 / C**0.5)
    for tile in (1, 0):
        for r in range(2 * tile, min(2 * tile + 2, RING - 1)):
            copy_to(kv.at[0, 0], qres.at[r], q_send.at[0], q_recv.at[r], sibling).wait_recv()
        both = qres[2 * tile : 2 * tile + 2].reshape(QT, C)
        normed = (both.astype(F32) * scale3 + shift3).astype(BF)
        q = (dot(normed, wp[0]) + vec(8)).astype(BF)
        qq[tile * QT : (tile + 1) * QT] = (dot(q, wp[1], NT) * to_exp2).astype(BF)
        if tile == 1:
            arrived(1)
            arrived(2)
            arrived(3)

    def keys(ck):
        return kv[pl.ds(2 * ck, 2)].reshape(KC, C)

    def score(qt, ck, s):
        s[...] = dot(qq[qt * QT : (qt + 1) * QT], keys(ck), NT)

    def soften(s, p, m, l, a):
        step = 32
        for r in range(0, QT, step):
            rows = slice(r, r + step)
            sc = s[rows]
            old = m[rows]
            new = jnp.maximum(old, jnp.max(sc, axis=1, keepdims=True))
            e = jnp.exp2(sc - jnp.concatenate([new] * (KC // 128), axis=1)).astype(BF)
            p[rows] = e
            factor = jnp.exp2(old - new)
            e32 = e.astype(F32)
            part = l[rows] * factor
            for j in range(KC // 128):
                part = part + e32[:, j * 128 : (j + 1) * 128]
            l[rows] = part
            m[rows] = new
            a[rows] = factor

    def weigh(p, acc, a, ck):
        factor = a[...]
        acc[...] = acc[...] * jnp.concatenate([factor] * 4, axis=1) + dot(p[...], keys(ck))

    def score_two(r, ck, s):
        for j in range(2):
            s[j * POS : (j + 1) * POS] = dot(qq[r * POS : (r + 1) * POS], keys(ck + j), NT)

    def soften_two(r, s, p, m, l, a):
        step, base = 16, (r % 2) * POS
        for i in range(0, POS, step):
            rows, at = slice(base + i, base + i + step), slice(i, i + step)
            low = slice(POS + i, POS + i + step)
            sc = jnp.concatenate([s[at], s[low]], axis=1)
            old = m[rows]
            new = jnp.maximum(old, jnp.max(sc, axis=1, keepdims=True))
            e = jnp.exp2(sc - jnp.concatenate([new] * (2 * KC // 128), axis=1)).astype(BF)
            p[at] = e[:, :KC]
            p[low] = e[:, KC:]
            factor = jnp.exp2(old - new)
            e32 = e.astype(F32)
            part = l[rows] * factor
            for j in range(2 * KC // 128):
                part = part + e32[:, j * 128 : (j + 1) * 128]
            l[rows] = part
            m[rows] = new
            a[at] = factor

    def weigh_two(r, p, acc, a, ck):
        rows = slice((r % 2) * POS, (r % 2 + 1) * POS)
        factor = jnp.concatenate([a[0:POS]] * 4, axis=1)
        acc[rows] = acc[rows] * factor + (
            dot(p[0:POS], keys(ck)) + dot(p[POS : 2 * POS], keys(ck + 1))
        )

    acc, m, l = (acc0, acc1), (m0, m1), (l0, l1)
    s, p, a = (s0, s1), (p0, p1), (a0, a1)

    def step(b, score_of, soft_of, weigh_of):
        if weigh_of is not None:
            tile, ck = weigh_of
            weigh(p[1 - b], acc[tile], a[1 - b], ck)
        if score_of is not None:
            score(*score_of, s[1 - b])
        if soft_of is not None:
            soften(s[b], p[b], m[soft_of], l[soft_of], a[b])

    arrived(4)
    ready(0)
    score(0, 0, s0)
    step(0, (1, 0), 0, None)
    arrived(5)
    arrived(6)
    ready(1)
    step(1, (0, 1), 1, (0, 0))
    arrived(7)
    arrived(8)
    ready(2)
    step(0, (1, 1), 0, (1, 0))
    step(1, (0, 2), 1, (0, 1))
    arrived(9)
    arrived(10)
    ready(3)
    step(0, (1, 2), 0, (1, 1))
    step(1, (0, 3), 1, (0, 2))
    arrived(11)
    arrived(12)
    step(0, (1, 3), 0, (1, 2))
    arrived(13)
    arrived(14)
    arrived(15)
    ready(4)
    ready(5)
    step(1, None, 1, (0, 3))
    score_two(1, 4, s0)
    ready(6)
    ready(7)
    def finish(r):
        rows = slice((r % 2) * POS, (r % 2 + 1) * POS)
        total_l = jnp.sum(l[r // 2][rows], axis=1, keepdims=True)
        ctx = acc[r // 2][rows] * (1.0 / total_l) * scale3 + shift3
        return ctx, m[r // 2][rows] + jnp.log2(total_l)

    sent = []

    def send(r):
        ctx, lse = finish(r)
        ctx_tx[r] = ctx.astype(BF)
        lse_tx[r] = lse.T[0:8]
        there = RING - 2 - r
        dev = (x, y, c, ring(z, r + 1))
        sent.append(copy_to(ctx_tx.at[r], ctx_rx.at[there], c_send.at[r], c_recv.at[there], dev))
        sent.append(copy_to(lse_tx.at[r], lse_rx.at[there], e_send.at[r], e_recv.at[there], dev))
        begin(sent[-2:])

    units = [(r, ck) for r in (1, 0, 2, 3) for ck in (4, 6)]
    for u, (r, ck) in enumerate(units):
        b = u % 2
        if u == 0:
            weigh(p1, acc1, a1, 3)
        else:
            last, at = units[u - 1]
            weigh_two(last, p[1 - b], acc[last // 2], a[1 - b], at)
        if u + 1 < len(units):
            score_two(*units[u + 1], s[1 - b])
        soften_two(r, s[b], p[b], m[r // 2], l[r // 2], a[b])
        if u in (2, 4, 6):
            send(units[u - 1][0])
    weigh_two(RING - 1, p1, acc1, a1, 6)
    ctx, lse = finish(RING - 1)
    for copy in sent:
        copy.wait_recv()
    others = [jnp.broadcast_to(lse_rx[r, 0:1], (128, POS)).T for r in range(RING - 1)]
    top = lse
    for o in others:
        top = jnp.maximum(top, o)
    weight = jnp.exp2(lse - top)
    norm = weight
    ctx = ctx * jnp.concatenate([weight] * 4, axis=1)
    for r, o in enumerate(others):
        w = jnp.exp2(o - top)
        norm = norm + w
        ctx = ctx + ctx_rx[r].astype(F32) * jnp.concatenate([w] * 4, axis=1)
    inv = 1.0 / norm
    ctx = (ctx * jnp.concatenate([inv] * 4, axis=1)).astype(BF)
    attended = (dot(ctx, wp[2]) + vec(9)).astype(BF)
    mixed = qres[RING - 1].astype(F32) + dot(attended, wp[3]) + vec(10)
    out[...] = mixed.astype(BF).reshape(ROWS, COLS, C)
    for copy in halo0 + halo1 + first_x + first_y + later_x + later_y + moved + to_z + sent:
        copy.wait_send()
    for n in range(SLOTS):
        pass_on(n).wait_send()


def per_device(latent, *params):
    row = lambda v: v.reshape(1, C)
    args = [latent]
    for p in params:
        args.append(row(p) if p.ndim == 1 else (p.reshape(9, C, C) if p.ndim == 4 else p))
    dma = pltpu.SemaphoreType.DMA
    v = pltpu.VMEM
    scratch = [
        v((11, 1, C), F32), v((9, C, C), BF), v((9, C, C), BF), v((4, C, C), BF),
        v((4, COLS + 2 * LPAD, C), BF), v((COLS + 2 * LPAD, C), F32), v((3, 4, COLS, C), BF),
        v((POS, C), F32), v((4, COLS + 2 * HPAD, C), F32),
        v((3, 2, 2, C), F32), v((3, 22, 2, C), F32),
        v((SLOTS, 2, POS, C), BF), v((RING, POS, C), BF), v((RING * POS, C), BF),
        v((QT, KC), F32), v((QT, KC), F32), v((QT, KC), BF), v((QT, KC), BF),
        v((QT, C), F32), v((QT, C), F32),
        v((QT, 128), F32), v((QT, 128), F32), v((QT, 128), F32), v((QT, 128), F32),
        v((QT, 128), F32), v((QT, 128), F32),
        v((3, POS, C), BF), v((3, 8, POS), F32), v((3, POS, C), BF), v((3, 8, POS), F32),
        dma((18,)), dma((2, 8)), dma((2, 8)), dma((3, 22)), dma((3, 22)),
        dma((30,)), dma((SLOTS, 2)), dma((SLOTS,)), dma((SLOTS,)), dma((3,)), dma((3,)),
        dma((3,)), dma((3,)), dma((3,)), dma((3,)),
    ]
    return pl.pallas_call(
        block_kernel,
        out_shape=jax.ShapeDtypeStruct((ROWS, COLS, C), BF),
        in_specs=[pl.BlockSpec(memory_space=pl.ANY)] * 18,
        out_specs=pl.BlockSpec(memory_space=pltpu.VMEM),
        scratch_shapes=scratch,
        compiler_params=pltpu.CompilerParams(
            collective_id=0, has_side_effects=True, vmem_limit_bytes=60 * 1024 * 1024
        ),
    )(*args)


def solution(mesh):
    finer = Mesh(mesh.devices.reshape(4, 4, 2, mesh.shape["head"]), AXES)
    return jax.shard_map(
        per_device,
        mesh=finer,
        in_specs=(P(TILE, "head", None),) + (P(),) * 17,
        out_specs=P(TILE, "head", None),
        check_vma=False,
    )
```

```python
import functools

import jax
import jax.numpy as jnp
from jax import lax
from jax.experimental import pallas as pl
from jax.experimental.pallas import tpu as pltpu
from jax.sharding import Mesh
from jax.sharding import PartitionSpec as P

C = 512
GROUPS = 32
AXES = ("tile_0", "tile_1", "tile_2", "head")
TILE = ("tile_0", "tile_1", "tile_2")
MESH = pl.DeviceIdType.MESH
BF = jnp.bfloat16
F32 = jnp.float32
EPS = 1e-06

ROWS, COLS = 2, 128
POS = ROWS * COLS
RING = 4
TILES = 32
SLOTS = 16
CHUNKS = 8
QT = 512
KC = 1024
LPAD = 16
HPAD = 8
NT = (((1,), (1,)), ((), ()))
NN = (((1,), (0,)), ((), ()))


ORDER = (
    (0, 0), (1, 0), (3, 0), (0, 1), (0, 3), (1, 1), (3, 3), (1, 3),
    (3, 1), (2, 0), (0, 2), (2, 2), (1, 2), (2, 1), (3, 2), (2, 3),
)
OWNER = (1, 3, 2, 0)


def slot_of(dx, dy):
    return ORDER.index((dx, dy))


def dot(a, b, dims=NN):
    return lax.dot_general(a, b, dims, preferred_element_type=F32)


def copy_to(src, dst, send, recv, dev):
    return pltpu.make_async_remote_copy(
        src_ref=src, dst_ref=dst, send_sem=send, recv_sem=recv, device_id=dev, device_id_type=MESH
    )


def block_kernel(*refs):
    hbm = refs[:18]
    out = refs[18]
    (
        vecs, w1, w2, wp, ext, tmp, act, acc_c, hext, ar_tx, ar_rx,
        kv, qres, qq, s0, s1, p0, p1, acc0, acc1, m0, m1, l0, l1, a0, a1,
        ctx_tx, lse_tx, ctx_rx, lse_rx,
        ld, h_send, h_recv, ar_send, ar_recv,
        kv_send, kv_recv, d_send, d_recv, q_send, q_recv, c_send, c_recv, e_send, e_recv,
    ) = refs[19:]
    x = lax.axis_index("tile_0")
    y = lax.axis_index("tile_1")
    c = lax.axis_index("tile_2")
    z = lax.axis_index("head")
    t = (x * RING + y) * 2 + c

    def ring(v, i):
        return lax.rem(v + i, RING)

    def tile_dev(dt, dz):
        n = lax.rem(t + dt + TILES, TILES)
        return (n // 8, lax.rem(n // 2, RING), lax.rem(n, 2), lax.rem(z + dz + RING, RING))

    sibling = (x, y, 1 - c, z)

    (lat, g1, b1, cw1, cb1, g2, b2, cw2, cb2, g3, b3, wq, bq, wk, wv, bv, wo, bo) = hbm
    loads = [pltpu.make_async_copy(lat, ext.at[1:3, LPAD : LPAD + COLS], ld.at[0])]
    for i, v in enumerate((g1, b1, cb1, g2, b2, cb2, g3, b3, bq, bv, bo)):
        loads.append(pltpu.make_async_copy(v, vecs.at[i], ld.at[1 + i]))
    loads.append(pltpu.make_async_copy(cw1, w1, ld.at[12]))
    loads.append(pltpu.make_async_copy(cw2, w2, ld.at[13]))
    for i, w in enumerate((wq, wk, wv, wo)):
        loads.append(pltpu.make_async_copy(w, wp.at[i], ld.at[14 + i]))
    for copy in loads:
        copy.start()

    for ref in (acc0, acc1, l0, l1):
        ref[...] = jnp.zeros_like(ref)
    for ref in (m0, m1):
        ref[...] = jnp.full_like(ref, -1e30)
    a1[...] = jnp.ones_like(a1)
    p1[...] = jnp.zeros_like(p1)

    barrier = pltpu.get_barrier_semaphore()
    column = [sibling]
    for i in (1, 3, 2):
        column += [(x, y, c, ring(z, i)), (x, y, 1 - c, ring(z, i))]
    plane = []
    for i in range(RING):
        plane += [(ring(x, i), ring(y, j), c, z) for j in range(RING) if i + j > 0]
    peers = column + plane
    for dt in (-1, 1):
        for dz in (-1, 0, 1):
            peers.append(tile_dev(dt, dz))
    for dev in peers:
        pl.semaphore_signal(barrier, inc=1, device_id=dev, device_id_type=MESH)
    pl.semaphore_wait(barrier, len(peers))

    loads[0].wait()

    def halo(buf, pad, k):
        lo, hi = pad, pad + COLS
        own = slice(lo, hi)
        first, last = slice(lo, lo + pad), slice(hi - pad, hi)
        left, right = slice(0, lo), slice(hi, hi + pad)
        plan = [
            ((1, 2, own), (3, 4, own), (-1, 0)),
            ((2, 3, own), (0, 1, own), (1, 0)),
            ((1, 3, first), (1, 3, right), (0, -1)),
            ((1, 3, last), (1, 3, left), (0, 1)),
            ((1, 2, first), (3, 4, right), (-1, -1)),
            ((1, 2, last), (3, 4, left), (-1, 1)),
            ((2, 3, first), (0, 1, right), (1, -1)),
            ((2, 3, last), (0, 1, left), (1, 1)),
        ]
        copies = []
        for n, (s, d, (dt, dz)) in enumerate(plan):
            copies.append(
                copy_to(
                    buf.at[s[0] : s[1], s[2]], buf.at[d[0] : d[1], d[2]],
                    h_send.at[k, n], h_recv.at[k, n], tile_dev(dt, dz),
                )
            )
        return copies

    def moments(v):
        return jnp.concatenate(
            [jnp.sum(v, axis=0, keepdims=True), jnp.sum(v * v, axis=0, keepdims=True)], axis=0
        )

    def all_stats(k, local, after_first, after_second, plane_first=False):
        total = local
        pending = []
        stages = [(0, column), (len(column), plane)]
        if plane_first:
            stages.reverse()
        for stage, ((base, devices), after) in enumerate(zip(stages, (after_first, after_second))):
            ar_tx[k, stage] = total
            copies = [
                copy_to(ar_tx.at[k, stage], ar_rx.at[k, base + n], ar_send.at[k, base + n],
                        ar_recv.at[k, base + n], dev)
                for n, dev in enumerate(devices)
            ]
            for copy in copies:
                copy.start()
            after()
            for n, copy in enumerate(copies):
                copy.wait_recv()
                total = total + ar_rx[k, base + n]
            pending += copies
        for copy in pending:
            copy.wait_send()
        return total

    lane = lax.broadcasted_iota(jnp.int32, (8, C), 1)

    def affine(total, gain, shift):
        both = jnp.concatenate([total, jnp.zeros((6, C), F32)], axis=0)
        for d in (1, 2, 4, 8):
            up = pltpu.roll(both, C - d, 1)
            down = pltpu.roll(both, d, 1)
            both = both + jnp.where((lane & d) == 0, up, down)
        members = float(POS * TILES * RING * (C // GROUPS))
        mean = both[0:1] / members
        var = jnp.maximum(both[1:2] / members - mean * mean, 0.0)
        scale = lax.rsqrt(var + EPS) * gain
        return scale, shift - mean * scale

    def activate(buf, pad, width, scale, shift):
        col = lax.broadcasted_iota(jnp.int32, (width, 1), 0)
        edge = ((col >= pad) | (z > 0)) & ((col < pad + COLS) | (z < RING - 1))

        def one_row(r, _):
            inside = ((r > 0) | (t > 0)) & ((r < 3) | (t < TILES - 1))
            u = buf[r].astype(F32) * scale + shift
            u = u / (1.0 + jnp.exp(-u))
            tmp[0:width] = jnp.where(edge & inside, u, 0.0)
            for dj in range(3):
                act[dj, r] = tmp[pad - 1 + dj : pad - 1 + dj + COLS].astype(BF)
            return 0

        lax.fori_loop(0, 4, one_row, 0)

    def conv(weight):
        acc_c[...] = jnp.zeros_like(acc_c)

        def three_taps(di, _):
            part = None
            for dj in range(3):
                a = act[dj, pl.ds(di, 2)].reshape(POS, C)
                d = dot(a, weight[di * 3 + dj])
                part = d if part is None else part + d
            acc_c[...] += part
            return 0

        lax.fori_loop(0, 3, three_taps, 0)

    def vec(i):
        return vecs[i]

    halo0 = halo(ext, LPAD, 0)
    latent = ext[1:3, LPAD : LPAD + COLS].astype(F32).reshape(POS, C)

    def start_halo0():
        for copy in halo0:
            copy.start()

    total = all_stats(0, moments(latent), start_halo0, lambda: None)
    for copy in loads[1:12]:
        copy.wait()
    for copy in halo0:
        copy.wait_recv()
    scale, shift = affine(total, vec(0), vec(1))
    activate(ext, LPAD, COLS + 2 * LPAD, scale, shift)
    loads[12].wait()
    conv(w1)

    hid = acc_c[...] + vec(2)
    hext[1:3, HPAD : HPAD + COLS] = hid.reshape(ROWS, COLS, C)
    halo1 = halo(hext, HPAD, 1)

    def start_halo1():
        for copy in halo1:
            copy.start()

    total = all_stats(1, moments(hid), start_halo1, lambda: None)
    for copy in halo1:
        copy.wait_recv()
    scale, shift = affine(total, vec(3), vec(4))
    activate(hext, HPAD, COLS + 2 * HPAD, scale, shift)
    loads[13].wait()
    conv(w2)
    latent = ext[1:3, LPAD : LPAD + COLS].astype(F32).reshape(POS, C)
    res = (latent + (acc_c[...] + vec(5))).astype(BF)
    kv[0, 0] = res

    def half(n, h):
        return kv.at[n, 0, pl.ds(h * COLS, COLS)]

    def own_copy(axis, i, h, n):
        dev = (ring(x, i), y, c, z) if axis == "x" else (x, ring(y, i), c, z)
        back = RING - i
        there = slot_of(back, 0) if axis == "x" else slot_of(0, back)
        return copy_to(half(0, h), half(there, h), kv_send.at[n], kv_recv.at[there, h], dev)

    first_x = [own_copy("x", i, 0, k) for k, i in enumerate((1, 3, 2))]
    first_y = [own_copy("y", i, 1, 3 + k) for k, i in enumerate((1, 3, 2))]
    later_x = [own_copy("x", i, 1, 6 + k) for k, i in enumerate((1, 3))]
    later_y = [own_copy("y", i, 0, 8 + k) for k, i in enumerate((1, 3))]
    moved = []

    def hand_on(axis, h, source, there):
        step = (source[0] - there[0], source[1] - there[1])
        dev = (ring(x, step[0] % RING), y, c, z) if axis == "x" else (x, ring(y, step[1] % RING), c, z)
        n = slot_of(*there)
        copy = copy_to(half(slot_of(*source), h), half(n, h), kv_send.at[10 + len(moved)],
                       kv_recv.at[n, h], dev)
        moved.append(copy)
        return copy

    onward = [
        copy
        for far in ((1, 1), (3, 3), (1, 3), (3, 1))
        for copy in (hand_on("y", 0, (far[0], 0), far), hand_on("x", 1, (0, far[1]), far))
    ]
    onward_two = [hand_on("y", 0, (2, 0), (2, 2)), hand_on("x", 1, (0, 2), (2, 2))]
    for k in (1, 3):
        onward_two.append(hand_on("y", 0, (2, 0), (2, k)))
        onward_two.append(hand_on("x", 1, (0, 2), (k, 2)))
    relays = {
        (1, 0): [hand_on("x", 1, (1, 0), (2, 0))],
        (0, 1): [hand_on("y", 0, (0, 1), (0, 2))],
        (1, 1): [hand_on("y", 0, (1, 1), (1, 2)), hand_on("x", 1, (1, 1), (2, 1))],
        (3, 3): [hand_on("y", 0, (3, 3), (3, 2)), hand_on("x", 1, (3, 3), (2, 3))],
    }
    to_z = []
    for i in (1, 3, 2):
        place = OWNER.index(RING - i)
        to_z.append(copy_to(kv.at[0, 0], qres.at[place], q_send.at[i - 1], q_recv.at[place],
                            (x, y, c, ring(z, i))))
    pass_own = copy_to(kv.at[0, 0], kv.at[0, 1], d_send.at[0], d_recv.at[0], sibling)

    def begin(copies):
        for copy in copies:
            copy.start()

    def far_half(n, h):
        return copy_to(half(0, h), half(n, h), kv_send.at[0], kv_recv.at[n, h], sibling)

    def forward():
        begin([pass_own] + to_z[2:])
        for k in (1, 3):
            far_half(slot_of(k, 0), 0).wait_recv()
            far_half(slot_of(0, k), 1).wait_recv()
        begin(onward)

    res32 = res.astype(F32)
    total = all_stats(
        2,
        moments(res32),
        lambda: begin(first_x + first_y + later_x + later_y + to_z[:2]),
        forward,
        plane_first=True,
    )
    def pass_on(n):
        return copy_to(kv.at[n, 0], kv.at[n, 1], d_send.at[n], d_recv.at[n], sibling)

    def wait_half(n, h):
        ref = kv.at[n, 0, pl.ds(h * COLS, COLS)]
        copy_to(ref, ref, kv_send.at[0], kv_recv.at[n, h], sibling).wait_recv()

    def arrived(n):
        dx, dy = ORDER[n]
        if dx:
            wait_half(n, 1)
        if dy:
            wait_half(n, 0)
        begin(relays.get((dx, dy), []))
        pass_on(n).start()

    def ready(ck):
        for j in range(2):
            pass_on(2 * ck + j).wait_recv()

    for n in range(1, 5):
        arrived(n)
    far_half(slot_of(2, 0), 0).wait_recv()
    far_half(slot_of(0, 2), 1).wait_recv()
    begin(onward_two)

    scale3, shift3 = affine(total, vec(6), vec(7))
    for copy in loads[14:]:
        copy.wait()
    qres[RING - 1] = res
    to_exp2 = scale3 * (1.4426950408889634 / C**0.5)

    def queries(tile):
        for r in range(2 * tile, min(2 * tile + 2, RING - 1)):
            copy_to(kv.at[0, 0], qres.at[r], q_send.at[0], q_recv.at[r], sibling).wait_recv()
        both = qres[2 * tile : 2 * tile + 2].reshape(QT, C)
        normed = (both.astype(F32) * scale3 + shift3).astype(BF)
        q = (dot(normed, wp[0]) + vec(8)).astype(BF)
        qq[tile * QT : (tile + 1) * QT] = (dot(q, wp[1], NT) * to_exp2).astype(BF)

    queries(0)

    def keys(ck):
        return kv[pl.ds(2 * ck, 2)].reshape(KC, C)

    def score(qt, ck, s):
        s[...] = dot(qq[qt * QT : (qt + 1) * QT], keys(ck), NT)

    def soften(s, p, m, l, a):
        step = 32
        for r in range(0, QT, step):
            rows = slice(r, r + step)
            sc = s[rows]
            old = m[rows]
            new = jnp.maximum(old, jnp.max(sc, axis=1, keepdims=True))
            e = jnp.exp2(sc - jnp.concatenate([new] * (KC // 128), axis=1)).astype(BF)
            p[rows] = e
            factor = jnp.exp2(old - new)
            e32 = e.astype(F32)
            part = l[rows] * factor
            for j in range(KC // 128):
                part = part + e32[:, j * 128 : (j + 1) * 128]
            l[rows] = part
            m[rows] = new
            a[rows] = factor

    def weigh(p, acc, a, ck):
        factor = a[...]
        acc[...] = acc[...] * jnp.concatenate([factor] * 4, axis=1) + dot(p[...], keys(ck))

    def score_two(r, ck, s):
        for j in range(2):
            s[j * POS : (j + 1) * POS] = dot(qq[r * POS : (r + 1) * POS], keys(ck + j), NT)

    def soften_two(r, s, p, m, l, a):
        step, base = 16, (r % 2) * POS
        for i in range(0, POS, step):
            rows, at = slice(base + i, base + i + step), slice(i, i + step)
            low = slice(POS + i, POS + i + step)
            sc = jnp.concatenate([s[at], s[low]], axis=1)
            old = m[rows]
            new = jnp.maximum(old, jnp.max(sc, axis=1, keepdims=True))
            e = jnp.exp2(sc - jnp.concatenate([new] * (2 * KC // 128), axis=1)).astype(BF)
            p[at] = e[:, :KC]
            p[low] = e[:, KC:]
            factor = jnp.exp2(old - new)
            e32 = e.astype(F32)
            part = l[rows] * factor
            for j in range(2 * KC // 128):
                part = part + e32[:, j * 128 : (j + 1) * 128]
            l[rows] = part
            m[rows] = new
            a[at] = factor

    def weigh_two(r, p, acc, a, ck):
        rows = slice((r % 2) * POS, (r % 2 + 1) * POS)
        factor = jnp.concatenate([a[0:POS]] * 4, axis=1)
        acc[rows] = acc[rows] * factor + (
            dot(p[0:POS], keys(ck)) + dot(p[POS : 2 * POS], keys(ck + 1))
        )

    def score_two(r, ck, s):
        for j in range(2):
            s[j * POS : (j + 1) * POS] = dot(qq[r * POS : (r + 1) * POS], keys(ck + j), NT)

    def soften_two(r, s, p, m, l, a):
        step, base = 16, (r % 2) * POS
        for i in range(0, POS, step):
            rows, at = slice(base + i, base + i + step), slice(i, i + step)
            low = slice(POS + i, POS + i + step)
            sc = jnp.concatenate([s[at], s[low]], axis=1)
            old = m[rows]
            new = jnp.maximum(old, jnp.max(sc, axis=1, keepdims=True))
            e = jnp.exp2(sc - jnp.concatenate([new] * (2 * KC // 128), axis=1)).astype(BF)
            p[at] = e[:, :KC]
            p[low] = e[:, KC:]
            factor = jnp.exp2(old - new)
            e32 = e.astype(F32)
            part = l[rows] * factor
            for j in range(2 * KC // 128):
                part = part + e32[:, j * 128 : (j + 1) * 128]
            l[rows] = part
            m[rows] = new
            a[at] = factor

    def weigh_two(r, p, acc, a, ck):
        rows = slice((r % 2) * POS, (r % 2 + 1) * POS)
        factor = jnp.concatenate([a[0:POS]] * 4, axis=1)
        acc[rows] = acc[rows] * factor + (
            dot(p[0:POS], keys(ck)) + dot(p[POS : 2 * POS], keys(ck + 1))
        )

    acc, m, l = (acc0, acc1), (m0, m1), (l0, l1)
    s, p, a = (s0, s1), (p0, p1), (a0, a1)

    def finish(r):
        rows = slice((r % 2) * POS, (r % 2 + 1) * POS)
        total_l = jnp.sum(l[r // 2][rows], axis=1, keepdims=True)
        ctx = acc[r // 2][rows] * (1.0 / total_l) * scale3 + shift3
        return ctx, m[r // 2][rows] + jnp.log2(total_l)

    sent = []

    def send(r):
        ctx, lse = finish(r)
        ctx_tx[r] = ctx.astype(BF)
        lse_tx[r] = lse.T[0:8]
        there = OWNER.index(RING - OWNER[r])
        dev = (x, y, c, ring(z, OWNER[r]))
        sent.append(copy_to(ctx_tx.at[r], ctx_rx.at[there], c_send.at[r], c_recv.at[there], dev))
        sent.append(copy_to(lse_tx.at[r], lse_rx.at[there], e_send.at[r], e_recv.at[there], dev))
        begin(sent[-2:])

    T, Z, O = 0, 2, 3
    units = [
        (T, 0), (T, 1), (Z, 0), (T, 2), (T, 3), (Z, 2), (T, 4), (T, 5),
        (Z, 4), (O, 0), (T, 6), (Z, 6), (T, 7), (O, 2), (O, 4), (O, 6),
    ]

    def score_unit(u):
        kind, ck = units[u]
        score(0, ck, s[u % 2]) if kind == T else score_two(kind, ck, s[u % 2])

    def weigh_unit(u):
        kind, ck = units[u]
        b = u % 2
        if kind == T:
            weigh(p[b], acc0, a[b], ck)
        else:
            weigh_two(kind, p[b], acc1, a[b], ck)

    before = {
        0: lambda: (arrived(5), arrived(6), ready(1)),
        1: lambda: queries(1),
        2: lambda: (arrived(7), ready(2)),
        3: lambda: (arrived(8), ready(3)),
        4: lambda: arrived(9),
        5: lambda: (ready(4), arrived(10), arrived(11)),
        6: lambda: ready(5),
        8: lambda: (arrived(12), arrived(13)),
        9: lambda: (ready(6), arrived(14), arrived(15)),
        10: lambda: ready(7),
    }
    after = {12: lambda: send(2), 13: lambda: (send(0), send(1))}
    ready(0)
    score_unit(0)
    for u, (kind, ck) in enumerate(units):
        if u in before:
            before[u]()
        if u > 0:
            weigh_unit(u - 1)
        if u + 1 < len(units):
            score_unit(u + 1)
        b = u % 2
        if kind == T:
            soften(s[b], p[b], m0, l0, a[b])
        else:
            soften_two(kind, s[b], p[b], m1, l1, a[b])
        if u in after:
            after[u]()
    weigh_unit(len(units) - 1)
    ctx, lse = finish(RING - 1)
    for copy in sent:
        copy.wait_recv()
    others = [jnp.broadcast_to(lse_rx[r, 0:1], (128, POS)).T for r in range(RING - 1)]
    top = lse
    for o in others:
        top = jnp.maximum(top, o)
    weight = jnp.exp2(lse - top)
    norm = weight
    ctx = ctx * jnp.concatenate([weight] * 4, axis=1)
    for r, o in enumerate(others):
        w = jnp.exp2(o - top)
        norm = norm + w
        ctx = ctx + ctx_rx[r].astype(F32) * jnp.concatenate([w] * 4, axis=1)
    inv = 1.0 / norm
    ctx = (ctx * jnp.concatenate([inv] * 4, axis=1)).astype(BF)
    attended = (dot(ctx, wp[2]) + vec(9)).astype(BF)
    mixed = qres[RING - 1].astype(F32) + dot(attended, wp[3]) + vec(10)
    out[...] = mixed.astype(BF).reshape(ROWS, COLS, C)
    for copy in halo0 + halo1 + first_x + first_y + later_x + later_y + moved + to_z + sent:
        copy.wait_send()
    for n in range(SLOTS):
        pass_on(n).wait_send()


def per_device(latent, *params):
    row = lambda v: v.reshape(1, C)
    args = [latent]
    for p in params:
        args.append(row(p) if p.ndim == 1 else (p.reshape(9, C, C) if p.ndim == 4 else p))
    dma = pltpu.SemaphoreType.DMA
    v = pltpu.VMEM
    scratch = [
        v((11, 1, C), F32), v((9, C, C), BF), v((9, C, C), BF), v((4, C, C), BF),
        v((4, COLS + 2 * LPAD, C), BF), v((COLS + 2 * LPAD, C), F32), v((3, 4, COLS, C), BF),
        v((POS, C), F32), v((4, COLS + 2 * HPAD, C), F32),
        v((3, 2, 2, C), F32), v((3, 22, 2, C), F32),
        v((SLOTS, 2, POS, C), BF), v((RING, POS, C), BF), v((RING * POS, C), BF),
        v((QT, KC), F32), v((QT, KC), F32), v((QT, KC), BF), v((QT, KC), BF),
        v((QT, C), F32), v((QT, C), F32),
        v((QT, 128), F32), v((QT, 128), F32), v((QT, 128), F32), v((QT, 128), F32),
        v((QT, 128), F32), v((QT, 128), F32),
        v((3, POS, C), BF), v((3, 8, POS), F32), v((3, POS, C), BF), v((3, 8, POS), F32),
        dma((18,)), dma((2, 8)), dma((2, 8)), dma((3, 22)), dma((3, 22)),
        dma((30,)), dma((SLOTS, 2)), dma((SLOTS,)), dma((SLOTS,)), dma((3,)), dma((3,)),
        dma((3,)), dma((3,)), dma((3,)), dma((3,)),
    ]
    return pl.pallas_call(
        block_kernel,
        out_shape=jax.ShapeDtypeStruct((ROWS, COLS, C), BF),
        in_specs=[pl.BlockSpec(memory_space=pl.ANY)] * 18,
        out_specs=pl.BlockSpec(memory_space=pltpu.VMEM),
        scratch_shapes=scratch,
        compiler_params=pltpu.CompilerParams(
            collective_id=0, has_side_effects=True, vmem_limit_bytes=60 * 1024 * 1024
        ),
    )(*args)


def solution(mesh):
    finer = Mesh(mesh.devices.reshape(4, 4, 2, mesh.shape["head"]), AXES)
    return jax.shard_map(
        per_device,
        mesh=finer,
        in_specs=(P(TILE, "head", None),) + (P(),) * 17,
        out_specs=P(TILE, "head", None),
        check_vma=False,
    )
```

```python
import functools

import jax
import jax.numpy as jnp
from jax import lax
from jax.experimental import pallas as pl
from jax.experimental.pallas import tpu as pltpu
from jax.sharding import Mesh
from jax.sharding import PartitionSpec as P

C = 512
GROUPS = 32
AXES = ("tile_0", "tile_1", "tile_2", "head")
TILE = ("tile_0", "tile_1", "tile_2")
MESH = pl.DeviceIdType.MESH
BF = jnp.bfloat16
F32 = jnp.float32
EPS = 1e-06

ROWS, COLS = 2, 128
POS = ROWS * COLS
RING = 4
TILES = 32
SLOTS = 16
CHUNKS = 8
QT = 512
KC = 1024
LPAD = 16
HPAD = 8
NT = (((1,), (1,)), ((), ()))
NN = (((1,), (0,)), ((), ()))


ORDER = (
    (0, 0), (1, 0), (3, 0), (0, 1), (0, 3), (1, 1), (3, 3), (1, 3),
    (3, 1), (2, 0), (0, 2), (2, 2), (1, 2), (2, 1), (3, 2), (2, 3),
)
OWNER = (1, 3, 2, 0)


def slot_of(dx, dy):
    return ORDER.index((dx, dy))


def dot(a, b, dims=NN):
    return lax.dot_general(a, b, dims, preferred_element_type=F32)


def copy_to(src, dst, send, recv, dev):
    return pltpu.make_async_remote_copy(
        src_ref=src, dst_ref=dst, send_sem=send, recv_sem=recv, device_id=dev, device_id_type=MESH
    )


def block_kernel(*refs):
    hbm = refs[:18]
    out = refs[18]
    (
        vecs, w1, w2, wp, ext, tmp, act, acc_c, hext, ar_tx, ar_rx,
        kv, qres, qq, s0, s1, p0, p1, acc0, acc1, m0, m1, l0, l1, a0, a1,
        ctx_tx, lse_tx, ctx_rx, lse_rx, mrg_ctx, mrg_lse,
        ld, h_send, h_recv, ar_send, ar_recv,
        kv_send, kv_recv, d_send, d_recv, q_send, q_recv, c_send, c_recv, e_send, e_recv,
    ) = refs[19:]
    x = lax.axis_index("tile_0")
    y = lax.axis_index("tile_1")
    c = lax.axis_index("tile_2")
    z = lax.axis_index("head")
    t = (x * RING + y) * 2 + c

    def ring(v, i):
        return lax.rem(v + i, RING)

    def tile_dev(dt, dz):
        n = lax.rem(t + dt + TILES, TILES)
        return (n // 8, lax.rem(n // 2, RING), lax.rem(n, 2), lax.rem(z + dz + RING, RING))

    sibling = (x, y, 1 - c, z)

    (lat, g1, b1, cw1, cb1, g2, b2, cw2, cb2, g3, b3, wq, bq, wk, wv, bv, wo, bo) = hbm
    loads = [pltpu.make_async_copy(lat, ext.at[1:3, LPAD : LPAD + COLS], ld.at[0])]
    for i, v in enumerate((g1, b1, cb1, g2, b2, cb2, g3, b3, bq, bv, bo)):
        loads.append(pltpu.make_async_copy(v, vecs.at[i], ld.at[1 + i]))
    loads.append(pltpu.make_async_copy(cw1, w1, ld.at[12]))
    loads.append(pltpu.make_async_copy(cw2, w2, ld.at[13]))
    for i, w in enumerate((wq, wk, wv, wo)):
        loads.append(pltpu.make_async_copy(w, wp.at[i], ld.at[14 + i]))
    for copy in loads:
        copy.start()

    for ref in (acc0, acc1, l0, l1):
        ref[...] = jnp.zeros_like(ref)
    for ref in (m0, m1):
        ref[...] = jnp.full_like(ref, -1e30)
    a1[...] = jnp.ones_like(a1)
    p1[...] = jnp.zeros_like(p1)

    barrier = pltpu.get_barrier_semaphore()
    column = [sibling]
    for i in (1, 3, 2):
        column += [(x, y, c, ring(z, i)), (x, y, 1 - c, ring(z, i))]
    plane = []
    for i in range(RING):
        plane += [(ring(x, i), ring(y, j), c, z) for j in range(RING) if i + j > 0]
    peers = column + plane
    for dt in (-1, 1):
        for dz in (-1, 0, 1):
            peers.append(tile_dev(dt, dz))
    for dev in peers:
        pl.semaphore_signal(barrier, inc=1, device_id=dev, device_id_type=MESH)
    pl.semaphore_wait(barrier, len(peers))

    loads[0].wait()

    def halo(buf, pad, k):
        lo, hi = pad, pad + COLS
        own = slice(lo, hi)
        first, last = slice(lo, lo + pad), slice(hi - pad, hi)
        left, right = slice(0, lo), slice(hi, hi + pad)
        plan = [
            ((1, 2, own), (3, 4, own), (-1, 0)),
            ((2, 3, own), (0, 1, own), (1, 0)),
            ((1, 3, first), (1, 3, right), (0, -1)),
            ((1, 3, last), (1, 3, left), (0, 1)),
            ((1, 2, first), (3, 4, right), (-1, -1)),
            ((1, 2, last), (3, 4, left), (-1, 1)),
            ((2, 3, first), (0, 1, right), (1, -1)),
            ((2, 3, last), (0, 1, left), (1, 1)),
        ]
        copies = []
        for n, (s, d, (dt, dz)) in enumerate(plan):
            copies.append(
                copy_to(
                    buf.at[s[0] : s[1], s[2]], buf.at[d[0] : d[1], d[2]],
                    h_send.at[k, n], h_recv.at[k, n], tile_dev(dt, dz),
                )
            )
        return copies

    def moments(v):
        return jnp.concatenate(
            [jnp.sum(v, axis=0, keepdims=True), jnp.sum(v * v, axis=0, keepdims=True)], axis=0
        )

    def all_stats(k, local, after_first, after_second, plane_first=False):
        total = local
        pending = []
        stages = [(0, column), (len(column), plane)]
        if plane_first:
            stages.reverse()
        for stage, ((base, devices), after) in enumerate(zip(stages, (after_first, after_second))):
            ar_tx[k, stage] = total
            copies = [
                copy_to(ar_tx.at[k, stage], ar_rx.at[k, base + n], ar_send.at[k, base + n],
                        ar_recv.at[k, base + n], dev)
                for n, dev in enumerate(devices)
            ]
            for copy in copies:
                copy.start()
            after()
            for n, copy in enumerate(copies):
                copy.wait_recv()
                total = total + ar_rx[k, base + n]
            pending += copies
        for copy in pending:
            copy.wait_send()
        return total

    lane = lax.broadcasted_iota(jnp.int32, (8, C), 1)

    def affine(total, gain, shift):
        both = jnp.concatenate([total, jnp.zeros((6, C), F32)], axis=0)
        for d in (1, 2, 4, 8):
            up = pltpu.roll(both, C - d, 1)
            down = pltpu.roll(both, d, 1)
            both = both + jnp.where((lane & d) == 0, up, down)
        members = float(POS * TILES * RING * (C // GROUPS))
        mean = both[0:1] / members
        var = jnp.maximum(both[1:2] / members - mean * mean, 0.0)
        scale = lax.rsqrt(var + EPS) * gain
        return scale, shift - mean * scale

    def activate(buf, pad, width, scale, shift):
        col = lax.broadcasted_iota(jnp.int32, (width, 1), 0)
        edge = ((col >= pad) | (z > 0)) & ((col < pad + COLS) | (z < RING - 1))

        def one_row(r, _):
            inside = ((r > 0) | (t > 0)) & ((r < 3) | (t < TILES - 1))
            u = buf[r].astype(F32) * scale + shift
            u = u / (1.0 + jnp.exp(-u))
            tmp[0:width] = jnp.where(edge & inside, u, 0.0)
            for dj in range(3):
                act[dj, r] = tmp[pad - 1 + dj : pad - 1 + dj + COLS].astype(BF)
            return 0

        lax.fori_loop(0, 4, one_row, 0)

    def conv(weight):
        acc_c[...] = jnp.zeros_like(acc_c)

        def three_taps(di, _):
            part = None
            for dj in range(3):
                a = act[dj, pl.ds(di, 2)].reshape(POS, C)
                d = dot(a, weight[di * 3 + dj])
                part = d if part is None else part + d
            acc_c[...] += part
            return 0

        lax.fori_loop(0, 3, three_taps, 0)

    def vec(i):
        return vecs[i]

    halo0 = halo(ext, LPAD, 0)
    latent = ext[1:3, LPAD : LPAD + COLS].astype(F32).reshape(POS, C)

    def start_halo0():
        for copy in halo0:
            copy.start()

    total = all_stats(0, moments(latent), start_halo0, lambda: None)
    for copy in loads[1:12]:
        copy.wait()
    for copy in halo0:
        copy.wait_recv()
    scale, shift = affine(total, vec(0), vec(1))
    activate(ext, LPAD, COLS + 2 * LPAD, scale, shift)
    loads[12].wait()
    conv(w1)

    hid = acc_c[...] + vec(2)
    hext[1:3, HPAD : HPAD + COLS] = hid.reshape(ROWS, COLS, C)
    halo1 = halo(hext, HPAD, 1)

    def start_halo1():
        for copy in halo1:
            copy.start()

    total = all_stats(1, moments(hid), start_halo1, lambda: None)
    for copy in halo1:
        copy.wait_recv()
    scale, shift = affine(total, vec(3), vec(4))
    activate(hext, HPAD, COLS + 2 * HPAD, scale, shift)
    loads[13].wait()
    conv(w2)
    latent = ext[1:3, LPAD : LPAD + COLS].astype(F32).reshape(POS, C)
    res = (latent + (acc_c[...] + vec(5))).astype(BF)
    kv[0, 0] = res

    def half(n, h):
        return kv.at[n, 0, pl.ds(h * COLS, COLS)]

    def own_copy(axis, i, h, n):
        dev = (ring(x, i), y, c, z) if axis == "x" else (x, ring(y, i), c, z)
        back = RING - i
        there = slot_of(back, 0) if axis == "x" else slot_of(0, back)
        return copy_to(half(0, h), half(there, h), kv_send.at[n], kv_recv.at[there, h], dev)

    first_x = [own_copy("x", i, 0, k) for k, i in enumerate((1, 3, 2))]
    first_y = [own_copy("y", i, 1, 3 + k) for k, i in enumerate((1, 3, 2))]
    later_x = [own_copy("x", i, 1, 6 + k) for k, i in enumerate((1, 3))]
    later_y = [own_copy("y", i, 0, 8 + k) for k, i in enumerate((1, 3))]
    moved = []

    def hand_on(axis, h, source, there):
        step = (source[0] - there[0], source[1] - there[1])
        dev = (ring(x, step[0] % RING), y, c, z) if axis == "x" else (x, ring(y, step[1] % RING), c, z)
        n = slot_of(*there)
        copy = copy_to(half(slot_of(*source), h), half(n, h), kv_send.at[10 + len(moved)],
                       kv_recv.at[n, h], dev)
        moved.append(copy)
        return copy

    onward = [
        copy
        for far in ((1, 1), (3, 3), (1, 3), (3, 1))
        for copy in (hand_on("y", 0, (far[0], 0), far), hand_on("x", 1, (0, far[1]), far))
    ]
    onward_two = [hand_on("y", 0, (2, 0), (2, 2)), hand_on("x", 1, (0, 2), (2, 2))]
    for k in (1, 3):
        onward_two.append(hand_on("y", 0, (2, 0), (2, k)))
        onward_two.append(hand_on("x", 1, (0, 2), (k, 2)))
    relays = {
        (1, 0): [hand_on("x", 1, (1, 0), (2, 0))],
        (0, 1): [hand_on("y", 0, (0, 1), (0, 2))],
        (1, 1): [hand_on("y", 0, (1, 1), (1, 2)), hand_on("x", 1, (1, 1), (2, 1))],
        (3, 3): [hand_on("y", 0, (3, 3), (3, 2)), hand_on("x", 1, (3, 3), (2, 3))],
    }
    def to_column(i, h):
        place = OWNER.index(RING - i)
        rows = pl.ds(h * COLS, COLS)
        return copy_to(kv.at[0, 0, rows], qres.at[place, rows], q_send.at[place, h],
                       q_recv.at[place, h], (x, y, c, ring(z, i)))

    to_z = [to_column(i, h) for i, h in ((1, 0), (3, 0), (1, 1), (3, 1), (2, 0), (2, 1))]
    pass_own = copy_to(kv.at[0, 0], kv.at[0, 1], d_send.at[0], d_recv.at[0], sibling)

    def begin(copies):
        for copy in copies:
            copy.start()

    def far_half(n, h):
        return copy_to(half(0, h), half(n, h), kv_send.at[0], kv_recv.at[n, h], sibling)

    def forward():
        begin([pass_own] + to_z[2:])
        for k in (1, 3):
            far_half(slot_of(k, 0), 0).wait_recv()
            far_half(slot_of(0, k), 1).wait_recv()
        begin(onward)

    res32 = res.astype(F32)
    total = all_stats(
        2,
        moments(res32),
        lambda: begin(first_x[:2] + first_y[:2] + later_x + later_y + first_x[2:] + first_y[2:] + to_z[:2]),
        forward,
        plane_first=True,
    )
    def pass_on(n):
        return copy_to(kv.at[n, 0], kv.at[n, 1], d_send.at[n], d_recv.at[n], sibling)

    def wait_half(n, h):
        ref = kv.at[n, 0, pl.ds(h * COLS, COLS)]
        copy_to(ref, ref, kv_send.at[0], kv_recv.at[n, h], sibling).wait_recv()

    def arrived(n):
        dx, dy = ORDER[n]
        if dx:
            wait_half(n, 1)
        if dy:
            wait_half(n, 0)
        begin(relays.get((dx, dy), []))
        pass_on(n).start()

    def ready(ck):
        for j in range(2):
            pass_on(2 * ck + j).wait_recv()

    for n in range(1, 5):
        arrived(n)
    scale3, shift3 = affine(total, vec(6), vec(7))
    for copy in loads[14:]:
        copy.wait()
    qres[RING - 1] = res
    to_exp2 = scale3 * (1.4426950408889634 / C**0.5)

    def queries(tile):
        for r in range(2 * tile, min(2 * tile + 2, RING - 1)):
            for h in range(2):
                to_column(RING - OWNER[r], h).wait_recv()
        both = qres[2 * tile : 2 * tile + 2].reshape(QT, C)
        normed = (both.astype(F32) * scale3 + shift3).astype(BF)
        q = (dot(normed, wp[0]) + vec(8)).astype(BF)
        qq[tile * QT : (tile + 1) * QT] = (dot(q, wp[1], NT) * to_exp2).astype(BF)

    queries(0)
    far_half(slot_of(2, 0), 0).wait_recv()
    far_half(slot_of(0, 2), 1).wait_recv()
    begin(onward_two)

    def keys(ck):
        return kv[pl.ds(2 * ck, 2)].reshape(KC, C)

    def score(qt, ck, s):
        s[...] = dot(qq[qt * QT : (qt + 1) * QT], keys(ck), NT)

    def soften(s, p, m, l, a):
        step = 32
        for r in range(0, QT, step):
            rows = slice(r, r + step)
            sc = s[rows]
            old = m[rows]
            new = jnp.maximum(old, jnp.max(sc, axis=1, keepdims=True))
            e = jnp.exp2(sc - jnp.concatenate([new] * (KC // 128), axis=1)).astype(BF)
            p[rows] = e
            factor = jnp.exp2(old - new)
            e32 = e.astype(F32)
            part = l[rows] * factor
            for j in range(KC // 128):
                part = part + e32[:, j * 128 : (j + 1) * 128]
            l[rows] = part
            m[rows] = new
            a[rows] = factor

    def weigh(p, acc, a, ck):
        factor = a[...]
        acc[...] = acc[...] * jnp.concatenate([factor] * 4, axis=1) + dot(p[...], keys(ck))

    def score_two(r, ck, s):
        for j in range(2):
            s[j * POS : (j + 1) * POS] = dot(qq[r * POS : (r + 1) * POS], keys(ck + j), NT)

    def soften_two(r, s, p, m, l, a):
        step, base = 16, (r % 2) * POS
        for i in range(0, POS, step):
            rows, at = slice(base + i, base + i + step), slice(i, i + step)
            low = slice(POS + i, POS + i + step)
            sc = jnp.concatenate([s[at], s[low]], axis=1)
            old = m[rows]
            new = jnp.maximum(old, jnp.max(sc, axis=1, keepdims=True))
            e = jnp.exp2(sc - jnp.concatenate([new] * (2 * KC // 128), axis=1)).astype(BF)
            p[at] = e[:, :KC]
            p[low] = e[:, KC:]
            factor = jnp.exp2(old - new)
            e32 = e.astype(F32)
            part = l[rows] * factor
            for j in range(2 * KC // 128):
                part = part + e32[:, j * 128 : (j + 1) * 128]
            l[rows] = part
            m[rows] = new
            a[at] = factor

    def weigh_two(r, p, acc, a, ck):
        rows = slice((r % 2) * POS, (r % 2 + 1) * POS)
        factor = jnp.concatenate([a[0:POS]] * 4, axis=1)
        acc[rows] = acc[rows] * factor + (
            dot(p[0:POS], keys(ck)) + dot(p[POS : 2 * POS], keys(ck + 1))
        )

    def score_two(r, ck, s):
        for j in range(2):
            s[j * POS : (j + 1) * POS] = dot(qq[r * POS : (r + 1) * POS], keys(ck + j), NT)

    def soften_two(r, s, p, m, l, a):
        step, base = 16, (r % 2) * POS
        for i in range(0, POS, step):
            rows, at = slice(base + i, base + i + step), slice(i, i + step)
            low = slice(POS + i, POS + i + step)
            sc = jnp.concatenate([s[at], s[low]], axis=1)
            old = m[rows]
            new = jnp.maximum(old, jnp.max(sc, axis=1, keepdims=True))
            e = jnp.exp2(sc - jnp.concatenate([new] * (2 * KC // 128), axis=1)).astype(BF)
            p[at] = e[:, :KC]
            p[low] = e[:, KC:]
            factor = jnp.exp2(old - new)
            e32 = e.astype(F32)
            part = l[rows] * factor
            for j in range(2 * KC // 128):
                part = part + e32[:, j * 128 : (j + 1) * 128]
            l[rows] = part
            m[rows] = new
            a[at] = factor

    def weigh_two(r, p, acc, a, ck):
        rows = slice((r % 2) * POS, (r % 2 + 1) * POS)
        factor = jnp.concatenate([a[0:POS]] * 4, axis=1)
        acc[rows] = acc[rows] * factor + (
            dot(p[0:POS], keys(ck)) + dot(p[POS : 2 * POS], keys(ck + 1))
        )

    acc, m, l = (acc0, acc1), (m0, m1), (l0, l1)
    s, p, a = (s0, s1), (p0, p1), (a0, a1)

    def finish(r, first, last):
        rows = slice((r % 2) * POS + first, (r % 2) * POS + last)
        total_l = jnp.sum(l[r // 2][rows], axis=1, keepdims=True)
        ctx = acc[r // 2][rows] * (1.0 / total_l) * scale3 + shift3
        return ctx, m[r // 2][rows] + jnp.log2(total_l)

    def wide(v):
        return jnp.concatenate([v] * 4, axis=1)

    def received(ref):
        return jnp.broadcast_to(ref[0:1], (COLS, COLS)).T

    PIECES = (
        (1, (mrg_ctx, mrg_lse), (0,)), (3, (mrg_ctx, mrg_lse), (1,)),
        (1, (ctx_rx, lse_rx), (0, 1)), (3, (ctx_rx, lse_rx), (1, 0)),
        (1, (ctx_rx, lse_rx), (0, 0)), (3, (ctx_rx, lse_rx), (1, 1)),
    )

    def piece(n):
        dz, (ctx_to, lse_to), at = PIECES[n]
        dev = (x, y, c, ring(z, dz))
        return (
            copy_to(ctx_tx.at[n], ctx_to.at[at], c_send.at[n], c_recv.at[n], dev),
            copy_to(lse_tx.at[n], lse_to.at[at], e_send.at[n], e_recv.at[n], dev),
        )

    def send(n, ctx, lse):
        ctx_tx[n] = ctx.astype(BF)
        lse_tx[n] = lse.T[0:8]
        begin(piece(n))

    def arrive(n):
        for copy in piece(n):
            copy.wait_recv()

    def send_two_away():
        send(0, *finish(2, 0, COLS))
        send(1, *finish(2, COLS, POS))

    def send_direct():
        send(2, *finish(0, COLS, POS))
        send(3, *finish(1, 0, COLS))

    def send_merged():
        for n, r, first in ((0, 0, 0), (1, 1, COLS)):
            arrive(n)
            ctx, lse = finish(r, first, first + COLS)
            other = received(mrg_lse[n])
            top = jnp.maximum(lse, other)
            one, two = jnp.exp2(lse - top), jnp.exp2(other - top)
            both = one + two
            inv = 1.0 / both
            send(4 + n, ctx * wide(one * inv) + mrg_ctx[n].astype(F32) * wide(two * inv),
                 top + jnp.log2(both))

    T, Z, O = 0, 2, 3
    units = [
        (T, 0), (T, 1), (Z, 0), (T, 2), (T, 3), (Z, 2), (T, 4), (T, 5),
        (Z, 4), (Z, 6), (T, 6), (T, 7), (O, 0), (O, 2), (O, 4), (O, 6),
    ]

    def score_unit(u):
        kind, ck = units[u]
        score(0, ck, s[u % 2]) if kind == T else score_two(kind, ck, s[u % 2])

    def weigh_unit(u):
        kind, ck = units[u]
        b = u % 2
        if kind == T:
            weigh(p[b], acc0, a[b], ck)
        else:
            weigh_two(kind, p[b], acc1, a[b], ck)

    before = {
        0: lambda: ready(1),
        1: lambda: (arrived(5), arrived(6), queries(1)),
        2: lambda: (arrived(7), ready(2)),
        3: lambda: ready(3),
        4: lambda: (arrived(8), arrived(9)),
        5: lambda: (ready(4), arrived(10), arrived(11)),
        6: lambda: ready(5),
        7: lambda: (arrived(12), arrived(13), arrived(14), arrived(15)),
        8: lambda: (ready(6), ready(7)),
    }
    after = {10: send_two_away, 12: send_direct, 13: send_merged}
    ready(0)
    score_unit(0)
    for u, (kind, ck) in enumerate(units):
        if u in before:
            before[u]()
        if u > 0:
            weigh_unit(u - 1)
        if u + 1 < len(units):
            score_unit(u + 1)
        b = u % 2
        if kind == T:
            soften(s[b], p[b], m0, l0, a[b])
        else:
            soften_two(kind, s[b], p[b], m1, l1, a[b])
        if u in after:
            after[u]()
    weigh_unit(len(units) - 1)
    ctx, lse = finish(RING - 1, 0, POS)
    for n in range(2, 6):
        arrive(n)
    others = [
        jnp.concatenate([received(lse_rx[f, h]) for h in range(2)], axis=0) for f in range(2)
    ]
    top = jnp.maximum(jnp.maximum(lse, others[0]), others[1])
    weight = jnp.exp2(lse - top)
    norm = weight
    ctx = ctx * wide(weight)
    for f, o in enumerate(others):
        w = jnp.exp2(o - top)
        norm = norm + w
        ctx = ctx + ctx_rx[f].reshape(POS, C).astype(F32) * wide(w)
    ctx = (ctx * wide(1.0 / norm)).astype(BF)
    attended = (dot(ctx, wp[2]) + vec(9)).astype(BF)
    mixed = qres[RING - 1].astype(F32) + dot(attended, wp[3]) + vec(10)
    out[...] = mixed.astype(BF).reshape(ROWS, COLS, C)
    for copy in halo0 + halo1 + first_x + first_y + later_x + later_y + moved + to_z:
        copy.wait_send()
    for n in range(SLOTS):
        pass_on(n).wait_send()
    for n in range(6):
        for copy in piece(n):
            copy.wait_send()


def per_device(latent, *params):
    row = lambda v: v.reshape(1, C)
    args = [latent]
    for p in params:
        args.append(row(p) if p.ndim == 1 else (p.reshape(9, C, C) if p.ndim == 4 else p))
    dma = pltpu.SemaphoreType.DMA
    v = pltpu.VMEM
    scratch = [
        v((11, 1, C), F32), v((9, C, C), BF), v((9, C, C), BF), v((4, C, C), BF),
        v((4, COLS + 2 * LPAD, C), BF), v((COLS + 2 * LPAD, C), F32), v((3, 4, COLS, C), BF),
        v((POS, C), F32), v((4, COLS + 2 * HPAD, C), F32),
        v((3, 2, 2, C), F32), v((3, 22, 2, C), F32),
        v((SLOTS, 2, POS, C), BF), v((RING, POS, C), BF), v((RING * POS, C), BF),
        v((QT, KC), F32), v((QT, KC), F32), v((QT, KC), BF), v((QT, KC), BF),
        v((QT, C), F32), v((QT, C), F32),
        v((QT, 128), F32), v((QT, 128), F32), v((QT, 128), F32), v((QT, 128), F32),
        v((QT, 128), F32), v((QT, 128), F32),
        v((6, COLS, C), BF), v((6, 8, COLS), F32), v((2, 2, COLS, C), BF), v((2, 2, 8, COLS), F32),
        v((2, COLS, C), BF), v((2, 8, COLS), F32),
        dma((18,)), dma((2, 8)), dma((2, 8)), dma((3, 22)), dma((3, 22)),
        dma((30,)), dma((SLOTS, 2)), dma((SLOTS,)), dma((SLOTS,)), dma((3, 2)), dma((3, 2)),
        dma((6,)), dma((6,)), dma((6,)), dma((6,)),
    ]
    return pl.pallas_call(
        block_kernel,
        out_shape=jax.ShapeDtypeStruct((ROWS, COLS, C), BF),
        in_specs=[pl.BlockSpec(memory_space=pl.ANY)] * 18,
        out_specs=pl.BlockSpec(memory_space=pltpu.VMEM),
        scratch_shapes=scratch,
        compiler_params=pltpu.CompilerParams(
            collective_id=0, has_side_effects=True, vmem_limit_bytes=60 * 1024 * 1024
        ),
    )(*args)


def solution(mesh):
    finer = Mesh(mesh.devices.reshape(4, 4, 2, mesh.shape["head"]), AXES)
    return jax.shard_map(
        per_device,
        mesh=finer,
        in_specs=(P(TILE, "head", None),) + (P(),) * 17,
        out_specs=P(TILE, "head", None),
        check_vma=False,
    )
```

```python
import functools

import jax
import jax.numpy as jnp
from jax import lax
from jax.experimental import pallas as pl
from jax.experimental.pallas import tpu as pltpu
from jax.sharding import Mesh
from jax.sharding import PartitionSpec as P

C = 512
GROUPS = 32
AXES = ("tile_0", "tile_1", "tile_2", "head")
TILE = ("tile_0", "tile_1", "tile_2")
MESH = pl.DeviceIdType.MESH
BF = jnp.bfloat16
F32 = jnp.float32
EPS = 1e-06

ROWS, COLS = 2, 128
POS = ROWS * COLS
RING = 4
TILES = 32
SLOTS = 16
CHUNKS = 8
QT = 512
KC = 1024
LPAD = 16
HPAD = 8
NT = (((1,), (1,)), ((), ()))
NN = (((1,), (0,)), ((), ()))


ORDER = (
    (0, 0), (1, 0), (3, 0), (0, 1), (0, 3), (1, 1), (3, 3), (1, 3),
    (3, 1), (2, 0), (0, 2), (2, 2), (1, 2), (2, 1), (3, 2), (2, 3),
)
OWNER = (1, 3, 2, 0)


def slot_of(dx, dy):
    return ORDER.index((dx, dy))


def dot(a, b, dims=NN):
    return lax.dot_general(a, b, dims, preferred_element_type=F32)


def copy_to(src, dst, send, recv, dev):
    return pltpu.make_async_remote_copy(
        src_ref=src, dst_ref=dst, send_sem=send, recv_sem=recv, device_id=dev, device_id_type=MESH
    )


def block_kernel(*refs):
    hbm = refs[:18]
    out = refs[18]
    (
        vecs, w1, w2, wp, ext, tmp, act, hext, ar_tx, ar_rx,
        kv, qres, qq, s0, s1, p0, p1, acc0, acc1, m0, m1, l0, l1, a0, a1,
        ctx_tx, lse_tx, ctx_rx, lse_rx, mrg_ctx, mrg_lse,
        ld, h_send, h_recv, ar_send, ar_recv,
        kv_send, kv_recv, d_send, d_recv, q_send, q_recv, c_send, c_recv, e_send, e_recv,
    ) = refs[19:]
    x = lax.axis_index("tile_0")
    y = lax.axis_index("tile_1")
    c = lax.axis_index("tile_2")
    z = lax.axis_index("head")
    t = (x * RING + y) * 2 + c

    def ring(v, i):
        return lax.rem(v + i, RING)

    def tile_dev(dt, dz):
        n = lax.rem(t + dt + TILES, TILES)
        return (n // 8, lax.rem(n // 2, RING), lax.rem(n, 2), lax.rem(z + dz + RING, RING))

    sibling = (x, y, 1 - c, z)

    (lat, g1, b1, cw1, cb1, g2, b2, cw2, cb2, g3, b3, wq, bq, wk, wv, bv, wo, bo) = hbm
    loads = [pltpu.make_async_copy(lat, ext.at[1:3, LPAD : LPAD + COLS], ld.at[0])]
    for i, v in enumerate((g1, b1, cb1, g2, b2, cb2, g3, b3, bq, bv, bo)):
        loads.append(pltpu.make_async_copy(v, vecs.at[i], ld.at[1 + i]))
    loads.append(pltpu.make_async_copy(cw1, w1, ld.at[12]))
    loads.append(pltpu.make_async_copy(cw2, w2, ld.at[13]))
    for i, w in enumerate((wq, wk, wv, wo)):
        loads.append(pltpu.make_async_copy(w, wp.at[i], ld.at[14 + i]))
    for copy in loads:
        copy.start()

    for ref in (acc0, acc1, l0, l1):
        ref[...] = jnp.zeros_like(ref)
    for ref in (m0, m1):
        ref[...] = jnp.full_like(ref, -1e30)
    a1[...] = jnp.ones_like(a1)
    p1[...] = jnp.zeros_like(p1)

    barrier = pltpu.get_barrier_semaphore()
    column = [sibling]
    for i in (1, 3, 2):
        column += [(x, y, c, ring(z, i)), (x, y, 1 - c, ring(z, i))]
    plane = []
    for i in range(RING):
        plane += [(ring(x, i), ring(y, j), c, z) for j in range(RING) if i + j > 0]
    peers = column + plane
    for dt in (-1, 1):
        for dz in (-1, 0, 1):
            peers.append(tile_dev(dt, dz))
    for dev in peers:
        pl.semaphore_signal(barrier, inc=1, device_id=dev, device_id_type=MESH)
    pl.semaphore_wait(barrier, len(peers))

    loads[0].wait()

    def halo(buf, pad, k):
        lo, hi = pad, pad + COLS
        own = slice(lo, hi)
        first, last = slice(lo, lo + pad), slice(hi - pad, hi)
        left, right = slice(0, lo), slice(hi, hi + pad)
        plan = [
            ((1, 2, own), (3, 4, own), (-1, 0)),
            ((2, 3, own), (0, 1, own), (1, 0)),
            ((1, 3, first), (1, 3, right), (0, -1)),
            ((1, 3, last), (1, 3, left), (0, 1)),
            ((1, 2, first), (3, 4, right), (-1, -1)),
            ((1, 2, last), (3, 4, left), (-1, 1)),
            ((2, 3, first), (0, 1, right), (1, -1)),
            ((2, 3, last), (0, 1, left), (1, 1)),
        ]
        copies = []
        for n, (s, d, (dt, dz)) in enumerate(plan):
            copies.append(
                copy_to(
                    buf.at[s[0] : s[1], s[2]], buf.at[d[0] : d[1], d[2]],
                    h_send.at[k, n], h_recv.at[k, n], tile_dev(dt, dz),
                )
            )
        return copies

    def moments(v):
        return jnp.concatenate(
            [jnp.sum(v, axis=0, keepdims=True), jnp.sum(v * v, axis=0, keepdims=True)], axis=0
        )

    def all_stats(k, local, after_first, after_second, plane_first=False):
        total = local
        pending = []
        stages = [(0, column), (len(column), plane)]
        if plane_first:
            stages.reverse()
        for stage, ((base, devices), after) in enumerate(zip(stages, (after_first, after_second))):
            ar_tx[k, stage] = total
            copies = [
                copy_to(ar_tx.at[k, stage], ar_rx.at[k, base + n], ar_send.at[k, base + n],
                        ar_recv.at[k, base + n], dev)
                for n, dev in enumerate(devices)
            ]
            for copy in copies:
                copy.start()
            after()
            for n, copy in enumerate(copies):
                copy.wait_recv()
                total = total + ar_rx[k, base + n]
            pending += copies
        for copy in pending:
            copy.wait_send()
        return total

    lane = lax.broadcasted_iota(jnp.int32, (8, C), 1)

    def affine(total, gain, shift):
        both = jnp.concatenate([total, jnp.zeros((6, C), F32)], axis=0)
        for d in (1, 2, 4, 8):
            up = pltpu.roll(both, C - d, 1)
            down = pltpu.roll(both, d, 1)
            both = both + jnp.where((lane & d) == 0, up, down)
        members = float(POS * TILES * RING * (C // GROUPS))
        mean = both[0:1] / members
        var = jnp.maximum(both[1:2] / members - mean * mean, 0.0)
        scale = lax.rsqrt(var + EPS) * gain
        return scale, shift - mean * scale

    def activate(buf, pad, width, scale, shift):
        col = lax.broadcasted_iota(jnp.int32, (width, 1), 0)
        edge = ((col >= pad) | (z > 0)) & ((col < pad + COLS) | (z < RING - 1))

        for r in range(4):
            inside = edge
            if r == 0:
                inside = edge & (t > 0)
            if r == 3:
                inside = edge & (t < TILES - 1)
            u = buf[r].astype(F32) * scale + shift
            u = u / (1.0 + jnp.exp(-u))
            tmp[r, 0:width] = jnp.where(inside, u, 0.0)
            for dj in range(3):
                act[dj, r] = tmp[r, pad - 1 + dj : pad - 1 + dj + COLS].astype(BF)

    def conv(weight):
        total = None
        for di in range(3):
            for dj in range(3):
                d = dot(act[dj, di : di + 2].reshape(POS, C), weight[di * 3 + dj])
                total = d if total is None else total + d
        return total

    def vec(i):
        return vecs[i]

    halo0 = halo(ext, LPAD, 0)
    latent = ext[1:3, LPAD : LPAD + COLS].astype(F32).reshape(POS, C)

    def start_halo0():
        for copy in halo0:
            copy.start()

    total = all_stats(0, moments(latent), start_halo0, lambda: None)
    for copy in loads[1:12]:
        copy.wait()
    for copy in halo0:
        copy.wait_recv()
    scale, shift = affine(total, vec(0), vec(1))
    activate(ext, LPAD, COLS + 2 * LPAD, scale, shift)
    loads[12].wait()
    hid = conv(w1) + vec(2)

    hext[1:3, HPAD : HPAD + COLS] = hid.reshape(ROWS, COLS, C)
    halo1 = halo(hext, HPAD, 1)

    def start_halo1():
        for copy in halo1:
            copy.start()

    total = all_stats(1, moments(hid), start_halo1, lambda: None)
    for copy in halo1:
        copy.wait_recv()
    scale, shift = affine(total, vec(3), vec(4))
    activate(hext, HPAD, COLS + 2 * HPAD, scale, shift)
    loads[13].wait()
    second = conv(w2) + vec(5)
    latent = ext[1:3, LPAD : LPAD + COLS].astype(F32).reshape(POS, C)
    res = (latent + second).astype(BF)
    kv[0, 0] = res

    def half(n, h):
        return kv.at[n, 0, pl.ds(h * COLS, COLS)]

    def own_copy(axis, i, h, n):
        dev = (ring(x, i), y, c, z) if axis == "x" else (x, ring(y, i), c, z)
        back = RING - i
        there = slot_of(back, 0) if axis == "x" else slot_of(0, back)
        return copy_to(half(0, h), half(there, h), kv_send.at[n], kv_recv.at[there, h], dev)

    first_x = [own_copy("x", i, 0, k) for k, i in enumerate((1, 3, 2))]
    first_y = [own_copy("y", i, 1, 3 + k) for k, i in enumerate((1, 3, 2))]
    later_x = [own_copy("x", i, 1, 6 + k) for k, i in enumerate((1, 3))]
    later_y = [own_copy("y", i, 0, 8 + k) for k, i in enumerate((1, 3))]
    moved = []

    def hand_on(axis, h, source, there):
        step = (source[0] - there[0], source[1] - there[1])
        dev = (ring(x, step[0] % RING), y, c, z) if axis == "x" else (x, ring(y, step[1] % RING), c, z)
        n = slot_of(*there)
        copy = copy_to(half(slot_of(*source), h), half(n, h), kv_send.at[10 + len(moved)],
                       kv_recv.at[n, h], dev)
        moved.append(copy)
        return copy

    onward = [
        copy
        for far in ((1, 1), (3, 3), (1, 3), (3, 1))
        for copy in (hand_on("y", 0, (far[0], 0), far), hand_on("x", 1, (0, far[1]), far))
    ]
    onward_two = [hand_on("y", 0, (2, 0), (2, 2)), hand_on("x", 1, (0, 2), (2, 2))]
    for k in (1, 3):
        onward_two.append(hand_on("y", 0, (2, 0), (2, k)))
        onward_two.append(hand_on("x", 1, (0, 2), (k, 2)))
    relays = {
        (1, 0): [hand_on("x", 1, (1, 0), (2, 0))],
        (0, 1): [hand_on("y", 0, (0, 1), (0, 2))],
        (1, 1): [hand_on("y", 0, (1, 1), (1, 2)), hand_on("x", 1, (1, 1), (2, 1))],
        (3, 3): [hand_on("y", 0, (3, 3), (3, 2)), hand_on("x", 1, (3, 3), (2, 3))],
    }
    def to_column(i, h):
        place = OWNER.index(RING - i)
        rows = pl.ds(h * COLS, COLS)
        return copy_to(kv.at[0, 0, rows], qres.at[place, rows], q_send.at[place, h],
                       q_recv.at[place, h], (x, y, c, ring(z, i)))

    to_z = [to_column(i, h) for i, h in ((1, 0), (3, 0), (1, 1), (3, 1), (2, 0), (2, 1))]
    pass_own = copy_to(kv.at[0, 0], kv.at[0, 1], d_send.at[0], d_recv.at[0], sibling)

    def begin(copies):
        for copy in copies:
            copy.start()

    def far_half(n, h):
        return copy_to(half(0, h), half(n, h), kv_send.at[0], kv_recv.at[n, h], sibling)

    def forward():
        begin([pass_own] + to_z[2:])
        for k in (1, 3):
            far_half(slot_of(k, 0), 0).wait_recv()
            far_half(slot_of(0, k), 1).wait_recv()
        begin(onward)

    res32 = res.astype(F32)
    total = all_stats(
        2,
        moments(res32),
        lambda: begin(first_x[:2] + first_y[:2] + later_x + later_y + first_x[2:] + first_y[2:] + to_z[:2]),
        forward,
        plane_first=True,
    )
    def pass_on(n):
        return copy_to(kv.at[n, 0], kv.at[n, 1], d_send.at[n], d_recv.at[n], sibling)

    def wait_half(n, h):
        ref = kv.at[n, 0, pl.ds(h * COLS, COLS)]
        copy_to(ref, ref, kv_send.at[0], kv_recv.at[n, h], sibling).wait_recv()

    def arrived(n):
        dx, dy = ORDER[n]
        if dx:
            wait_half(n, 1)
        if dy:
            wait_half(n, 0)
        begin(relays.get((dx, dy), []))
        pass_on(n).start()

    def ready(ck):
        for j in range(2):
            pass_on(2 * ck + j).wait_recv()

    for n in range(1, 5):
        arrived(n)
    scale3, shift3 = affine(total, vec(6), vec(7))
    for copy in loads[14:]:
        copy.wait()
    qres[RING - 1] = res
    to_exp2 = scale3 * (1.4426950408889634 / C**0.5)

    def queries(tile):
        for r in range(2 * tile, min(2 * tile + 2, RING - 1)):
            for h in range(2):
                to_column(RING - OWNER[r], h).wait_recv()
        both = qres[2 * tile : 2 * tile + 2].reshape(QT, C)
        normed = (both.astype(F32) * scale3 + shift3).astype(BF)
        q = (dot(normed, wp[0]) + vec(8)).astype(BF)
        qq[tile * QT : (tile + 1) * QT] = (dot(q, wp[1], NT) * to_exp2).astype(BF)

    queries(0)
    far_half(slot_of(2, 0), 0).wait_recv()
    far_half(slot_of(0, 2), 1).wait_recv()
    begin(onward_two)

    def keys(ck):
        return kv[pl.ds(2 * ck, 2)].reshape(KC, C)

    def score(qt, ck, s):
        s[...] = dot(qq[qt * QT : (qt + 1) * QT], keys(ck), NT)

    def soften(s, p, m, l, a):
        step = 32
        for r in range(0, QT, step):
            rows = slice(r, r + step)
            sc = s[rows]
            old = m[rows]
            new = jnp.maximum(old, jnp.max(sc, axis=1, keepdims=True))
            e = jnp.exp2(sc - jnp.concatenate([new] * (KC // 128), axis=1))
            p[rows] = e.astype(BF)
            factor = jnp.exp2(old - new)
            part = l[rows] * factor
            for j in range(KC // 128):
                part = part + e[:, j * 128 : (j + 1) * 128]
            l[rows] = part
            m[rows] = new
            a[rows] = factor

    def weigh(p, acc, a, ck):
        factor = a[...]
        acc[...] = acc[...] * jnp.concatenate([factor] * 4, axis=1) + dot(p[...], keys(ck))

    def score_two(r, ck, s):
        for j in range(2):
            s[j * POS : (j + 1) * POS] = dot(qq[r * POS : (r + 1) * POS], keys(ck + j), NT)

    def soften_two(r, s, p, m, l, a):
        step, base = 16, (r % 2) * POS
        for i in range(0, POS, step):
            rows, at = slice(base + i, base + i + step), slice(i, i + step)
            low = slice(POS + i, POS + i + step)
            sc = jnp.concatenate([s[at], s[low]], axis=1)
            old = m[rows]
            new = jnp.maximum(old, jnp.max(sc, axis=1, keepdims=True))
            e = jnp.exp2(sc - jnp.concatenate([new] * (2 * KC // 128), axis=1))
            p[at] = e[:, :KC].astype(BF)
            p[low] = e[:, KC:].astype(BF)
            factor = jnp.exp2(old - new)
            part = l[rows] * factor
            for j in range(2 * KC // 128):
                part = part + e[:, j * 128 : (j + 1) * 128]
            l[rows] = part
            m[rows] = new
            a[at] = factor

    def weigh_two(r, p, acc, a, ck):
        rows = slice((r % 2) * POS, (r % 2 + 1) * POS)
        factor = jnp.concatenate([a[0:POS]] * 4, axis=1)
        acc[rows] = acc[rows] * factor + (
            dot(p[0:POS], keys(ck)) + dot(p[POS : 2 * POS], keys(ck + 1))
        )

    acc, m, l = (acc0, acc1), (m0, m1), (l0, l1)
    s, p, a = (s0, s1), (p0, p1), (a0, a1)

    def finish(r, first, last):
        rows = slice((r % 2) * POS + first, (r % 2) * POS + last)
        total_l = jnp.sum(l[r // 2][rows], axis=1, keepdims=True)
        ctx = acc[r // 2][rows] * (1.0 / total_l) * scale3 + shift3
        return ctx, m[r // 2][rows] + jnp.log2(total_l)

    def wide(v):
        return jnp.concatenate([v] * 4, axis=1)

    def received(ref):
        return jnp.broadcast_to(ref[0:1], (COLS, COLS)).T

    PIECES = (
        (1, (mrg_ctx, mrg_lse), (0,)), (3, (mrg_ctx, mrg_lse), (1,)),
        (1, (ctx_rx, lse_rx), (0, 1)), (3, (ctx_rx, lse_rx), (1, 0)),
        (1, (ctx_rx, lse_rx), (0, 0)), (3, (ctx_rx, lse_rx), (1, 1)),
    )

    def piece(n):
        dz, (ctx_to, lse_to), at = PIECES[n]
        dev = (x, y, c, ring(z, dz))
        return (
            copy_to(ctx_tx.at[n], ctx_to.at[at], c_send.at[n], c_recv.at[n], dev),
            copy_to(lse_tx.at[n], lse_to.at[at], e_send.at[n], e_recv.at[n], dev),
        )

    def send(n, ctx, lse):
        ctx_tx[n] = ctx.astype(BF)
        lse_tx[n] = lse.T[0:8]
        begin(piece(n))

    def arrive(n):
        for copy in piece(n):
            copy.wait_recv()

    def send_two_away():
        send(0, *finish(2, 0, COLS))
        send(1, *finish(2, COLS, POS))

    def send_direct():
        send(2, *finish(0, COLS, POS))
        send(3, *finish(1, 0, COLS))

    def send_merged():
        for n, r, first in ((0, 0, 0), (1, 1, COLS)):
            arrive(n)
            ctx, lse = finish(r, first, first + COLS)
            other = received(mrg_lse[n])
            top = jnp.maximum(lse, other)
            one, two = jnp.exp2(lse - top), jnp.exp2(other - top)
            both = one + two
            inv = 1.0 / both
            send(4 + n, ctx * wide(one * inv) + mrg_ctx[n].astype(F32) * wide(two * inv),
                 top + jnp.log2(both))

    T, Z, O = 0, 2, 3
    units = [
        (T, 0), (T, 1), (Z, 0), (T, 2), (T, 3), (Z, 2), (T, 4), (T, 5),
        (Z, 4), (Z, 6), (T, 6), (T, 7), (O, 0), (O, 2), (O, 4), (O, 6),
    ]

    def score_unit(u):
        kind, ck = units[u]
        score(0, ck, s[u % 2]) if kind == T else score_two(kind, ck, s[u % 2])

    def weigh_unit(u):
        kind, ck = units[u]
        b = u % 2
        if kind == T:
            weigh(p[b], acc0, a[b], ck)
        else:
            weigh_two(kind, p[b], acc1, a[b], ck)

    before = {
        0: lambda: ready(1),
        1: lambda: (arrived(5), arrived(6), queries(1)),
        2: lambda: (arrived(7), ready(2)),
        3: lambda: ready(3),
        4: lambda: (arrived(8), arrived(9)),
        5: lambda: (ready(4), arrived(10), arrived(11)),
        6: lambda: ready(5),
        7: lambda: (arrived(12), arrived(13), arrived(14), arrived(15)),
        8: lambda: (ready(6), ready(7)),
    }
    after = {10: send_two_away, 12: send_direct, 13: send_merged}
    ready(0)
    score_unit(0)
    for u, (kind, ck) in enumerate(units):
        if u in before:
            before[u]()
        if u > 0:
            weigh_unit(u - 1)
        if u + 1 < len(units):
            score_unit(u + 1)
        b = u % 2
        if kind == T:
            soften(s[b], p[b], m0, l0, a[b])
        else:
            soften_two(kind, s[b], p[b], m1, l1, a[b])
        if u in after:
            after[u]()
    weigh_unit(len(units) - 1)
    ctx, lse = finish(RING - 1, 0, POS)
    for n in range(2, 6):
        arrive(n)
    others = [
        jnp.concatenate([received(lse_rx[f, h]) for h in range(2)], axis=0) for f in range(2)
    ]
    top = jnp.maximum(jnp.maximum(lse, others[0]), others[1])
    weight = jnp.exp2(lse - top)
    norm = weight
    ctx = ctx * wide(weight)
    for f, o in enumerate(others):
        w = jnp.exp2(o - top)
        norm = norm + w
        ctx = ctx + ctx_rx[f].reshape(POS, C).astype(F32) * wide(w)
    ctx = (ctx * wide(1.0 / norm)).astype(BF)
    attended = (dot(ctx, wp[2]) + vec(9)).astype(BF)
    mixed = qres[RING - 1].astype(F32) + dot(attended, wp[3]) + vec(10)
    out[...] = mixed.astype(BF).reshape(ROWS, COLS, C)
    for copy in halo0 + halo1 + first_x + first_y + later_x + later_y + moved + to_z:
        copy.wait_send()
    for n in range(SLOTS):
        pass_on(n).wait_send()
    for n in range(6):
        for copy in piece(n):
            copy.wait_send()


def per_device(latent, *params):
    row = lambda v: v.reshape(1, C)
    args = [latent]
    for p in params:
        args.append(row(p) if p.ndim == 1 else (p.reshape(9, C, C) if p.ndim == 4 else p))
    dma = pltpu.SemaphoreType.DMA
    v = pltpu.VMEM
    scratch = [
        v((11, 1, C), F32), v((9, C, C), BF), v((9, C, C), BF), v((4, C, C), BF),
        v((4, COLS + 2 * LPAD, C), BF), v((4, COLS + 2 * LPAD, C), F32), v((3, 4, COLS, C), BF),
        v((4, COLS + 2 * HPAD, C), F32),
        v((3, 2, 2, C), F32), v((3, 22, 2, C), F32),
        v((SLOTS, 2, POS, C), BF), v((RING, POS, C), BF), v((RING * POS, C), BF),
        v((QT, KC), F32), v((QT, KC), F32), v((QT, KC), BF), v((QT, KC), BF),
        v((QT, C), F32), v((QT, C), F32),
        v((QT, 128), F32), v((QT, 128), F32), v((QT, 128), F32), v((QT, 128), F32),
        v((QT, 128), F32), v((QT, 128), F32),
        v((6, COLS, C), BF), v((6, 8, COLS), F32), v((2, 2, COLS, C), BF), v((2, 2, 8, COLS), F32),
        v((2, COLS, C), BF), v((2, 8, COLS), F32),
        dma((18,)), dma((2, 8)), dma((2, 8)), dma((3, 22)), dma((3, 22)),
        dma((30,)), dma((SLOTS, 2)), dma((SLOTS,)), dma((SLOTS,)), dma((3, 2)), dma((3, 2)),
        dma((6,)), dma((6,)), dma((6,)), dma((6,)),
    ]
    return pl.pallas_call(
        block_kernel,
        out_shape=jax.ShapeDtypeStruct((ROWS, COLS, C), BF),
        in_specs=[pl.BlockSpec(memory_space=pl.ANY)] * 18,
        out_specs=pl.BlockSpec(memory_space=pltpu.VMEM),
        scratch_shapes=scratch,
        compiler_params=pltpu.CompilerParams(
            collective_id=0, has_side_effects=True, vmem_limit_bytes=60 * 1024 * 1024
        ),
    )(*args)


def solution(mesh):
    finer = Mesh(mesh.devices.reshape(4, 4, 2, mesh.shape["head"]), AXES)
    return jax.shard_map(
        per_device,
        mesh=finer,
        in_specs=(P(TILE, "head", None),) + (P(),) * 17,
        out_specs=P(TILE, "head", None),
        check_vma=False,
    )
```

```python
import functools

import jax
import jax.numpy as jnp
from jax import lax
from jax.experimental import pallas as pl
from jax.experimental.pallas import tpu as pltpu
from jax.sharding import Mesh
from jax.sharding import PartitionSpec as P

C = 512
GROUPS = 32
AXES = ("tile_0", "tile_1", "tile_2", "head")
TILE = ("tile_0", "tile_1", "tile_2")
MESH = pl.DeviceIdType.MESH
BF = jnp.bfloat16
F32 = jnp.float32
EPS = 1e-06

ROWS, COLS = 2, 128
POS = ROWS * COLS
RING = 4
TILES = 32
SLOTS = 16
CHUNKS = 8
QT = 512
KC = 1024
LPAD = 16
HPAD = 8
NT = (((1,), (1,)), ((), ()))
NN = (((1,), (0,)), ((), ()))


ORDER = (
    (0, 0), (1, 0), (3, 0), (0, 1), (0, 3), (1, 1), (3, 3), (1, 3),
    (3, 1), (2, 0), (0, 2), (2, 2), (1, 2), (2, 1), (3, 2), (2, 3),
)
OWNER = (1, 3, 2, 0)


def slot_of(dx, dy):
    return ORDER.index((dx, dy))


def dot(a, b, dims=NN):
    return lax.dot_general(a, b, dims, preferred_element_type=F32)


def copy_to(src, dst, send, recv, dev):
    return pltpu.make_async_remote_copy(
        src_ref=src, dst_ref=dst, send_sem=send, recv_sem=recv, device_id=dev, device_id_type=MESH
    )


def block_kernel(*refs):
    hbm = refs[:18]
    out = refs[18]
    (
        vecs, w1, w2, wp, ext, tmp, act, hext, ar_tx, ar_rx,
        kv, qres, qq, s0, s1, p0, p1, acc0, acc1, m0, m1, l0, l1, a0, a1,
        ctx_tx, lse_tx, ctx_rx, lse_rx, mrg_ctx, mrg_lse,
        ld, h_send, h_recv, ar_send, ar_recv,
        kv_send, kv_recv, d_send, d_recv, q_send, q_recv, c_send, c_recv, e_send, e_recv,
    ) = refs[19:]
    x = lax.axis_index("tile_0")
    y = lax.axis_index("tile_1")
    c = lax.axis_index("tile_2")
    z = lax.axis_index("head")
    t = (x * RING + y) * 2 + c

    def ring(v, i):
        return lax.rem(v + i, RING)

    def tile_dev(dt, dz):
        n = lax.rem(t + dt + TILES, TILES)
        return (n // 8, lax.rem(n // 2, RING), lax.rem(n, 2), lax.rem(z + dz + RING, RING))

    sibling = (x, y, 1 - c, z)

    (lat, g1, b1, cw1, cb1, g2, b2, cw2, cb2, g3, b3, wq, bq, wk, wv, bv, wo, bo) = hbm
    loads = [pltpu.make_async_copy(lat, ext.at[1:3, LPAD : LPAD + COLS], ld.at[0])]
    for i, v in enumerate((g1, b1, cb1, g2, b2, cb2, g3, b3, bq, bv, bo)):
        loads.append(pltpu.make_async_copy(v, vecs.at[i], ld.at[1 + i]))
    loads.append(pltpu.make_async_copy(cw1, w1, ld.at[12]))
    loads.append(pltpu.make_async_copy(cw2, w2, ld.at[13]))
    for i, w in enumerate((wq, wk, wv, wo)):
        loads.append(pltpu.make_async_copy(w, wp.at[i], ld.at[14 + i]))
    for copy in loads:
        copy.start()

    for ref in (acc0, acc1, l0, l1):
        ref[...] = jnp.zeros_like(ref)
    for ref in (m0, m1):
        ref[...] = jnp.full_like(ref, -1e30)
    a1[...] = jnp.ones_like(a1)
    p1[...] = jnp.zeros_like(p1)

    barrier = pltpu.get_barrier_semaphore()
    column = [sibling]
    for i in (1, 3, 2):
        column += [(x, y, c, ring(z, i)), (x, y, 1 - c, ring(z, i))]
    plane = []
    for i in range(RING):
        plane += [(ring(x, i), ring(y, j), c, z) for j in range(RING) if i + j > 0]
    peers = column + plane
    for dt in (-1, 1):
        for dz in (-1, 0, 1):
            peers.append(tile_dev(dt, dz))
    for dev in peers:
        pl.semaphore_signal(barrier, inc=1, device_id=dev, device_id_type=MESH)
    pl.semaphore_wait(barrier, len(peers))

    loads[0].wait()

    def halo(buf, pad, k):
        lo, hi = pad, pad + COLS
        own = slice(lo, hi)
        first, last = slice(lo, lo + pad), slice(hi - pad, hi)
        left, right = slice(0, lo), slice(hi, hi + pad)
        plan = [
            ((1, 2, own), (3, 4, own), (-1, 0)),
            ((2, 3, own), (0, 1, own), (1, 0)),
            ((1, 3, first), (1, 3, right), (0, -1)),
            ((1, 3, last), (1, 3, left), (0, 1)),
            ((1, 2, first), (3, 4, right), (-1, -1)),
            ((1, 2, last), (3, 4, left), (-1, 1)),
            ((2, 3, first), (0, 1, right), (1, -1)),
            ((2, 3, last), (0, 1, left), (1, 1)),
        ]
        copies = []
        for n, (s, d, (dt, dz)) in enumerate(plan):
            copies.append(
                copy_to(
                    buf.at[s[0] : s[1], s[2]], buf.at[d[0] : d[1], d[2]],
                    h_send.at[k, n], h_recv.at[k, n], tile_dev(dt, dz),
                )
            )
        return copies

    lane = lax.broadcasted_iota(jnp.int32, (8, 128), 1)
    mine = lax.rem(lane, 16) == lax.broadcasted_iota(jnp.int32, (8, 128), 0)

    def over_groups(v):
        for d in (1, 2, 4, 8):
            v = v + jnp.where((lane & d) == 0, pltpu.roll(v, 128 - d, 1), pltpu.roll(v, d, 1))
        return v

    def moments(v):
        both = (jnp.sum(v, axis=0, keepdims=True), jnp.sum(v * v, axis=0, keepdims=True))
        rows = [b[:, n * 128 : (n + 1) * 128] for b in both for n in range(4)]
        return jnp.sum(
            jnp.where(mine, over_groups(jnp.concatenate(rows, axis=0)), 0.0), axis=0, keepdims=True
        )

    def all_stats(k, local, after_first, after_second, plane_first=False):
        total = local
        pending = []
        stages = [(0, column), (len(column), plane)]
        if plane_first:
            stages.reverse()
        for stage, ((base, devices), after) in enumerate(zip(stages, (after_first, after_second))):
            ar_tx[k, stage] = total
            copies = [
                copy_to(ar_tx.at[k, stage], ar_rx.at[k, base + n], ar_send.at[k, base + n],
                        ar_recv.at[k, base + n], dev)
                for n, dev in enumerate(devices)
            ]
            for copy in copies:
                copy.start()
            after()
            for n, copy in enumerate(copies):
                copy.wait_recv()
                total = total + ar_rx[k, base + n]
            pending += copies
        for copy in pending:
            copy.wait_send()
        return total

    def affine(total, gain, shift):
        rows = over_groups(jnp.where(mine, jnp.broadcast_to(total, (8, 128)), 0.0))
        sums, squares = (
            jnp.concatenate([rows[n : n + 1] for n in range(k, k + 4)], axis=1) for k in (0, 4)
        )
        members = float(POS * TILES * RING * (C // GROUPS))
        mean = sums / members
        var = jnp.maximum(squares / members - mean * mean, 0.0)
        scale = lax.rsqrt(var + EPS) * gain
        return scale, shift - mean * scale

    def activate(buf, pad, width, scale, shift):
        col = lax.broadcasted_iota(jnp.int32, (width, 1), 0)
        edge = ((col >= pad) | (z > 0)) & ((col < pad + COLS) | (z < RING - 1))

        for r in range(4):
            inside = edge
            if r == 0:
                inside = edge & (t > 0)
            if r == 3:
                inside = edge & (t < TILES - 1)
            u = buf[r].astype(F32) * scale + shift
            u = u / (1.0 + jnp.exp(-u))
            tmp[r, 0:width] = jnp.where(inside, u, 0.0)
            for dj in range(3):
                act[dj, r] = tmp[r, pad - 1 + dj : pad - 1 + dj + COLS].astype(BF)

    def conv(weight):
        total = None
        for di in range(3):
            for dj in range(3):
                d = dot(act[dj, di : di + 2].reshape(POS, C), weight[di * 3 + dj])
                total = d if total is None else total + d
        return total

    def vec(i):
        return vecs[i]

    halo0 = halo(ext, LPAD, 0)
    latent = ext[1:3, LPAD : LPAD + COLS].astype(F32).reshape(POS, C)

    def start_halo0():
        for copy in halo0:
            copy.start()

    total = all_stats(0, moments(latent), start_halo0, lambda: None)
    for copy in loads[1:12]:
        copy.wait()
    for copy in halo0:
        copy.wait_recv()
    scale, shift = affine(total, vec(0), vec(1))
    activate(ext, LPAD, COLS + 2 * LPAD, scale, shift)
    loads[12].wait()
    hid = conv(w1) + vec(2)

    hext[1:3, HPAD : HPAD + COLS] = hid.reshape(ROWS, COLS, C)
    halo1 = halo(hext, HPAD, 1)

    def start_halo1():
        for copy in halo1:
            copy.start()

    total = all_stats(1, moments(hid), start_halo1, lambda: None)
    for copy in halo1:
        copy.wait_recv()
    scale, shift = affine(total, vec(3), vec(4))
    activate(hext, HPAD, COLS + 2 * HPAD, scale, shift)
    loads[13].wait()
    second = conv(w2) + vec(5)
    latent = ext[1:3, LPAD : LPAD + COLS].astype(F32).reshape(POS, C)
    res = (latent + second).astype(BF)
    kv[0, 0] = res

    def half(n, h):
        return kv.at[n, 0, pl.ds(h * COLS, COLS)]

    def own_copy(axis, i, h, n):
        dev = (ring(x, i), y, c, z) if axis == "x" else (x, ring(y, i), c, z)
        back = RING - i
        there = slot_of(back, 0) if axis == "x" else slot_of(0, back)
        return copy_to(half(0, h), half(there, h), kv_send.at[n], kv_recv.at[there, h], dev)

    first_x = [own_copy("x", i, 0, k) for k, i in enumerate((1, 3, 2))]
    first_y = [own_copy("y", i, 1, 3 + k) for k, i in enumerate((1, 3, 2))]
    later_x = [own_copy("x", i, 1, 6 + k) for k, i in enumerate((1, 3))]
    later_y = [own_copy("y", i, 0, 8 + k) for k, i in enumerate((1, 3))]
    moved = []

    def hand_on(axis, h, source, there, first=0, rows=COLS):
        step = (source[0] - there[0], source[1] - there[1])
        dev = (ring(x, step[0] % RING), y, c, z) if axis == "x" else (x, ring(y, step[1] % RING), c, z)
        n = slot_of(*there)
        part = pl.ds(h * COLS + first, rows)
        copy = copy_to(kv.at[slot_of(*source), 0, part], kv.at[n, 0, part],
                       kv_send.at[10 + len(moved)], kv_recv.at[n, h], dev)
        moved.append(copy)
        return copy

    onward = [
        copy
        for far in ((1, 1), (3, 3), (1, 3), (3, 1))
        for copy in (hand_on("y", 0, (far[0], 0), far), hand_on("x", 1, (0, far[1]), far))
    ]
    onward_two = [hand_on("y", 0, (2, 0), (2, 2)), hand_on("x", 1, (0, 2), (2, 2))]
    for k in (1, 3):
        onward_two.append(hand_on("y", 0, (2, 0), (2, k)))
        onward_two.append(hand_on("x", 1, (0, 2), (k, 2)))
    relays = {
        (1, 0): [hand_on("x", 1, (1, 0), (2, 0), 0, 64)],
        (3, 0): [hand_on("x", 1, (3, 0), (2, 0), 64, 64)],
        (0, 1): [hand_on("y", 0, (0, 1), (0, 2), 0, 64)],
        (0, 3): [hand_on("y", 0, (0, 3), (0, 2), 64, 64)],
        (1, 1): [hand_on("y", 0, (1, 1), (1, 2)), hand_on("x", 1, (1, 1), (2, 1))],
        (3, 3): [hand_on("y", 0, (3, 3), (3, 2)), hand_on("x", 1, (3, 3), (2, 3))],
    }
    def to_column(i, h):
        place = OWNER.index(RING - i)
        rows = pl.ds(h * COLS, COLS)
        return copy_to(kv.at[0, 0, rows], qres.at[place, rows], q_send.at[place, h],
                       q_recv.at[place, h], (x, y, c, ring(z, i)))

    to_z = [to_column(i, h) for i, h in ((1, 0), (3, 0), (1, 1), (3, 1), (2, 0), (2, 1))]
    pass_own = copy_to(kv.at[0, 0], kv.at[0, 1], d_send.at[0], d_recv.at[0], sibling)

    def begin(copies):
        for copy in copies:
            copy.start()

    def far_half(n, h):
        return copy_to(half(0, h), half(n, h), kv_send.at[0], kv_recv.at[n, h], sibling)

    def forward():
        begin([pass_own] + to_z[2:])
        for k in (1, 3):
            far_half(slot_of(k, 0), 0).wait_recv()
            far_half(slot_of(0, k), 1).wait_recv()
        begin(onward)

    res32 = res.astype(F32)
    total = all_stats(
        2,
        moments(res32),
        lambda: begin(first_x[:2] + first_y[:2] + later_x + later_y + first_x[2:] + first_y[2:] + to_z[:2]),
        forward,
        plane_first=True,
    )
    def pass_on(n):
        return copy_to(kv.at[n, 0], kv.at[n, 1], d_send.at[n], d_recv.at[n], sibling)

    def wait_half(n, h):
        ref = kv.at[n, 0, pl.ds(h * COLS, COLS)]
        copy_to(ref, ref, kv_send.at[0], kv_recv.at[n, h], sibling).wait_recv()

    def arrived(n):
        dx, dy = ORDER[n]
        if dx:
            wait_half(n, 1)
        if dy:
            wait_half(n, 0)
        begin(relays.get((dx, dy), []))
        pass_on(n).start()

    def ready(ck):
        for j in range(2):
            pass_on(2 * ck + j).wait_recv()

    for n in range(1, 5):
        arrived(n)
    scale3, shift3 = affine(total, vec(6), vec(7))
    for copy in loads[14:]:
        copy.wait()
    qres[RING - 1] = res
    to_exp2 = scale3 * (1.4426950408889634 / C**0.5)

    def queries(tile):
        for r in range(2 * tile, min(2 * tile + 2, RING - 1)):
            for h in range(2):
                to_column(RING - OWNER[r], h).wait_recv()
        both = qres[2 * tile : 2 * tile + 2].reshape(QT, C)
        normed = (both.astype(F32) * scale3 + shift3).astype(BF)
        q = (dot(normed, wp[0]) + vec(8)).astype(BF)
        qq[tile * QT : (tile + 1) * QT] = (dot(q, wp[1], NT) * to_exp2).astype(BF)

    queries(0)
    far_half(slot_of(2, 0), 0).wait_recv()
    far_half(slot_of(0, 2), 1).wait_recv()
    begin(onward_two)

    def keys(ck):
        return kv[pl.ds(2 * ck, 2)].reshape(KC, C)

    def score(qt, ck, s):
        s[...] = dot(qq[qt * QT : (qt + 1) * QT], keys(ck), NT)

    def soften(s, p, m, l, a):
        step = 32
        for r in range(0, QT, step):
            rows = slice(r, r + step)
            sc = s[rows]
            old = m[rows]
            new = jnp.maximum(old, jnp.max(sc, axis=1, keepdims=True))
            e = jnp.exp2(sc - jnp.concatenate([new] * (KC // 128), axis=1))
            p[rows] = e.astype(BF)
            factor = jnp.exp2(old - new)
            part = l[rows] * factor
            for j in range(KC // 128):
                part = part + e[:, j * 128 : (j + 1) * 128]
            l[rows] = part
            m[rows] = new
            a[rows] = factor

    def weigh(p, acc, a, ck):
        factor = a[...]
        acc[...] = acc[...] * jnp.concatenate([factor] * 4, axis=1) + dot(p[...], keys(ck))

    def score_two(r, ck, s):
        for j in range(2):
            s[j * POS : (j + 1) * POS] = dot(qq[r * POS : (r + 1) * POS], keys(ck + j), NT)

    def soften_two(r, s, p, m, l, a):
        step, base = 16, (r % 2) * POS
        for i in range(0, POS, step):
            rows, at = slice(base + i, base + i + step), slice(i, i + step)
            low = slice(POS + i, POS + i + step)
            sc = jnp.concatenate([s[at], s[low]], axis=1)
            old = m[rows]
            new = jnp.maximum(old, jnp.max(sc, axis=1, keepdims=True))
            e = jnp.exp2(sc - jnp.concatenate([new] * (2 * KC // 128), axis=1))
            p[at] = e[:, :KC].astype(BF)
            p[low] = e[:, KC:].astype(BF)
            factor = jnp.exp2(old - new)
            part = l[rows] * factor
            for j in range(2 * KC // 128):
                part = part + e[:, j * 128 : (j + 1) * 128]
            l[rows] = part
            m[rows] = new
            a[at] = factor

    def weigh_two(r, p, acc, a, ck):
        rows = slice((r % 2) * POS, (r % 2 + 1) * POS)
        factor = jnp.concatenate([a[0:POS]] * 4, axis=1)
        acc[rows] = acc[rows] * factor + (
            dot(p[0:POS], keys(ck)) + dot(p[POS : 2 * POS], keys(ck + 1))
        )

    acc, m, l = (acc0, acc1), (m0, m1), (l0, l1)
    s, p, a = (s0, s1), (p0, p1), (a0, a1)

    def finish(r, first, last):
        rows = slice((r % 2) * POS + first, (r % 2) * POS + last)
        total_l = jnp.sum(l[r // 2][rows], axis=1, keepdims=True)
        ctx = acc[r // 2][rows] * (1.0 / total_l) * scale3 + shift3
        return ctx, m[r // 2][rows] + jnp.log2(total_l)

    def wide(v):
        return jnp.concatenate([v] * 4, axis=1)

    def received(ref):
        return jnp.broadcast_to(ref[0:1], (COLS, COLS)).T

    PIECES = (
        (1, (mrg_ctx, mrg_lse), (0,)), (3, (mrg_ctx, mrg_lse), (1,)),
        (1, (ctx_rx, lse_rx), (0, 1)), (3, (ctx_rx, lse_rx), (1, 0)),
        (1, (ctx_rx, lse_rx), (0, 0)), (3, (ctx_rx, lse_rx), (1, 1)),
    )

    def piece(n):
        dz, (ctx_to, lse_to), at = PIECES[n]
        dev = (x, y, c, ring(z, dz))
        return (
            copy_to(ctx_tx.at[n], ctx_to.at[at], c_send.at[n], c_recv.at[n], dev),
            copy_to(lse_tx.at[n], lse_to.at[at], e_send.at[n], e_recv.at[n], dev),
        )

    def send(n, ctx, lse):
        ctx_tx[n] = ctx.astype(BF)
        lse_tx[n] = lse.T[0:8]
        begin(piece(n))

    def arrive(n):
        for copy in piece(n):
            copy.wait_recv()

    def send_two_away():
        send(0, *finish(2, 0, COLS))
        send(1, *finish(2, COLS, POS))

    def send_direct():
        send(2, *finish(0, COLS, POS))
        send(3, *finish(1, 0, COLS))

    def send_merged():
        for n, r, first in ((0, 0, 0), (1, 1, COLS)):
            arrive(n)
            ctx, lse = finish(r, first, first + COLS)
            other = received(mrg_lse[n])
            top = jnp.maximum(lse, other)
            one, two = jnp.exp2(lse - top), jnp.exp2(other - top)
            both = one + two
            inv = 1.0 / both
            send(4 + n, ctx * wide(one * inv) + mrg_ctx[n].astype(F32) * wide(two * inv),
                 top + jnp.log2(both))

    T, Z, O = 0, 2, 3
    units = [
        (T, 0), (T, 1), (Z, 0), (T, 2), (T, 3), (Z, 2), (T, 4), (T, 5),
        (Z, 4), (Z, 6), (T, 6), (T, 7), (O, 0), (O, 2), (O, 4), (O, 6),
    ]

    def score_unit(u):
        kind, ck = units[u]
        score(0, ck, s[u % 2]) if kind == T else score_two(kind, ck, s[u % 2])

    def weigh_unit(u):
        kind, ck = units[u]
        b = u % 2
        if kind == T:
            weigh(p[b], acc0, a[b], ck)
        else:
            weigh_two(kind, p[b], acc1, a[b], ck)

    before = {
        0: lambda: ready(1),
        1: lambda: (arrived(5), arrived(6), queries(1)),
        2: lambda: (arrived(7), ready(2)),
        3: lambda: ready(3),
        4: lambda: (arrived(8), arrived(9)),
        5: lambda: (ready(4), arrived(10), arrived(11)),
        6: lambda: ready(5),
        7: lambda: (arrived(12), arrived(13), arrived(14), arrived(15)),
        8: lambda: (ready(6), ready(7)),
    }
    after = {10: send_two_away, 12: send_direct, 13: send_merged}
    ready(0)
    score_unit(0)
    for u, (kind, ck) in enumerate(units):
        if u in before:
            before[u]()
        if u > 0:
            weigh_unit(u - 1)
        if u + 1 < len(units):
            score_unit(u + 1)
        b = u % 2
        if kind == T:
            soften(s[b], p[b], m0, l0, a[b])
        else:
            soften_two(kind, s[b], p[b], m1, l1, a[b])
        if u in after:
            after[u]()
    weigh_unit(len(units) - 1)
    ctx, lse = finish(RING - 1, 0, POS)
    for n in range(2, 6):
        arrive(n)
    others = [
        jnp.concatenate([received(lse_rx[f, h]) for h in range(2)], axis=0) for f in range(2)
    ]
    top = jnp.maximum(jnp.maximum(lse, others[0]), others[1])
    weight = jnp.exp2(lse - top)
    norm = weight
    ctx = ctx * wide(weight)
    for f, o in enumerate(others):
        w = jnp.exp2(o - top)
        norm = norm + w
        ctx = ctx + ctx_rx[f].reshape(POS, C).astype(F32) * wide(w)
    ctx = (ctx * wide(1.0 / norm)).astype(BF)
    attended = (dot(ctx, wp[2]) + vec(9)).astype(BF)
    mixed = qres[RING - 1].astype(F32) + dot(attended, wp[3]) + vec(10)
    out[...] = mixed.astype(BF).reshape(ROWS, COLS, C)
    for copy in halo0 + halo1 + first_x + first_y + later_x + later_y + moved + to_z:
        copy.wait_send()
    for n in range(SLOTS):
        pass_on(n).wait_send()
    for n in range(6):
        for copy in piece(n):
            copy.wait_send()


def per_device(latent, *params):
    row = lambda v: v.reshape(1, C)
    args = [latent]
    for p in params:
        args.append(row(p) if p.ndim == 1 else (p.reshape(9, C, C) if p.ndim == 4 else p))
    dma = pltpu.SemaphoreType.DMA
    v = pltpu.VMEM
    scratch = [
        v((11, 1, C), F32), v((9, C, C), BF), v((9, C, C), BF), v((4, C, C), BF),
        v((4, COLS + 2 * LPAD, C), BF), v((4, COLS + 2 * LPAD, C), F32), v((3, 4, COLS, C), BF),
        v((4, COLS + 2 * HPAD, C), F32),
        v((3, 2, 1, 128), F32), v((3, 22, 1, 128), F32),
        v((SLOTS, 2, POS, C), BF), v((RING, POS, C), BF), v((RING * POS, C), BF),
        v((QT, KC), F32), v((QT, KC), F32), v((QT, KC), BF), v((QT, KC), BF),
        v((QT, C), F32), v((QT, C), F32),
        v((QT, 128), F32), v((QT, 128), F32), v((QT, 128), F32), v((QT, 128), F32),
        v((QT, 128), F32), v((QT, 128), F32),
        v((6, COLS, C), BF), v((6, 8, COLS), F32), v((2, 2, COLS, C), BF), v((2, 2, 8, COLS), F32),
        v((2, COLS, C), BF), v((2, 8, COLS), F32),
        dma((18,)), dma((2, 8)), dma((2, 8)), dma((3, 22)), dma((3, 22)),
        dma((32,)), dma((SLOTS, 2)), dma((SLOTS,)), dma((SLOTS,)), dma((3, 2)), dma((3, 2)),
        dma((6,)), dma((6,)), dma((6,)), dma((6,)),
    ]
    return pl.pallas_call(
        block_kernel,
        out_shape=jax.ShapeDtypeStruct((ROWS, COLS, C), BF),
        in_specs=[pl.BlockSpec(memory_space=pl.ANY)] * 18,
        out_specs=pl.BlockSpec(memory_space=pltpu.VMEM),
        scratch_shapes=scratch,
        compiler_params=pltpu.CompilerParams(
            collective_id=0, has_side_effects=True, vmem_limit_bytes=60 * 1024 * 1024
        ),
    )(*args)


def solution(mesh):
    finer = Mesh(mesh.devices.reshape(4, 4, 2, mesh.shape["head"]), AXES)
    return jax.shard_map(
        per_device,
        mesh=finer,
        in_specs=(P(TILE, "head", None),) + (P(),) * 17,
        out_specs=P(TILE, "head", None),
        check_vma=False,
    )
```

```python
import functools

import jax
import jax.numpy as jnp
from jax import lax
from jax.experimental import pallas as pl
from jax.experimental.pallas import tpu as pltpu
from jax.sharding import Mesh
from jax.sharding import PartitionSpec as P

C = 512
GROUPS = 32
AXES = ("tile_0", "tile_1", "tile_2", "head")
TILE = ("tile_0", "tile_1", "tile_2")
MESH = pl.DeviceIdType.MESH
BF = jnp.bfloat16
F32 = jnp.float32
EPS = 1e-06

ROWS, COLS = 2, 128
POS = ROWS * COLS
RING = 4
TILES = 32
SLOTS = 16
CHUNKS = 8
QT = 512
KC = 1024
LPAD = 16
HPAD = 8
NT = (((1,), (1,)), ((), ()))
NN = (((1,), (0,)), ((), ()))


ORDER = (
    (0, 0), (1, 0), (3, 0), (0, 1), (0, 3), (1, 1), (3, 3), (1, 3),
    (3, 1), (2, 0), (0, 2), (2, 2), (1, 2), (2, 1), (3, 2), (2, 3),
)
OWNER = (1, 3, 2, 0)


def slot_of(dx, dy):
    return ORDER.index((dx, dy))


def dot(a, b, dims=NN):
    return lax.dot_general(a, b, dims, preferred_element_type=F32)


def copy_to(src, dst, send, recv, dev):
    return pltpu.make_async_remote_copy(
        src_ref=src, dst_ref=dst, send_sem=send, recv_sem=recv, device_id=dev, device_id_type=MESH
    )


def block_kernel(*refs):
    hbm = refs[:18]
    out = refs[18]
    (
        vecs, w1, w2, wp, ext, tmp, act, hext, ar_tx, ar_rx,
        kv, qres, qq, s0, s1, p0, p1, acc0, acc1, m0, m1, l0, l1, a0, a1,
        ctx_tx, lse_tx, ctx_rx, lse_rx, mrg_ctx, mrg_lse,
        ld, h_send, h_recv, ar_send, ar_recv,
        kv_send, kv_recv, d_send, d_recv, q_send, q_recv, c_send, c_recv, e_send, e_recv,
    ) = refs[19:]
    x = lax.axis_index("tile_0")
    y = lax.axis_index("tile_1")
    c = lax.axis_index("tile_2")
    z = lax.axis_index("head")
    t = (x * RING + y) * 2 + c

    def ring(v, i):
        return lax.rem(v + i, RING)

    def tile_dev(dt, dz):
        n = lax.rem(t + dt + TILES, TILES)
        return (n // 8, lax.rem(n // 2, RING), lax.rem(n, 2), lax.rem(z + dz + RING, RING))

    sibling = (x, y, 1 - c, z)

    (lat, g1, b1, cw1, cb1, g2, b2, cw2, cb2, g3, b3, wq, bq, wk, wv, bv, wo, bo) = hbm
    loads = [pltpu.make_async_copy(lat, ext.at[1:3, LPAD : LPAD + COLS], ld.at[0])]
    for i, v in enumerate((g1, b1, cb1, g2, b2, cb2, g3, b3, bq, bv, bo)):
        loads.append(pltpu.make_async_copy(v, vecs.at[i], ld.at[1 + i]))
    loads.append(pltpu.make_async_copy(cw1, w1, ld.at[12]))
    loads.append(pltpu.make_async_copy(cw2, w2, ld.at[13]))
    for i, w in enumerate((wq, wk, wv, wo)):
        loads.append(pltpu.make_async_copy(w, wp.at[i], ld.at[14 + i]))
    loads[0].start()

    barrier = pltpu.get_barrier_semaphore()
    column = [sibling]
    for i in (1, 3, 2):
        column += [(x, y, c, ring(z, i)), (x, y, 1 - c, ring(z, i))]
    plane = []
    for i in range(RING):
        plane += [(ring(x, i), ring(y, j), c, z) for j in range(RING) if i + j > 0]
    peers = column + plane
    for dt in (-1, 1):
        for dz in (-1, 0, 1):
            peers.append(tile_dev(dt, dz))
    for dev in peers:
        pl.semaphore_signal(barrier, inc=1, device_id=dev, device_id_type=MESH)
    for copy in loads[1:]:
        copy.start()

    for ref in (acc0, acc1, l0, l1):
        ref[...] = jnp.zeros_like(ref)
    for ref in (m0, m1):
        ref[...] = jnp.full_like(ref, -1e30)
    a1[...] = jnp.ones_like(a1)
    p1[...] = jnp.zeros_like(p1)

    loads[0].wait()

    def halo(buf, pad, k):
        lo, hi = pad, pad + COLS
        own = slice(lo, hi)
        first, last = slice(lo, lo + pad), slice(hi - pad, hi)
        left, right = slice(0, lo), slice(hi, hi + pad)
        plan = [
            ((1, 2, own), (3, 4, own), (-1, 0)),
            ((2, 3, own), (0, 1, own), (1, 0)),
            ((1, 3, first), (1, 3, right), (0, -1)),
            ((1, 3, last), (1, 3, left), (0, 1)),
            ((1, 2, first), (3, 4, right), (-1, -1)),
            ((1, 2, last), (3, 4, left), (-1, 1)),
            ((2, 3, first), (0, 1, right), (1, -1)),
            ((2, 3, last), (0, 1, left), (1, 1)),
        ]
        copies = []
        for n, (s, d, (dt, dz)) in enumerate(plan):
            copies.append(
                copy_to(
                    buf.at[s[0] : s[1], s[2]], buf.at[d[0] : d[1], d[2]],
                    h_send.at[k, n], h_recv.at[k, n], tile_dev(dt, dz),
                )
            )
        return copies

    lane = lax.broadcasted_iota(jnp.int32, (8, 128), 1)
    mine = lax.rem(lane, 16) == lax.broadcasted_iota(jnp.int32, (8, 128), 0)

    def over_groups(v):
        for d in (1, 2, 4, 8):
            v = v + jnp.where((lane & d) == 0, pltpu.roll(v, 128 - d, 1), pltpu.roll(v, d, 1))
        return v

    def moments(v):
        both = (jnp.sum(v, axis=0, keepdims=True), jnp.sum(v * v, axis=0, keepdims=True))
        rows = [b[:, n * 128 : (n + 1) * 128] for b in both for n in range(4)]
        return jnp.sum(
            jnp.where(mine, over_groups(jnp.concatenate(rows, axis=0)), 0.0), axis=0, keepdims=True
        )

    stats_sent = []

    def all_stats(k, local, after_first, after_second, plane_first=False):
        total = local
        stages = [(0, column), (len(column), plane)]
        if plane_first:
            stages.reverse()
        for stage, ((base, devices), after) in enumerate(zip(stages, (after_first, after_second))):
            ar_tx[k, stage] = total
            copies = [
                copy_to(ar_tx.at[k, stage], ar_rx.at[k, base + n], ar_send.at[k, base + n],
                        ar_recv.at[k, base + n], dev)
                for n, dev in enumerate(devices)
            ]
            for copy in copies:
                copy.start()
            after()
            for n, copy in enumerate(copies):
                copy.wait_recv()
                total = total + ar_rx[k, base + n]
            stats_sent.extend(copies)
        return total

    def affine(total, gain, shift):
        rows = over_groups(jnp.where(mine, jnp.broadcast_to(total, (8, 128)), 0.0))
        sums, squares = (
            jnp.concatenate([rows[n : n + 1] for n in range(k, k + 4)], axis=1) for k in (0, 4)
        )
        members = float(POS * TILES * RING * (C // GROUPS))
        mean = sums / members
        var = jnp.maximum(squares / members - mean * mean, 0.0)
        scale = lax.rsqrt(var + EPS) * gain
        return scale, shift - mean * scale

    def activate(buf, pad, width, scale, shift):
        col = lax.broadcasted_iota(jnp.int32, (width, 1), 0)
        edge = ((col >= pad) | (z > 0)) & ((col < pad + COLS) | (z < RING - 1))

        for r in range(4):
            inside = edge
            if r == 0:
                inside = edge & (t > 0)
            if r == 3:
                inside = edge & (t < TILES - 1)
            u = buf[r].astype(F32) * scale + shift
            u = u / (1.0 + jnp.exp(-u))
            tmp[r, 0:width] = jnp.where(inside, u, 0.0)
            for dj in range(3):
                act[dj, r] = tmp[r, pad - 1 + dj : pad - 1 + dj + COLS].astype(BF)

    def conv(weight):
        total = None
        for di in range(3):
            for dj in range(3):
                d = dot(act[dj, di : di + 2].reshape(POS, C), weight[di * 3 + dj])
                total = d if total is None else total + d
        return total

    def vec(i):
        return vecs[i]

    halo0 = halo(ext, LPAD, 0)
    latent = ext[1:3, LPAD : LPAD + COLS].astype(F32).reshape(POS, C)

    def start_halo0():
        for copy in halo0:
            copy.start()

    first_moments = moments(latent)
    pl.semaphore_wait(barrier, len(peers))
    total = all_stats(0, first_moments, start_halo0, lambda: None)
    for copy in loads[1:12]:
        copy.wait()
    for copy in halo0:
        copy.wait_recv()
    scale, shift = affine(total, vec(0), vec(1))
    activate(ext, LPAD, COLS + 2 * LPAD, scale, shift)
    loads[12].wait()
    hid = conv(w1) + vec(2)

    hext[1:3, HPAD : HPAD + COLS] = hid.reshape(ROWS, COLS, C)
    halo1 = halo(hext, HPAD, 1)

    def start_halo1():
        for copy in halo1:
            copy.start()

    total = all_stats(1, moments(hid), start_halo1, lambda: None)
    for copy in halo1:
        copy.wait_recv()
    scale, shift = affine(total, vec(3), vec(4))
    activate(hext, HPAD, COLS + 2 * HPAD, scale, shift)
    loads[13].wait()
    second = conv(w2) + vec(5)
    latent = ext[1:3, LPAD : LPAD + COLS].astype(F32).reshape(POS, C)
    res = (latent + second).astype(BF)
    kv[0, 0] = res

    def half(n, h):
        return kv.at[n, 0, pl.ds(h * COLS, COLS)]

    def own_copy(axis, i, h, n):
        dev = (ring(x, i), y, c, z) if axis == "x" else (x, ring(y, i), c, z)
        back = RING - i
        there = slot_of(back, 0) if axis == "x" else slot_of(0, back)
        return copy_to(half(0, h), half(there, h), kv_send.at[n], kv_recv.at[there, h], dev)

    first_x = [own_copy("x", i, 0, k) for k, i in enumerate((1, 3, 2))]
    first_y = [own_copy("y", i, 1, 3 + k) for k, i in enumerate((1, 3, 2))]
    later_x = [own_copy("x", i, 1, 6 + k) for k, i in enumerate((1, 3))]
    later_y = [own_copy("y", i, 0, 8 + k) for k, i in enumerate((1, 3))]
    moved = []

    def hand_on(axis, h, source, there, first=0, rows=COLS):
        step = (source[0] - there[0], source[1] - there[1])
        dev = (ring(x, step[0] % RING), y, c, z) if axis == "x" else (x, ring(y, step[1] % RING), c, z)
        n = slot_of(*there)
        part = pl.ds(h * COLS + first, rows)
        copy = copy_to(kv.at[slot_of(*source), 0, part], kv.at[n, 0, part],
                       kv_send.at[10 + len(moved)], kv_recv.at[n, h], dev)
        moved.append(copy)
        return copy

    onward = [
        copy
        for far in ((1, 1), (3, 3), (1, 3), (3, 1))
        for copy in (hand_on("y", 0, (far[0], 0), far), hand_on("x", 1, (0, far[1]), far))
    ]
    onward_two = [hand_on("y", 0, (2, 0), (2, 2)), hand_on("x", 1, (0, 2), (2, 2))]
    for k in (1, 3):
        onward_two.append(hand_on("y", 0, (2, 0), (2, k)))
        onward_two.append(hand_on("x", 1, (0, 2), (k, 2)))
    relays = {
        (1, 0): [hand_on("x", 1, (1, 0), (2, 0), 0, 64)],
        (3, 0): [hand_on("x", 1, (3, 0), (2, 0), 64, 64)],
        (0, 1): [hand_on("y", 0, (0, 1), (0, 2), 0, 64)],
        (0, 3): [hand_on("y", 0, (0, 3), (0, 2), 64, 64)],
        (1, 1): [hand_on("y", 0, (1, 1), (1, 2)), hand_on("x", 1, (1, 1), (2, 1))],
        (3, 3): [hand_on("y", 0, (3, 3), (3, 2)), hand_on("x", 1, (3, 3), (2, 3))],
    }
    def to_column(i, h):
        place = OWNER.index(RING - i)
        rows = pl.ds(h * COLS, COLS)
        return copy_to(kv.at[0, 0, rows], qres.at[place, rows], q_send.at[place, h],
                       q_recv.at[place, h], (x, y, c, ring(z, i)))

    to_z = [to_column(i, h) for i, h in ((1, 0), (3, 0), (1, 1), (3, 1), (2, 0), (2, 1))]
    pass_own = copy_to(kv.at[0, 0], kv.at[0, 1], d_send.at[0], d_recv.at[0], sibling)

    def begin(copies):
        for copy in copies:
            copy.start()

    def far_half(n, h):
        return copy_to(half(0, h), half(n, h), kv_send.at[0], kv_recv.at[n, h], sibling)

    def forward():
        begin([pass_own] + to_z[2:])
        for k in (1, 3):
            far_half(slot_of(k, 0), 0).wait_recv()
            far_half(slot_of(0, k), 1).wait_recv()
        begin(onward)

    res32 = res.astype(F32)
    total = all_stats(
        2,
        moments(res32),
        lambda: begin(first_x[:2] + first_y[:2] + later_x + later_y + first_x[2:] + first_y[2:] + to_z[:2]),
        forward,
        plane_first=True,
    )
    def pass_on(n):
        return copy_to(kv.at[n, 0], kv.at[n, 1], d_send.at[n], d_recv.at[n], sibling)

    def wait_half(n, h):
        ref = kv.at[n, 0, pl.ds(h * COLS, COLS)]
        copy_to(ref, ref, kv_send.at[0], kv_recv.at[n, h], sibling).wait_recv()

    def arrived(n):
        dx, dy = ORDER[n]
        if dx:
            wait_half(n, 1)
        if dy:
            wait_half(n, 0)
        begin(relays.get((dx, dy), []))
        pass_on(n).start()

    def ready(ck):
        for j in range(2):
            pass_on(2 * ck + j).wait_recv()

    for n in range(1, 5):
        arrived(n)
    scale3, shift3 = affine(total, vec(6), vec(7))
    for copy in loads[14:]:
        copy.wait()
    qres[RING - 1] = res
    to_exp2 = scale3 * (1.4426950408889634 / C**0.5)

    def queries(tile):
        for r in range(2 * tile, min(2 * tile + 2, RING - 1)):
            for h in range(2):
                to_column(RING - OWNER[r], h).wait_recv()
        both = qres[2 * tile : 2 * tile + 2].reshape(QT, C)
        normed = (both.astype(F32) * scale3 + shift3).astype(BF)
        q = (dot(normed, wp[0]) + vec(8)).astype(BF)
        qq[tile * QT : (tile + 1) * QT] = (dot(q, wp[1], NT) * to_exp2).astype(BF)

    queries(0)
    far_half(slot_of(2, 0), 0).wait_recv()
    far_half(slot_of(0, 2), 1).wait_recv()
    begin(onward_two)

    def keys(ck):
        return kv[pl.ds(2 * ck, 2)].reshape(KC, C)

    def score(qt, ck, s):
        s[...] = dot(qq[qt * QT : (qt + 1) * QT], keys(ck), NT)

    def soften(s, p, m, l, a):
        step = 32
        for r in range(0, QT, step):
            rows = slice(r, r + step)
            sc = s[rows]
            old = m[rows]
            new = jnp.maximum(old, jnp.max(sc, axis=1, keepdims=True))
            e = jnp.exp2(sc - jnp.concatenate([new] * (KC // 128), axis=1))
            p[rows] = e.astype(BF)
            factor = jnp.exp2(old - new)
            part = l[rows] * factor
            for j in range(KC // 128):
                part = part + e[:, j * 128 : (j + 1) * 128]
            l[rows] = part
            m[rows] = new
            a[rows] = factor

    def weigh(p, acc, a, ck):
        factor = a[...]
        acc[...] = acc[...] * jnp.concatenate([factor] * 4, axis=1) + dot(p[...], keys(ck))

    def score_two(r, ck, s):
        for j in range(2):
            s[j * POS : (j + 1) * POS] = dot(qq[r * POS : (r + 1) * POS], keys(ck + j), NT)

    def soften_two(r, s, p, m, l, a):
        step, base = 16, (r % 2) * POS
        for i in range(0, POS, step):
            rows, at = slice(base + i, base + i + step), slice(i, i + step)
            low = slice(POS + i, POS + i + step)
            sc = jnp.concatenate([s[at], s[low]], axis=1)
            old = m[rows]
            new = jnp.maximum(old, jnp.max(sc, axis=1, keepdims=True))
            e = jnp.exp2(sc - jnp.concatenate([new] * (2 * KC // 128), axis=1))
            p[at] = e[:, :KC].astype(BF)
            p[low] = e[:, KC:].astype(BF)
            factor = jnp.exp2(old - new)
            part = l[rows] * factor
            for j in range(2 * KC // 128):
                part = part + e[:, j * 128 : (j + 1) * 128]
            l[rows] = part
            m[rows] = new
            a[at] = factor

    def weigh_two(r, p, acc, a, ck):
        rows = slice((r % 2) * POS, (r % 2 + 1) * POS)
        factor = jnp.concatenate([a[0:POS]] * 4, axis=1)
        acc[rows] = acc[rows] * factor + (
            dot(p[0:POS], keys(ck)) + dot(p[POS : 2 * POS], keys(ck + 1))
        )

    acc, m, l = (acc0, acc1), (m0, m1), (l0, l1)
    s, p, a = (s0, s1), (p0, p1), (a0, a1)

    def finish(r, first, last):
        rows = slice((r % 2) * POS + first, (r % 2) * POS + last)
        total_l = jnp.sum(l[r // 2][rows], axis=1, keepdims=True)
        ctx = acc[r // 2][rows] * (1.0 / total_l) * scale3 + shift3
        return ctx, m[r // 2][rows] + jnp.log2(total_l)

    def wide(v):
        return jnp.concatenate([v] * 4, axis=1)

    def received(ref):
        return jnp.broadcast_to(ref[0:1], (COLS, COLS)).T

    PIECES = (
        (1, (mrg_ctx, mrg_lse), (0,)), (3, (mrg_ctx, mrg_lse), (1,)),
        (1, (ctx_rx, lse_rx), (0, 1)), (3, (ctx_rx, lse_rx), (1, 0)),
        (1, (ctx_rx, lse_rx), (0, 0)), (3, (ctx_rx, lse_rx), (1, 1)),
    )

    def piece(n):
        dz, (ctx_to, lse_to), at = PIECES[n]
        dev = (x, y, c, ring(z, dz))
        return (
            copy_to(ctx_tx.at[n], ctx_to.at[at], c_send.at[n], c_recv.at[n], dev),
            copy_to(lse_tx.at[n], lse_to.at[at], e_send.at[n], e_recv.at[n], dev),
        )

    def send(n, ctx, lse):
        ctx_tx[n] = ctx.astype(BF)
        lse_tx[n] = lse.T[0:8]
        begin(piece(n))

    def arrive(n):
        for copy in piece(n):
            copy.wait_recv()

    def send_two_away():
        send(0, *finish(2, 0, COLS))
        send(1, *finish(2, COLS, POS))

    def send_direct():
        send(2, *finish(0, COLS, POS))
        send(3, *finish(1, 0, COLS))

    def send_merged():
        for n, r, first in ((0, 0, 0), (1, 1, COLS)):
            arrive(n)
            ctx, lse = finish(r, first, first + COLS)
            other = received(mrg_lse[n])
            top = jnp.maximum(lse, other)
            one, two = jnp.exp2(lse - top), jnp.exp2(other - top)
            both = one + two
            inv = 1.0 / both
            send(4 + n, ctx * wide(one * inv) + mrg_ctx[n].astype(F32) * wide(two * inv),
                 top + jnp.log2(both))

    T, Z, O = 0, 2, 3
    units = [
        (T, 0), (T, 1), (Z, 0), (T, 2), (T, 3), (Z, 2), (T, 4), (T, 5),
        (Z, 4), (Z, 6), (T, 6), (T, 7), (O, 0), (O, 2), (O, 4), (O, 6),
    ]

    def score_unit(u):
        kind, ck = units[u]
        score(0, ck, s[u % 2]) if kind == T else score_two(kind, ck, s[u % 2])

    def weigh_unit(u):
        kind, ck = units[u]
        b = u % 2
        if kind == T:
            weigh(p[b], acc0, a[b], ck)
        else:
            weigh_two(kind, p[b], acc1, a[b], ck)

    before = {
        0: lambda: ready(1),
        1: lambda: (arrived(5), arrived(6), queries(1)),
        2: lambda: (arrived(7), ready(2)),
        3: lambda: ready(3),
        4: lambda: (arrived(8), arrived(9)),
        5: lambda: (ready(4), arrived(10), arrived(11)),
        6: lambda: ready(5),
        7: lambda: (arrived(12), arrived(13), arrived(14), arrived(15)),
        8: lambda: (ready(6), ready(7)),
    }
    leave = {10: send_two_away, 12: send_direct}
    after = {13: send_merged}
    ready(0)
    score_unit(0)
    for u, (kind, ck) in enumerate(units):
        if u in before:
            before[u]()
        if u > 0:
            weigh_unit(u - 1)
        if u in leave:
            leave[u]()
        if u + 1 < len(units):
            score_unit(u + 1)
        b = u % 2
        if kind == T:
            soften(s[b], p[b], m0, l0, a[b])
        else:
            soften_two(kind, s[b], p[b], m1, l1, a[b])
        if u in after:
            after[u]()
    weigh_unit(len(units) - 1)
    ctx, lse = finish(RING - 1, 0, POS)
    for copy in stats_sent + halo0 + halo1 + first_x + first_y + later_x + later_y + moved + to_z:
        copy.wait_send()
    for n in range(SLOTS):
        pass_on(n).wait_send()
    for n in range(2, 6):
        arrive(n)
    others = [
        jnp.concatenate([received(lse_rx[f, h]) for h in range(2)], axis=0) for f in range(2)
    ]
    top = jnp.maximum(jnp.maximum(lse, others[0]), others[1])
    weight = jnp.exp2(lse - top)
    norm = weight
    ctx = ctx * wide(weight)
    for f, o in enumerate(others):
        w = jnp.exp2(o - top)
        norm = norm + w
        ctx = ctx + ctx_rx[f].reshape(POS, C).astype(F32) * wide(w)
    ctx = (ctx * wide(1.0 / norm)).astype(BF)
    attended = (dot(ctx, wp[2]) + vec(9)).astype(BF)
    mixed = qres[RING - 1].astype(F32) + dot(attended, wp[3]) + vec(10)
    out[...] = mixed.astype(BF).reshape(ROWS, COLS, C)
    for n in range(6):
        for copy in piece(n):
            copy.wait_send()


def per_device(latent, *params):
    row = lambda v: v.reshape(1, C)
    args = [latent]
    for p in params:
        args.append(row(p) if p.ndim == 1 else (p.reshape(9, C, C) if p.ndim == 4 else p))
    dma = pltpu.SemaphoreType.DMA
    v = pltpu.VMEM
    scratch = [
        v((11, 1, C), F32), v((9, C, C), BF), v((9, C, C), BF), v((4, C, C), BF),
        v((4, COLS + 2 * LPAD, C), BF), v((4, COLS + 2 * LPAD, C), F32), v((3, 4, COLS, C), BF),
        v((4, COLS + 2 * HPAD, C), F32),
        v((3, 2, 1, 128), F32), v((3, 22, 1, 128), F32),
        v((SLOTS, 2, POS, C), BF), v((RING, POS, C), BF), v((RING * POS, C), BF),
        v((QT, KC), F32), v((QT, KC), F32), v((QT, KC), BF), v((QT, KC), BF),
        v((QT, C), F32), v((QT, C), F32),
        v((QT, 128), F32), v((QT, 128), F32), v((QT, 128), F32), v((QT, 128), F32),
        v((QT, 128), F32), v((QT, 128), F32),
        v((6, COLS, C), BF), v((6, 8, COLS), F32), v((2, 2, COLS, C), BF), v((2, 2, 8, COLS), F32),
        v((2, COLS, C), BF), v((2, 8, COLS), F32),
        dma((18,)), dma((2, 8)), dma((2, 8)), dma((3, 22)), dma((3, 22)),
        dma((32,)), dma((SLOTS, 2)), dma((SLOTS,)), dma((SLOTS,)), dma((3, 2)), dma((3, 2)),
        dma((6,)), dma((6,)), dma((6,)), dma((6,)),
    ]
    return pl.pallas_call(
        block_kernel,
        out_shape=jax.ShapeDtypeStruct((ROWS, COLS, C), BF),
        in_specs=[pl.BlockSpec(memory_space=pl.ANY)] * 18,
        out_specs=pl.BlockSpec(memory_space=pltpu.VMEM),
        scratch_shapes=scratch,
        compiler_params=pltpu.CompilerParams(
            collective_id=0, has_side_effects=True, vmem_limit_bytes=60 * 1024 * 1024
        ),
    )(*args)


def solution(mesh):
    finer = Mesh(mesh.devices.reshape(4, 4, 2, mesh.shape["head"]), AXES)
    return jax.shard_map(
        per_device,
        mesh=finer,
        in_specs=(P(TILE, "head", None),) + (P(),) * 17,
        out_specs=P(TILE, "head", None),
        check_vma=False,
    )
```

```python
import functools

import jax
import jax.numpy as jnp
from jax import lax
from jax.experimental import pallas as pl
from jax.experimental.pallas import tpu as pltpu
from jax.sharding import Mesh
from jax.sharding import PartitionSpec as P

C = 512
GROUPS = 32
AXES = ("tile_0", "tile_1", "tile_2", "head")
TILE = ("tile_0", "tile_1", "tile_2")
MESH = pl.DeviceIdType.MESH
BF = jnp.bfloat16
F32 = jnp.float32
EPS = 1e-06

ROWS, COLS = 2, 128
POS = ROWS * COLS
RING = 4
TILES = 32
SLOTS = 16
CHUNKS = 8
QT = 512
KC = 1024
LPAD = 16
HPAD = 8
NT = (((1,), (1,)), ((), ()))
NN = (((1,), (0,)), ((), ()))


ORDER = (
    (0, 0), (1, 0), (3, 0), (0, 1), (0, 3), (1, 1), (3, 3), (1, 3),
    (3, 1), (2, 0), (0, 2), (2, 2), (1, 2), (2, 1), (3, 2), (2, 3),
)
OWNER = (1, 3, 2, 0)


def slot_of(dx, dy):
    return ORDER.index((dx, dy))


def dot(a, b, dims=NN):
    return lax.dot_general(a, b, dims, preferred_element_type=F32)


def copy_to(src, dst, send, recv, dev):
    return pltpu.make_async_remote_copy(
        src_ref=src, dst_ref=dst, send_sem=send, recv_sem=recv, device_id=dev, device_id_type=MESH
    )


def block_kernel(*refs):
    hbm = refs[:18]
    out = refs[18]
    (
        vecs, w1, w2, wp, ext, tmp, act, hext, ar_tx, ar_rx,
        kv, qres, qq, s0, s1, p0, p1, acc0, acc1, m0, m1, l0, l1, a0, a1,
        ctx_tx, lse_tx, ctx_rx, lse_rx, mrg_ctx, mrg_lse,
        ld, h_send, h_recv, ar_send, ar_recv,
        kv_send, kv_recv, d_send, d_recv, q_send, q_recv, c_send, c_recv, e_send, e_recv,
    ) = refs[19:]
    x = lax.axis_index("tile_0")
    y = lax.axis_index("tile_1")
    c = lax.axis_index("tile_2")
    z = lax.axis_index("head")
    t = (x * RING + y) * 2 + c

    def ring(v, i):
        return lax.rem(v + i, RING)

    def tile_dev(dt, dz):
        n = lax.rem(t + dt + TILES, TILES)
        return (n // 8, lax.rem(n // 2, RING), lax.rem(n, 2), lax.rem(z + dz + RING, RING))

    sibling = (x, y, 1 - c, z)

    (lat, g1, b1, cw1, cb1, g2, b2, cw2, cb2, g3, b3, wq, bq, wk, wv, bv, wo, bo) = hbm
    loads = [pltpu.make_async_copy(lat, ext.at[1:3, LPAD : LPAD + COLS], ld.at[0])]
    for i, v in enumerate((g1, b1, cb1, g2, b2, cb2, g3, b3, bq, bv, bo)):
        loads.append(pltpu.make_async_copy(v, vecs.at[i], ld.at[1 + i]))
    loads.append(pltpu.make_async_copy(cw1, w1, ld.at[12]))
    loads.append(pltpu.make_async_copy(cw2, w2, ld.at[13]))
    for i, w in enumerate((wq, wk, wv, wo)):
        loads.append(pltpu.make_async_copy(w, wp.at[i], ld.at[14 + i]))
    loads[0].start()

    barrier = pltpu.get_barrier_semaphore()
    column = [sibling]
    for i in (1, 3, 2):
        column += [(x, y, c, ring(z, i)), (x, y, 1 - c, ring(z, i))]
    plane = []
    for i in range(RING):
        plane += [(ring(x, i), ring(y, j), c, z) for j in range(RING) if i + j > 0]
    peers = column + plane
    for dt in (-1, 1):
        for dz in (-1, 0, 1):
            peers.append(tile_dev(dt, dz))
    for dev in peers:
        pl.semaphore_signal(barrier, inc=1, device_id=dev, device_id_type=MESH)
    for copy in loads[1:]:
        copy.start()

    for ref in (acc0, acc1, l0, l1):
        ref[...] = jnp.zeros_like(ref)
    for ref in (m0, m1):
        ref[...] = jnp.full_like(ref, -1e30)
    a1[...] = jnp.ones_like(a1)
    p1[...] = jnp.zeros_like(p1)

    loads[0].wait()

    def halo(buf, pad, k):
        lo, hi = pad, pad + COLS
        own = slice(lo, hi)
        first, last = slice(lo, lo + pad), slice(hi - pad, hi)
        left, right = slice(0, lo), slice(hi, hi + pad)
        plan = [
            ((1, 2, own), (3, 4, own), (-1, 0)),
            ((2, 3, own), (0, 1, own), (1, 0)),
            ((1, 3, first), (1, 3, right), (0, -1)),
            ((1, 3, last), (1, 3, left), (0, 1)),
            ((1, 2, first), (3, 4, right), (-1, -1)),
            ((1, 2, last), (3, 4, left), (-1, 1)),
            ((2, 3, first), (0, 1, right), (1, -1)),
            ((2, 3, last), (0, 1, left), (1, 1)),
        ]
        copies = []
        for n, (s, d, (dt, dz)) in enumerate(plan):
            copies.append(
                copy_to(
                    buf.at[s[0] : s[1], s[2]], buf.at[d[0] : d[1], d[2]],
                    h_send.at[k, n], h_recv.at[k, n], tile_dev(dt, dz),
                )
            )
        return copies

    lane = lax.broadcasted_iota(jnp.int32, (8, 128), 1)
    mine = lax.rem(lane, 16) == lax.broadcasted_iota(jnp.int32, (8, 128), 0)

    def over_groups(v):
        for d in (1, 2, 4, 8):
            v = v + jnp.where((lane & d) == 0, pltpu.roll(v, 128 - d, 1), pltpu.roll(v, d, 1))
        return v

    def moments(v):
        both = (jnp.sum(v, axis=0, keepdims=True), jnp.sum(v * v, axis=0, keepdims=True))
        rows = [b[:, n * 128 : (n + 1) * 128] for b in both for n in range(4)]
        return jnp.sum(
            jnp.where(mine, over_groups(jnp.concatenate(rows, axis=0)), 0.0), axis=0, keepdims=True
        )

    stats_sent = []

    def all_stats(k, local, after_first, after_second, plane_first=False):
        total = local
        stages = [(0, column), (len(column), plane)]
        if plane_first:
            stages.reverse()
        for stage, ((base, devices), after) in enumerate(zip(stages, (after_first, after_second))):
            ar_tx[k, stage] = total
            copies = [
                copy_to(ar_tx.at[k, stage], ar_rx.at[k, base + n], ar_send.at[k, base + n],
                        ar_recv.at[k, base + n], dev)
                for n, dev in enumerate(devices)
            ]
            for copy in copies:
                copy.start()
            after()
            for n, copy in enumerate(copies):
                copy.wait_recv()
                total = total + ar_rx[k, base + n]
            stats_sent.extend(copies)
        return total

    def affine(total, gain, shift):
        rows = over_groups(jnp.where(mine, jnp.broadcast_to(total, (8, 128)), 0.0))
        sums, squares = (
            jnp.concatenate([rows[n : n + 1] for n in range(k, k + 4)], axis=1) for k in (0, 4)
        )
        members = float(POS * TILES * RING * (C // GROUPS))
        mean = sums / members
        var = jnp.maximum(squares / members - mean * mean, 0.0)
        scale = lax.rsqrt(var + EPS) * gain
        return scale, shift - mean * scale

    def activate(buf, pad, width, scale, shift):
        col = lax.broadcasted_iota(jnp.int32, (width, 1), 0)
        edge = ((col >= pad) | (z > 0)) & ((col < pad + COLS) | (z < RING - 1))

        for r in range(4):
            inside = edge
            if r == 0:
                inside = edge & (t > 0)
            if r == 3:
                inside = edge & (t < TILES - 1)
            u = buf[r].astype(F32) * scale + shift
            u = u / (1.0 + jnp.exp(-u))
            tmp[r, 0:width] = jnp.where(inside, u, 0.0)
            for dj in range(3):
                act[dj, r] = tmp[r, pad - 1 + dj : pad - 1 + dj + COLS].astype(BF)

    def conv(weight):
        total = None
        for di in range(3):
            for dj in range(3):
                d = dot(act[dj, di : di + 2].reshape(POS, C), weight[di * 3 + dj])
                total = d if total is None else total + d
        return total

    def vec(i):
        return vecs[i]

    halo0 = halo(ext, LPAD, 0)
    latent = ext[1:3, LPAD : LPAD + COLS].astype(F32).reshape(POS, C)

    def start_halo0():
        for copy in halo0:
            copy.start()

    first_moments = moments(latent)
    pl.semaphore_wait(barrier, len(peers))
    total = all_stats(0, first_moments, start_halo0, lambda: None)
    for copy in loads[1:12]:
        copy.wait()
    for copy in halo0:
        copy.wait_recv()
    scale, shift = affine(total, vec(0), vec(1))
    activate(ext, LPAD, COLS + 2 * LPAD, scale, shift)
    loads[12].wait()
    hid = conv(w1) + vec(2)

    hext[1:3, HPAD : HPAD + COLS] = hid.reshape(ROWS, COLS, C)
    halo1 = halo(hext, HPAD, 1)

    def start_halo1():
        for copy in halo1:
            copy.start()

    total = all_stats(1, moments(hid), start_halo1, lambda: None)
    for copy in halo1:
        copy.wait_recv()
    scale, shift = affine(total, vec(3), vec(4))
    activate(hext, HPAD, COLS + 2 * HPAD, scale, shift)
    loads[13].wait()
    second = conv(w2) + vec(5)
    latent = ext[1:3, LPAD : LPAD + COLS].astype(F32).reshape(POS, C)
    res = (latent + second).astype(BF)
    kv[0, 0] = res

    def half(n, h):
        return kv.at[n, 0, pl.ds(h * COLS, COLS)]

    def own_copy(axis, i, h, n):
        dev = (ring(x, i), y, c, z) if axis == "x" else (x, ring(y, i), c, z)
        back = RING - i
        there = slot_of(back, 0) if axis == "x" else slot_of(0, back)
        return copy_to(half(0, h), half(there, h), kv_send.at[n], kv_recv.at[there, h], dev)

    first_x = [own_copy("x", i, 0, k) for k, i in enumerate((1, 3, 2))]
    first_y = [own_copy("y", i, 1, 3 + k) for k, i in enumerate((1, 3, 2))]
    later_x = [own_copy("x", i, 1, 6 + k) for k, i in enumerate((1, 3))]
    later_y = [own_copy("y", i, 0, 8 + k) for k, i in enumerate((1, 3))]
    moved = []

    def hand_on(axis, h, source, there, first=0, rows=COLS):
        step = (source[0] - there[0], source[1] - there[1])
        dev = (ring(x, step[0] % RING), y, c, z) if axis == "x" else (x, ring(y, step[1] % RING), c, z)
        n = slot_of(*there)
        part = pl.ds(h * COLS + first, rows)
        copy = copy_to(kv.at[slot_of(*source), 0, part], kv.at[n, 0, part],
                       kv_send.at[10 + len(moved)], kv_recv.at[n, h], dev)
        moved.append(copy)
        return copy

    onward = [
        copy
        for far in ((1, 1), (3, 3), (1, 3), (3, 1))
        for copy in (hand_on("y", 0, (far[0], 0), far), hand_on("x", 1, (0, far[1]), far))
    ]
    onward_two = [hand_on("y", 0, (2, 0), (2, 2)), hand_on("x", 1, (0, 2), (2, 2))]
    for k in (1, 3):
        onward_two.append(hand_on("y", 0, (2, 0), (2, k)))
        onward_two.append(hand_on("x", 1, (0, 2), (k, 2)))
    relays = {
        (1, 0): [hand_on("x", 1, (1, 0), (2, 0), 0, 64)],
        (3, 0): [hand_on("x", 1, (3, 0), (2, 0), 64, 64)],
        (0, 1): [hand_on("y", 0, (0, 1), (0, 2), 0, 64)],
        (0, 3): [hand_on("y", 0, (0, 3), (0, 2), 64, 64)],
        (1, 1): [hand_on("y", 0, (1, 1), (1, 2)), hand_on("x", 1, (1, 1), (2, 1))],
        (3, 3): [hand_on("y", 0, (3, 3), (3, 2)), hand_on("x", 1, (3, 3), (2, 3))],
    }
    def to_column(i, h):
        place = OWNER.index(RING - i)
        rows = pl.ds(h * COLS, COLS)
        return copy_to(kv.at[0, 0, rows], qres.at[place, rows], q_send.at[place, h],
                       q_recv.at[place, h], (x, y, c, ring(z, i)))

    to_z = [to_column(i, h) for i, h in ((1, 0), (3, 0), (1, 1), (3, 1), (2, 0), (2, 1))]
    pass_own = copy_to(kv.at[0, 0], kv.at[0, 1], d_send.at[0], d_recv.at[0], sibling)

    def begin(copies):
        for copy in copies:
            copy.start()

    def far_half(n, h):
        return copy_to(half(0, h), half(n, h), kv_send.at[0], kv_recv.at[n, h], sibling)

    def forward():
        begin([pass_own] + to_z[2:])
        for k in (1, 3):
            far_half(slot_of(k, 0), 0).wait_recv()
            far_half(slot_of(0, k), 1).wait_recv()
        begin(onward)

    res32 = res.astype(F32)
    total = all_stats(
        2,
        moments(res32),
        lambda: begin(first_x[:2] + first_y[:2] + later_x + later_y + first_x[2:] + first_y[2:] + to_z[:2]),
        forward,
        plane_first=True,
    )
    def pass_on(n):
        return copy_to(kv.at[n, 0], kv.at[n, 1], d_send.at[n], d_recv.at[n], sibling)

    def wait_half(n, h):
        ref = kv.at[n, 0, pl.ds(h * COLS, COLS)]
        copy_to(ref, ref, kv_send.at[0], kv_recv.at[n, h], sibling).wait_recv()

    def arrived(n):
        dx, dy = ORDER[n]
        if dx:
            wait_half(n, 1)
        if dy:
            wait_half(n, 0)
        begin(relays.get((dx, dy), []))
        pass_on(n).start()

    def ready(ck):
        for j in range(2):
            pass_on(2 * ck + j).wait_recv()

    for n in range(1, 5):
        arrived(n)
    scale3, shift3 = affine(total, vec(6), vec(7))
    for copy in loads[14:]:
        copy.wait()
    qres[RING - 1] = res
    to_exp2 = scale3 * (1.4426950408889634 / C**0.5)

    def queries(tile):
        for r in range(2 * tile, min(2 * tile + 2, RING - 1)):
            for h in range(2):
                to_column(RING - OWNER[r], h).wait_recv()
        both = qres[2 * tile : 2 * tile + 2].reshape(QT, C)
        normed = (both.astype(F32) * scale3 + shift3).astype(BF)
        q = (dot(normed, wp[0]) + vec(8)).astype(BF)
        qq[tile * QT : (tile + 1) * QT] = (dot(q, wp[1], NT) * to_exp2).astype(BF)

    queries(0)
    far_half(slot_of(2, 0), 0).wait_recv()
    far_half(slot_of(0, 2), 1).wait_recv()
    begin(onward_two)

    def keys(ck):
        return kv[pl.ds(2 * ck, 2)].reshape(KC, C)

    def score(qt, ck, s):
        s[...] = dot(qq[qt * QT : (qt + 1) * QT], keys(ck), NT)

    def soften(s, p, m, l, a):
        step = 32
        for r in range(0, QT, step):
            rows = slice(r, r + step)
            sc = s[rows]
            old = m[rows]
            new = jnp.maximum(old, jnp.max(sc, axis=1, keepdims=True))
            e = jnp.exp2(sc - jnp.concatenate([new] * (KC // 128), axis=1))
            p[rows] = e.astype(BF)
            factor = jnp.exp2(old - new)
            part = l[rows] * factor
            for j in range(KC // 128):
                part = part + e[:, j * 128 : (j + 1) * 128]
            l[rows] = part
            m[rows] = new
            a[rows] = factor

    def weigh(p, acc, a, ck):
        factor = a[...]
        acc[...] = acc[...] * jnp.concatenate([factor] * 4, axis=1) + dot(p[...], keys(ck))

    def score_two(r, ck, s):
        for j in range(2):
            s[j * POS : (j + 1) * POS] = dot(qq[r * POS : (r + 1) * POS], keys(ck + j), NT)

    def soften_two(r, s, p, m, l, a):
        step, base = 16, (r % 2) * POS
        for i in range(0, POS, step):
            rows, at = slice(base + i, base + i + step), slice(i, i + step)
            low = slice(POS + i, POS + i + step)
            sc = jnp.concatenate([s[at], s[low]], axis=1)
            old = m[rows]
            new = jnp.maximum(old, jnp.max(sc, axis=1, keepdims=True))
            e = jnp.exp2(sc - jnp.concatenate([new] * (2 * KC // 128), axis=1))
            p[at] = e[:, :KC].astype(BF)
            p[low] = e[:, KC:].astype(BF)
            factor = jnp.exp2(old - new)
            part = l[rows] * factor
            for j in range(2 * KC // 128):
                part = part + e[:, j * 128 : (j + 1) * 128]
            l[rows] = part
            m[rows] = new
            a[at] = factor

    def weigh_two(r, p, acc, a, ck):
        rows = slice((r % 2) * POS, (r % 2 + 1) * POS)
        factor = jnp.concatenate([a[0:POS]] * 4, axis=1)
        acc[rows] = acc[rows] * factor + (
            dot(p[0:POS], keys(ck)) + dot(p[POS : 2 * POS], keys(ck + 1))
        )

    acc, m, l = (acc0, acc1), (m0, m1), (l0, l1)
    s, p, a = (s0, s1), (p0, p1), (a0, a1)

    def finish(r, first, last):
        rows = slice((r % 2) * POS + first, (r % 2) * POS + last)
        total_l = jnp.sum(l[r // 2][rows], axis=1, keepdims=True)
        ctx = acc[r // 2][rows] * (1.0 / total_l) * scale3 + shift3
        return ctx, m[r // 2][rows] + jnp.log2(total_l)

    def wide(v):
        return jnp.concatenate([v] * 4, axis=1)

    def received(ref):
        return jnp.broadcast_to(ref[0:1], (COLS, COLS)).T

    PIECES = (
        (1, (mrg_ctx, mrg_lse), (0,)), (3, (mrg_ctx, mrg_lse), (1,)),
        (1, (ctx_rx, lse_rx), (0, 1)), (3, (ctx_rx, lse_rx), (1, 0)),
        (1, (ctx_rx, lse_rx), (0, 0)), (3, (ctx_rx, lse_rx), (1, 1)),
    )

    def piece(n):
        dz, (ctx_to, lse_to), at = PIECES[n]
        dev = (x, y, c, ring(z, dz))
        return (
            copy_to(ctx_tx.at[n], ctx_to.at[at], c_send.at[n], c_recv.at[n], dev),
            copy_to(lse_tx.at[n], lse_to.at[at], e_send.at[n], e_recv.at[n], dev),
        )

    def send(n, ctx, lse):
        ctx_tx[n] = ctx.astype(BF)
        lse_tx[n] = lse.T[0:8]
        begin(piece(n))

    def arrive(n):
        for copy in piece(n):
            copy.wait_recv()

    def send_two_away():
        send(0, *finish(2, 0, COLS))
        send(1, *finish(2, COLS, POS))

    def send_direct():
        send(2, *finish(0, COLS, POS))
        send(3, *finish(1, 0, COLS))

    def send_merged():
        for n, r, first in ((0, 0, 0), (1, 1, COLS)):
            arrive(n)
            ctx, lse = finish(r, first, first + COLS)
            other = received(mrg_lse[n])
            top = jnp.maximum(lse, other)
            one, two = jnp.exp2(lse - top), jnp.exp2(other - top)
            both = one + two
            inv = 1.0 / both
            send(4 + n, ctx * wide(one * inv) + mrg_ctx[n].astype(F32) * wide(two * inv),
                 top + jnp.log2(both))

    T, Z, O = 0, 2, 3
    units = [
        (T, 0), (T, 1), (Z, 0), (T, 2), (T, 3), (Z, 2), (T, 4), (T, 5),
        (Z, 4), (Z, 6), (T, 6), (T, 7), (O, 0), (O, 2), (O, 4), (O, 6),
    ]

    def score_unit(u):
        kind, ck = units[u]
        score(0, ck, s[u % 2]) if kind == T else score_two(kind, ck, s[u % 2])

    def weigh_unit(u):
        kind, ck = units[u]
        b = u % 2
        if kind == T:
            weigh(p[b], acc0, a[b], ck)
        else:
            weigh_two(kind, p[b], acc1, a[b], ck)

    before = {
        0: lambda: ready(1),
        1: lambda: (arrived(5), arrived(6), queries(1)),
        2: lambda: (arrived(7), ready(2)),
        3: lambda: ready(3),
        4: lambda: (arrived(8), arrived(9)),
        5: lambda: (ready(4), arrived(10), arrived(11)),
        6: lambda: ready(5),
        7: lambda: (arrived(12), arrived(13), arrived(14), arrived(15)),
        8: lambda: (ready(6), ready(7)),
    }
    leave = {10: send_two_away, 12: send_direct}
    after = {13: send_merged}
    ready(0)
    score_unit(0)
    for u, (kind, ck) in enumerate(units):
        if u > 0:
            weigh_unit(u - 1)
        if u in leave:
            leave[u]()
        if u in before:
            before[u]()
        if u + 1 < len(units):
            score_unit(u + 1)
        b = u % 2
        if kind == T:
            soften(s[b], p[b], m0, l0, a[b])
        else:
            soften_two(kind, s[b], p[b], m1, l1, a[b])
        if u in after:
            after[u]()
    weigh_unit(len(units) - 1)
    ctx, lse = finish(RING - 1, 0, POS)
    for copy in stats_sent + halo0 + halo1 + first_x + first_y + later_x + later_y + moved + to_z:
        copy.wait_send()
    for n in range(SLOTS):
        pass_on(n).wait_send()
    for n in range(2, 6):
        arrive(n)
    others = [
        jnp.concatenate([received(lse_rx[f, h]) for h in range(2)], axis=0) for f in range(2)
    ]
    top = jnp.maximum(jnp.maximum(lse, others[0]), others[1])
    weight = jnp.exp2(lse - top)
    norm = weight
    ctx = ctx * wide(weight)
    for f, o in enumerate(others):
        w = jnp.exp2(o - top)
        norm = norm + w
        ctx = ctx + ctx_rx[f].reshape(POS, C).astype(F32) * wide(w)
    ctx = (ctx * wide(1.0 / norm)).astype(BF)
    attended = (dot(ctx, wp[2]) + vec(9)).astype(BF)
    mixed = qres[RING - 1].astype(F32) + dot(attended, wp[3]) + vec(10)
    out[...] = mixed.astype(BF).reshape(ROWS, COLS, C)
    for n in range(6):
        for copy in piece(n):
            copy.wait_send()


def per_device(latent, *params):
    row = lambda v: v.reshape(1, C)
    args = [latent]
    for p in params:
        args.append(row(p) if p.ndim == 1 else (p.reshape(9, C, C) if p.ndim == 4 else p))
    dma = pltpu.SemaphoreType.DMA
    v = pltpu.VMEM
    scratch = [
        v((11, 1, C), F32), v((9, C, C), BF), v((9, C, C), BF), v((4, C, C), BF),
        v((4, COLS + 2 * LPAD, C), BF), v((4, COLS + 2 * LPAD, C), F32), v((3, 4, COLS, C), BF),
        v((4, COLS + 2 * HPAD, C), F32),
        v((3, 2, 1, 128), F32), v((3, 22, 1, 128), F32),
        v((SLOTS, 2, POS, C), BF), v((RING, POS, C), BF), v((RING * POS, C), BF),
        v((QT, KC), F32), v((QT, KC), F32), v((QT, KC), BF), v((QT, KC), BF),
        v((QT, C), F32), v((QT, C), F32),
        v((QT, 128), F32), v((QT, 128), F32), v((QT, 128), F32), v((QT, 128), F32),
        v((QT, 128), F32), v((QT, 128), F32),
        v((6, COLS, C), BF), v((6, 8, COLS), F32), v((2, 2, COLS, C), BF), v((2, 2, 8, COLS), F32),
        v((2, COLS, C), BF), v((2, 8, COLS), F32),
        dma((18,)), dma((2, 8)), dma((2, 8)), dma((3, 22)), dma((3, 22)),
        dma((32,)), dma((SLOTS, 2)), dma((SLOTS,)), dma((SLOTS,)), dma((3, 2)), dma((3, 2)),
        dma((6,)), dma((6,)), dma((6,)), dma((6,)),
    ]
    return pl.pallas_call(
        block_kernel,
        out_shape=jax.ShapeDtypeStruct((ROWS, COLS, C), BF),
        in_specs=[pl.BlockSpec(memory_space=pl.ANY)] * 18,
        out_specs=pl.BlockSpec(memory_space=pltpu.VMEM),
        scratch_shapes=scratch,
        compiler_params=pltpu.CompilerParams(
            collective_id=0, has_side_effects=True, vmem_limit_bytes=60 * 1024 * 1024
        ),
    )(*args)


def solution(mesh):
    finer = Mesh(mesh.devices.reshape(4, 4, 2, mesh.shape["head"]), AXES)
    return jax.shard_map(
        per_device,
        mesh=finer,
        in_specs=(P(TILE, "head", None),) + (P(),) * 17,
        out_specs=P(TILE, "head", None),
        check_vma=False,
    )
```
